32 devices in a mesh: rows: 8 (over z, y), fib: 4 (over x, core).
Axes of the slice: x: 2, y: 2, z: 4, core: 2. Of those that a mesh axis runs over, the one named last changes fastest.
Arguments:
- frames: bfloat16 [20, 1024, 1024], P('fib', 'rows'), may hold values from 0 to 2
- amplitude: float32 [20, 128], P('fib'), may hold values from 0.5 to 2
- line_start: int32 [20, 24], P('fib'), may hold values from 0 to 1016
- bundle_width: float32 [20], replicated, may hold values from 0.8 to 1.6
- fiber_bundle: int32 [128], replicated, may hold values from 0 to 19
- trace_coef: float32 [128, 11], P(('rows', 'fib')), may hold values from -1 to 1
- width_coef: float32 [128, 11], P(('rows', 'fib')), may hold values from -0.15 to 0.15
Outputs:
- trace_fit: float32 [128, 11], P(('rows', 'fib'))
- width_fit: float32 [128, 11], P(('rows', 'fib'))
- residual: bfloat16 [20, 1024, 1024], P('fib', 'rows')
The draws below stay inside these ranges and needn't reach their ends.
All inputs are finite; a program needn't handle non-finite values.
Results may differ from the reference program's by a relative error of at most 0.001.
Values sent between devices are 32-bit elements; how exact they have to be, the bound alone decides.
No kernel may reach another device: no remote copies, remote signals or barrier semaphores. Data moves between devices by JAX's collectives and lax.ppermute only.
A program may use at most 128 MiB of HBM per device.

```python
import math
import jax
import jax.numpy as jnp
from jax import lax

K = 11
LAMPS = 20
PIX = 8
LINES = 24
WIN = 8
BUNDLES = 20
ITERS = 3
FIBERS = 128
COLS = 1024
NR = 1024


def place_ends(result, own_key, least, largest):
    longest = result.shape.index(max(result.shape))
    spots = []
    for shift in (0, 1):
        where = [jax.random.randint(jax.random.fold_in(own_key, axis), (), 0, length) for axis, length in enumerate(result.shape)]
        where[longest] = (where[longest] + shift) % result.shape[longest]
        spots.append(tuple(where))
    return result.at[spots[0]].set(least).at[spots[1]].set(largest)


def level_of(key, extent, cuts, least, high):
    loudness, own = 1.0, jax.random.fold_in(key, 6)
    for position, blocks in cuts:
        steps = jnp.exp(jax.random.uniform(jax.random.fold_in(own, position), (blocks,), jnp.float32, least / len(cuts), high / len(cuts)))
        loudness = loudness * jnp.repeat(steps, extent[position] // blocks).reshape([-1 if axis == position else 1 for axis in range(len(extent))])
    return loudness


def bell_draw(own_key, shape, deviation, limit, cuts=(), kind=jnp.bfloat16):
    entries = deviation * jax.random.normal(own_key, shape, jnp.float32)
    if cuts:
        entries = entries * level_of(own_key, shape, cuts, -0.22, 0.18)
    return jnp.clip(entries, -limit, limit).astype(kind)


def setup_inputs(seed: int = 0) -> dict:
    streams_of = jax.random.split(jax.random.key(seed), 8)
    return {
        "frames": jnp.clip(2.0 * jax.random.uniform(streams_of[0], (LAMPS, NR, COLS), jnp.float32) ** level_of(streams_of[0], (LAMPS, NR, COLS), ((0, 4), (1, 8)), -0.2, 0.2), 0.0, 2.0).astype(jnp.bfloat16),
        "amplitude": jnp.clip(jnp.exp(math.log(2.0) - 1.3862944 * jax.random.uniform(streams_of[1], (LAMPS, FIBERS), jnp.float32) ** level_of(streams_of[1], (LAMPS, FIBERS), ((0, 4),), -0.2, 0.2)), 0.5, 2.0),
        "line_start": place_ends(jax.random.randint(streams_of[2], (LAMPS, LINES), 0, NR - WIN + 1), jax.random.fold_in(streams_of[2], 1), 0, NR - WIN).astype(jnp.int32),
        "bundle_width": jnp.clip(jnp.exp(jax.random.uniform(streams_of[3], (BUNDLES,), jnp.float32, math.log(0.8), math.log(1.6))), 0.8, 1.6),
        "fiber_bundle": place_ends(jax.random.randint(streams_of[4], (FIBERS,), 0, BUNDLES), jax.random.fold_in(streams_of[4], 1), 0, BUNDLES - 1).astype(jnp.int32),
        "trace_coef": bell_draw(streams_of[5], (FIBERS, K), 0.3, 1.0, ((0, 32),), jnp.float32),
        "width_coef": bell_draw(streams_of[6], (FIBERS, K), 0.05, 0.15, ((0, 32),), jnp.float32),
    }


HIGH = lax.Precision.HIGHEST

def legendre_table(first, count, total):
    rowpos = (first + jnp.arange(count, dtype=jnp.int32)).astype(jnp.float32)
    tvals = (2.0 * rowpos + 1.0) / total - 1.0
    polys = [jnp.ones_like(tvals), tvals]
    for order in range(1, K - 1):
        polys.append(((2 * order + 1) * tvals * polys[order] - order * polys[order - 1]) / (order + 1))
    return jnp.stack(polys[:K], axis=1)

def lit_rows(line_start, first, count):
    rowid = first + jnp.arange(count, dtype=jnp.int32)
    low = line_start[:, None, :]
    inside = (rowid[None, :, None] >= low) & (rowid[None, :, None] < low + WIN)
    return jnp.any(inside, axis=2).astype(jnp.float32)

def profile_cols(trace, width, bundle_width, fiber_bundle, ptab):
    onehot = (fiber_bundle[:, None] == jnp.arange(bundle_width.shape[0], dtype=jnp.int32)[None, :]).astype(jnp.float32)
    base = jnp.dot(onehot, bundle_width, precision=HIGH)
    centre = jnp.dot(ptab, trace.T, precision=HIGH)
    spread = base[None, :] * jnp.exp(jnp.dot(ptab, width.T, precision=HIGH))
    offsets = jnp.arange(PIX, dtype=jnp.float32) - (PIX - 1) / 2.0
    fibers = trace.shape[0]
    return (jnp.repeat(centre, PIX, axis=1), jnp.repeat(spread, PIX, axis=1), jnp.tile(offsets, fibers))

def lamp_model(lit_row, amp_row, centre, spread, offsets):
    scaled = (offsets[None, :] - centre) / spread
    shape = lit_row[:, None] * amp_row[None, :] * jnp.exp(-0.5 * scaled * scaled)
    return (shape, scaled)

def accumulate(frames, lit, amp_cols, centre, spread, offsets):

    def one_lamp(carry, item):
        frame, lit_row, amp_row = item
        shape, scaled = lamp_model(lit_row, amp_row, centre, spread, offsets)
        resid = frame.astype(jnp.float32) - shape
        slope = shape * scaled / spread
        widen = shape * scaled * scaled
        return ((carry[0] + slope * slope, carry[1] + slope * widen, carry[2] + widen * widen, carry[3] + resid * slope, carry[4] + resid * widen), None)
    zeros = jnp.zeros(centre.shape, jnp.float32)
    sums, _ = lax.scan(one_lamp, (zeros, zeros, zeros, zeros, zeros), (frames, lit, amp_cols))
    rows_here, cols = centre.shape
    return tuple((item.reshape(rows_here, cols // PIX, PIX).sum(axis=2) for item in sums))

def normal_blocks(sums, ptab):
    rows_here = ptab.shape[0]
    pairs = (ptab[:, :, None] * ptab[:, None, :]).reshape(rows_here, K * K)
    fibers = sums[0].shape[1]
    nxx = jnp.dot(sums[0].T, pairs, precision=HIGH).reshape(fibers, K, K)
    nxs = jnp.dot(sums[1].T, pairs, precision=HIGH).reshape(fibers, K, K)
    nss = jnp.dot(sums[2].T, pairs, precision=HIGH).reshape(fibers, K, K)
    upper = jnp.concatenate([nxx, nxs], axis=2)
    lower = jnp.concatenate([jnp.swapaxes(nxs, 1, 2), nss], axis=2)
    normal = jnp.concatenate([upper, lower], axis=1).reshape(fibers, 4 * K * K)
    grad = jnp.concatenate([jnp.dot(sums[3].T, ptab, precision=HIGH), jnp.dot(sums[4].T, ptab, precision=HIGH)], axis=1)
    return (normal, grad)

def solve_step(normal, grad, trace, width):
    fibers = normal.shape[0]
    matrix = normal.reshape(fibers, 2 * K, 2 * K)
    diag_vals = jnp.diagonal(matrix, axis1=1, axis2=2)
    eye_mat = jnp.eye(2 * K, dtype=jnp.float32)
    matrix = matrix + (0.5 * diag_vals + 1.0)[:, :, None] * eye_mat[None, :, :]
    factor = jnp.linalg.cholesky(matrix)
    inner = jax.scipy.linalg.solve_triangular(factor, grad[:, :, None], lower=True)
    update = jax.scipy.linalg.solve_triangular(factor, inner, lower=True, trans=1)[:, :, 0]
    return (trace + update[:, :K], width + update[:, K:])

def residual_image(frames, lit, amp_cols, centre, spread, offsets):

    def one_lamp(item):
        frame, lit_row, amp_row = item
        shape, scaled = lamp_model(lit_row, amp_row, centre, spread, offsets)
        return (frame.astype(jnp.float32) - shape).astype(jnp.bfloat16)
    return lax.map(one_lamp, (frames, lit, amp_cols))

def reference(frames, amplitude, line_start, bundle_width, fiber_bundle, trace_coef, width_coef):
    nrow = frames.shape[1]
    ptab = legendre_table(0, nrow, nrow)
    lit = lit_rows(line_start, 0, nrow)
    amp_cols = jnp.repeat(amplitude, PIX, axis=1)
    trace, width = (trace_coef, width_coef)
    for step in range(ITERS):
        centre, spread, offsets = profile_cols(trace, width, bundle_width, fiber_bundle, ptab)
        sums = accumulate(frames, lit, amp_cols, centre, spread, offsets)
        normal, grad = normal_blocks(sums, ptab)
        trace, width = solve_step(normal, grad, trace, width)
    centre, spread, offsets = profile_cols(trace, width, bundle_width, fiber_bundle, ptab)
    return (trace, width, residual_image(frames, lit, amp_cols, centre, spread, offsets))
```

```python
import functools

import jax
import jax.numpy as jnp
from jax import lax
from jax.experimental import pallas as pl
from jax.experimental.pallas import tpu as pltpu
from jax.sharding import PartitionSpec as P

K = 11
PIX = 8
WIN = 8
ITERS = 3
SUB = 8
LANE = 128
KROWS = 24
RHS = 2 * K

HIGH = lax.Precision.HIGHEST
BOTH = ("rows", "fib")


def legendre_list(rowpos, total):
    tvals = (2.0 * rowpos + 1.0) / total - 1.0
    polys = [jnp.ones_like(tvals), tvals]
    for order in range(1, K - 1):
        polys.append(
            ((2 * order + 1) * tvals * polys[order] - order * polys[order - 1]) / (order + 1)
        )
    return polys


def stacked_legendre(rowpos, total):
    polys = legendre_list(rowpos, total)
    row = lax.broadcasted_iota(jnp.int32, (KROWS, rowpos.shape[1]), 0)
    table = jnp.zeros((KROWS, rowpos.shape[1]), jnp.float32)
    for order in range(K):
        table = jnp.where((row == order) | (row == K + order), polys[order], table)
    return jnp.where(row == RHS, 1.0, table)


def lit_by_lamp(start, first, rows):
    lamps, lines = start.shape
    rowid = first + lax.broadcasted_iota(jnp.int32, (lamps, rows), 1)
    lit = jnp.zeros((lamps, rows), jnp.float32)
    for line in range(lines):
        away = rowid - start[:, line : line + 1]
        lit = jnp.where((away >= 0) & (away < WIN), 1.0, lit)
    return lit


def lit_columns(lit):
    lamps, rows = lit.shape
    which = lax.broadcasted_iota(jnp.int32, (lamps, lamps * LANE), 1) // LANE
    own = lax.broadcasted_iota(jnp.int32, (lamps, lamps * LANE), 0)
    spread = jnp.where(which == own, 1.0, 0.0)
    return lax.dot_general(
        lit, spread, (((0,), (0,)), ((), ())), preferred_element_type=jnp.float32
    )


def per_column(values, tile):
    each = LANE // PIX
    part = (tile * each) // LANE
    lane = lax.broadcasted_iota(jnp.int32, (values.shape[0], LANE), 1)
    index = (tile * each) % LANE + lane // PIX
    block = values[:, part * LANE : (part + 1) * LANE]
    return jnp.take_along_axis(block, index, axis=1, mode="promise_in_bounds")


def collapse_kernel(owned, frames_ref, amp_ref, start_ref, out_ref, lit_ref):
    lamps, rows, cols = frames_ref.shape
    first = lax.axis_index("rows") * rows
    amp = amp_ref[...]
    lit = lit_by_lamp(start_ref[...], first, rows)
    lit_ref[...] = lit_columns(lit)
    square = lax.dot_general(
        amp * amp, lit, (((0,), (0,)), ((), ())), precision=HIGH, preferred_element_type=jnp.float32
    )
    wide = owned * PIX
    for dest in range(cols // wide):
        out_ref[dest, wide : wide + owned, :] = square[dest * owned : (dest + 1) * owned]
    for tile in range(cols // LANE):
        amp_cols = per_column(amp, tile)
        total = jnp.zeros((rows, LANE), jnp.float32)
        for lamp in range(lamps):
            frame = frames_ref[lamp, :, tile * LANE : (tile + 1) * LANE].astype(jnp.float32)
            weight = lit_ref[:, lamp * LANE : (lamp + 1) * LANE] * amp_cols[lamp : lamp + 1]
            total = total + weight * frame
        flipped = total.T
        for part in range(LANE // wide):
            out_ref[tile * (LANE // wide) + part, 0:wide, :] = flipped[
                part * wide : (part + 1) * wide
            ]


def collapse(frames, amplitude, line_start, owned, height, devices):
    lamps, rows, cols = frames.shape
    return pl.pallas_call(
        functools.partial(collapse_kernel, owned),
        out_shape=jax.ShapeDtypeStruct((devices, height, rows), jnp.float32),
        in_specs=[pl.BlockSpec(memory_space=pltpu.VMEM)] * 3,
        out_specs=pl.BlockSpec(memory_space=pltpu.VMEM),
        scratch_shapes=[pltpu.VMEM((rows, lamps * LANE), jnp.float32)],
        name="collapse",
    )(frames, amplitude, line_start)


def fit_kernel(
    height,
    sources,
    bundle_ref,
    which_ref,
    got_ref,
    trace_ref,
    width_ref,
    trace_out,
    width_out,
    send_ref,
    sum_ref,
    poly_ref,
    high_ref,
    low_ref,
    weight_ref,
    coef_ref,
    splat_ref,
    square_ref,
):
    owned = trace_ref.shape[0]
    wide = owned * PIX
    steps = got_ref.shape[0] // (height * sources)
    rows = got_ref.shape[1]
    total_rows = steps * rows
    used = wide + owned
    me = lax.axis_index("rows") * sources + lax.axis_index("fib")

    for group in range(steps // SUB):
        for item in range(used):
            value = None
            for source in range(sources):
                start = (group * SUB * sources + source) * height + item
                part = got_ref[pl.ds(start, SUB, stride=sources * height), :]
                value = part if value is None else value + part
            sum_ref[item, group * SUB : (group + 1) * SUB, :] = value

    rowpos = (
        lax.broadcasted_iota(jnp.int32, (steps, rows), 0) * rows
        + lax.broadcasted_iota(jnp.int32, (steps, rows), 1)
    ).astype(jnp.float32)
    polys = legendre_list(rowpos, total_rows)
    for order in range(K):
        poly_ref[order * steps : (order + 1) * steps, :] = polys[order]
        poly_ref[(K + order) * steps : (K + order + 1) * steps, :] = polys[order]
    poly_ref[RHS * steps : (RHS + 1) * steps, :] = jnp.ones((steps, rows), jnp.float32)
    poly_ref[(RHS + 1) * steps :, :] = jnp.zeros((steps, rows), jnp.float32)
    for step in range(steps):
        stack = poly_ref[pl.ds(step, KROWS, stride=steps), :]
        pairs = jnp.concatenate([stack * stack[i : i + 1] for i in range(K)], axis=0)
        high = pairs.astype(jnp.bfloat16)
        high_ref[:, step * rows : (step + 1) * rows] = high
        low_ref[:, step * rows : (step + 1) * rows] = (pairs - high.astype(jnp.float32)).astype(
            jnp.bfloat16
        )

    square_ref[...] = jnp.zeros_like(square_ref)
    square_ref[0:owned, 0:K] = trace_ref[...]
    square_ref[0:owned, K : 2 * K] = width_ref[...]
    coef_ref[...] = square_ref[...].T[0:KROWS]
    weight_ref[...] = jnp.zeros_like(weight_ref)

    inverse_base = []
    for fiber in range(owned):
        base = bundle_ref[which_ref[me * owned + fiber]]
        inverse_base.append(1.0 / jnp.full((1, rows), base, jnp.float32))

    def newton_step(index, carry):
        for fiber in range(owned):
            splat_ref[fiber] = jnp.broadcast_to(
                coef_ref[:, fiber : fiber + 1], (KROWS, rows)
            )
        for group in range(steps // SUB):
            here = slice(group * SUB, (group + 1) * SUB)
            for fiber in range(owned):
                centre = jnp.zeros((SUB, rows), jnp.float32)
                spread = jnp.zeros((SUB, rows), jnp.float32)
                for order in range(K):
                    poly = poly_ref[order * steps + group * SUB : order * steps + (group + 1) * SUB, :]
                    centre = centre + splat_ref[fiber, order : order + 1, :] * poly
                    spread = spread + splat_ref[fiber, K + order : K + order + 1, :] * poly
                inverse = jnp.exp(-spread) * inverse_base[fiber]
                power = sum_ref[wide + fiber, here, :]
                sums = [jnp.zeros((SUB, rows), jnp.float32) for _ in range(5)]
                for pixel in range(PIX):
                    scaled = ((pixel - (PIX - 1) / 2.0) - centre) * inverse
                    shape = jnp.exp(-0.5 * scaled * scaled)
                    bend = shape * scaled
                    slope = bend * inverse
                    widen = bend * scaled
                    resid = sum_ref[fiber * PIX + pixel, here, :] - power * shape
                    sums[0] = sums[0] + slope * slope
                    sums[1] = sums[1] + slope * widen
                    sums[2] = sums[2] + widen * widen
                    sums[3] = sums[3] + resid * slope
                    sums[4] = sums[4] + resid * widen
                for kind in range(5):
                    value = sums[kind] * power if kind < 3 else sums[kind]
                    at = (kind * owned + fiber) * steps + group * SUB
                    weight_ref[at : at + SUB, :] = value
        count = weight_ref.shape[0] // steps
        weights = jnp.concatenate(
            [weight_ref[pl.ds(step, count, stride=steps), :] for step in range(steps)], axis=1
        )
        upper = weights.astype(jnp.bfloat16).astype(jnp.float32)
        both = jnp.concatenate([upper, weights - upper], axis=0).astype(jnp.bfloat16)
        dims = (((1,), (1,)), ((), ()))
        moments = lax.dot_general(
            high_ref[...], both, dims, preferred_element_type=jnp.float32
        ) + lax.dot_general(low_ref[...], both, dims, preferred_element_type=jnp.float32)
        lanes = moments.shape[1]
        moments = jnp.concatenate(
            [moments, jnp.zeros((moments.shape[0], LANE - lanes), jnp.float32)], axis=1
        )
        moments = moments + pltpu.roll(moments, LANE - count, 1)
        aligned = [moments] + [
            pltpu.roll(moments, LANE - kind * owned, 1) for kind in range(1, 5)
        ]
        row = lax.broadcasted_iota(jnp.int32, (KROWS, LANE), 0)

        def matrix_row(i, second):
            block = [item[i * KROWS : (i + 1) * KROWS] for item in aligned]
            left, right, side = (block[1], block[2], block[4]) if second else (
                block[0],
                block[1],
                block[3],
            )
            value = jnp.where(row < K, left, jnp.where(row < 2 * K, right, side))
            at = i + K if second else i
            return jnp.where(row == at, 1.5 * value + 1.0, value)

        matrix = [matrix_row(i, False) for i in range(K)] + [matrix_row(i, True) for i in range(K)]
        for pivot in range(2 * K):
            cut = KROWS - matrix[pivot].shape[0]
            inverse = 1.0 / matrix[pivot][pivot - cut : pivot - cut + 1]
            chosen = matrix[pivot] * inverse
            for i in range(2 * K):
                if i != pivot:
                    scale = matrix[i][pivot - cut : pivot - cut + 1]
                    matrix[i] = matrix[i] - scale * chosen
            matrix[pivot] = chosen
            if (pivot + 1) % SUB == 0:
                matrix = [item[SUB:] for item in matrix]
        for i in range(2 * K):
            cut = KROWS - matrix[i].shape[0]
            coef_ref[i : i + 1, :] = coef_ref[i : i + 1, :] + matrix[i][RHS - cut : RHS - cut + 1]
        return carry

    lax.fori_loop(0, ITERS, newton_step, 0)

    square_ref[...] = jnp.zeros_like(square_ref)
    lane = lax.broadcasted_iota(jnp.int32, (KROWS, LANE), 1)
    square_ref[0:KROWS, :] = jnp.where(lane < owned, coef_ref[...], 0.0)
    result = square_ref[...].T[0:owned]
    trace_out[...] = result[:, 0:K]
    width_out[...] = result[:, K : 2 * K]
    for device in range(send_ref.shape[0]):
        send_ref[device] = result


def fit(got, bundle_width, fiber_bundle, trace_coef, width_coef, devices, height, sources):
    owned = trace_coef.shape[0]
    rows = got.shape[1]
    steps = devices // sources
    count = -(-5 * owned // SUB) * SUB
    vmem = pl.BlockSpec(memory_space=pltpu.VMEM)
    smem = pl.BlockSpec(memory_space=pltpu.SMEM)
    return pl.pallas_call(
        functools.partial(fit_kernel, height, sources),
        out_shape=(
            jax.ShapeDtypeStruct((owned, K), jnp.float32),
            jax.ShapeDtypeStruct((owned, K), jnp.float32),
            jax.ShapeDtypeStruct((devices, owned, LANE), jnp.float32),
        ),
        in_specs=[smem, smem, vmem, vmem, vmem],
        out_specs=(vmem, vmem, vmem),
        scratch_shapes=[
            pltpu.VMEM((owned * PIX + owned, steps, rows), jnp.float32),
            pltpu.VMEM((KROWS * steps, rows), jnp.float32),
            pltpu.VMEM((K * KROWS, steps * rows), jnp.bfloat16),
            pltpu.VMEM((K * KROWS, steps * rows), jnp.bfloat16),
            pltpu.VMEM((count * steps, rows), jnp.float32),
            pltpu.VMEM((KROWS, LANE), jnp.float32),
            pltpu.VMEM((owned, KROWS, rows), jnp.float32),
            pltpu.VMEM((LANE, LANE), jnp.float32),
        ],
        name="fit",
    )(bundle_width, fiber_bundle, got, trace_coef, width_coef)


def residual_kernel(
    bundle_ref, which_ref, coef_ref, frames_ref, amp_ref, start_ref, out_ref, lit_ref
):
    lamps, rows, cols = frames_ref.shape
    total_rows = rows * lax.axis_size("rows")
    fibers = coef_ref.shape[0]
    first = lax.axis_index("rows") * rows
    lit_ref[...] = lit_columns(lit_by_lamp(start_ref[...], first, rows))
    which = which_ref[...]
    base = jnp.zeros((1, fibers), jnp.float32)
    for bundle in range(bundle_ref.shape[0]):
        base = jnp.where(which == bundle, bundle_ref[bundle], base)

    rowpos = (first + lax.broadcasted_iota(jnp.int32, (1, rows), 1)).astype(jnp.float32)
    stack = stacked_legendre(rowpos, total_rows)
    row = lax.broadcasted_iota(jnp.int32, (KROWS, rows), 0)
    tables = jnp.concatenate(
        [jnp.where(row < K, stack, 0.0), jnp.where((row >= K) & (row < 2 * K), stack, 0.0)], axis=1
    )
    coef = coef_ref[...].T[0:KROWS]
    curves = lax.dot_general(
        tables, coef, (((0,), (0,)), ((), ())), precision=HIGH, preferred_element_type=jnp.float32
    )
    centre = curves[0:rows]
    inverse = jnp.exp(-curves[rows : 2 * rows]) * (1.0 / base)
    amp = amp_ref[...]
    pixel = (lax.broadcasted_iota(jnp.int32, (rows, LANE), 1) % PIX).astype(jnp.float32)
    offset = pixel - (PIX - 1) / 2.0
    for tile in range(cols // LANE):
        here = slice(tile * LANE, (tile + 1) * LANE)
        scaled = (offset - per_column(centre, tile)) * per_column(inverse, tile)
        shape = jnp.exp(-0.5 * scaled * scaled)
        amp_cols = per_column(amp, tile)
        for lamp in range(lamps):
            weight = lit_ref[:, lamp * LANE : (lamp + 1) * LANE] * amp_cols[lamp : lamp + 1]
            frame = frames_ref[lamp, :, here].astype(jnp.float32)
            out_ref[lamp, :, here] = (frame - weight * shape).astype(jnp.bfloat16)


def residual(bundle_width, fiber_bundle, coef, frames, amplitude, line_start):
    lamps, rows, cols = frames.shape
    vmem = pl.BlockSpec(memory_space=pltpu.VMEM)
    smem = pl.BlockSpec(memory_space=pltpu.SMEM)
    return pl.pallas_call(
        residual_kernel,
        out_shape=jax.ShapeDtypeStruct(frames.shape, jnp.bfloat16),
        in_specs=[smem, vmem, vmem, vmem, vmem, vmem],
        out_specs=vmem,
        scratch_shapes=[pltpu.VMEM((rows, lamps * LANE), jnp.float32)],
        name="residual",
    )(bundle_width, fiber_bundle.reshape(1, -1), coef, frames, amplitude, line_start)


def body(frames, amplitude, line_start, bundle_width, fiber_bundle, trace_coef, width_coef):
    sources = lax.axis_size("fib")
    devices = lax.axis_size("rows") * sources
    rows = frames.shape[1]
    owned = trace_coef.shape[0]
    height = -(-(owned * PIX + owned) // SUB) * SUB
    partial = collapse(frames, amplitude, line_start, owned, height, devices)
    got = lax.all_to_all(partial, BOTH, 0, 0, tiled=True).reshape(devices * height, rows)
    trace_fit, width_fit, send = fit(
        got, bundle_width, fiber_bundle, trace_coef, width_coef, devices, height, sources
    )
    coef = lax.all_to_all(send, BOTH, 0, 0, tiled=True).reshape(devices * owned, LANE)
    image = residual(bundle_width, fiber_bundle, coef, frames, amplitude, line_start)
    return (trace_fit, width_fit, image)


def solution(mesh):
    return jax.shard_map(
        body,
        mesh=mesh,
        in_specs=(
            P("fib", "rows", None),
            P("fib", None),
            P("fib", None),
            P(),
            P(),
            P(BOTH, None),
            P(BOTH, None),
        ),
        out_specs=(P(BOTH, None), P(BOTH, None), P("fib", "rows", None)),
        check_vma=False,
    )
```

```python
import functools

import jax
import jax.numpy as jnp
from jax import lax
from jax.experimental import pallas as pl
from jax.experimental.pallas import tpu as pltpu
from jax.sharding import PartitionSpec as P

K = 11
PIX = 8
WIN = 8
ITERS = 3
SUB = 8
LANE = 128
KROWS = 24
RHS = 2 * K
VMEM_BYTES = 20 << 20

HIGH = lax.Precision.HIGHEST
BOTH = ("rows", "fib")


def legendre_list(rowpos, total):
    tvals = (2.0 * rowpos + 1.0) / total - 1.0
    polys = [jnp.ones_like(tvals), tvals]
    for order in range(1, K - 1):
        polys.append(
            ((2 * order + 1) * tvals * polys[order] - order * polys[order - 1]) / (order + 1)
        )
    return polys


def stacked_legendre(rowpos, total):
    polys = legendre_list(rowpos, total)
    row = lax.broadcasted_iota(jnp.int32, (KROWS, rowpos.shape[1]), 0)
    table = jnp.zeros((KROWS, rowpos.shape[1]), jnp.float32)
    for order in range(K):
        table = jnp.where((row == order) | (row == K + order), polys[order], table)
    return jnp.where(row == RHS, 1.0, table)


def lit_by_lamp(start, first, rows):
    lamps, lines = start.shape
    rowid = first + lax.broadcasted_iota(jnp.int32, (lamps, rows), 1)
    lit = jnp.zeros((lamps, rows), jnp.float32)
    for line in range(lines):
        away = rowid - start[:, line : line + 1]
        lit = jnp.where((away >= 0) & (away < WIN), 1.0, lit)
    return lit


def lit_columns(lit):
    lamps, rows = lit.shape
    which = lax.broadcasted_iota(jnp.int32, (lamps, lamps * LANE), 1) // LANE
    own = lax.broadcasted_iota(jnp.int32, (lamps, lamps * LANE), 0)
    spread = jnp.where(which == own, 1.0, 0.0)
    return lax.dot_general(
        lit, spread, (((0,), (0,)), ((), ())), preferred_element_type=jnp.float32
    )


def per_column(values, tile):
    each = LANE // PIX
    part = (tile * each) // LANE
    lane = lax.broadcasted_iota(jnp.int32, (values.shape[0], LANE), 1)
    index = (tile * each) % LANE + lane // PIX
    block = values[:, part * LANE : (part + 1) * LANE]
    return jnp.take_along_axis(block, index, axis=1, mode="promise_in_bounds")


def collapse_kernel(owned, frames_ref, amp_ref, start_ref, out_ref, lit_ref):
    lamps, rows, cols = frames_ref.shape
    first = lax.axis_index("rows") * rows
    amp = amp_ref[...]
    lit = lit_by_lamp(start_ref[...], first, rows)
    lit_ref[...] = lit_columns(lit)
    square = lax.dot_general(
        amp * amp, lit, (((0,), (0,)), ((), ())), precision=HIGH, preferred_element_type=jnp.float32
    )
    wide = owned * PIX
    for dest in range(cols // wide):
        out_ref[dest, wide : wide + owned, :] = square[dest * owned : (dest + 1) * owned]
    for tile in range(cols // LANE):
        amp_cols = per_column(amp, tile)
        total = jnp.zeros((rows, LANE), jnp.float32)
        for lamp in range(lamps):
            frame = frames_ref[lamp, :, tile * LANE : (tile + 1) * LANE].astype(jnp.float32)
            weight = lit_ref[:, lamp * LANE : (lamp + 1) * LANE] * amp_cols[lamp : lamp + 1]
            total = total + weight * frame
        flipped = total.T
        for part in range(LANE // wide):
            out_ref[tile * (LANE // wide) + part, 0:wide, :] = flipped[
                part * wide : (part + 1) * wide
            ]


def collapse(frames, amplitude, line_start, owned, height, devices):
    lamps, rows, cols = frames.shape
    return pl.pallas_call(
        functools.partial(collapse_kernel, owned),
        out_shape=jax.ShapeDtypeStruct((devices, height, rows), jnp.float32),
        in_specs=[pl.BlockSpec(memory_space=pltpu.VMEM)] * 3,
        out_specs=pl.BlockSpec(memory_space=pltpu.VMEM),
        scratch_shapes=[pltpu.VMEM((rows, lamps * LANE), jnp.float32)],
        compiler_params=pltpu.CompilerParams(vmem_limit_bytes=VMEM_BYTES),
        name="collapse",
    )(frames, amplitude, line_start)


def fit_kernel(
    height,
    sources,
    bundle_ref,
    which_ref,
    got_ref,
    trace_ref,
    width_ref,
    trace_out,
    width_out,
    send_ref,
    sum_ref,
    poly_ref,
    high_ref,
    low_ref,
    weight_ref,
    coef_ref,
    splat_ref,
    square_ref,
):
    owned = trace_ref.shape[0]
    wide = owned * PIX
    steps = got_ref.shape[0] // (height * sources)
    rows = got_ref.shape[1]
    total_rows = steps * rows
    used = wide + owned
    me = lax.axis_index("rows") * sources + lax.axis_index("fib")

    for group in range(steps // SUB):
        for item in range(used):
            value = None
            for source in range(sources):
                start = (group * SUB * sources + source) * height + item
                part = got_ref[pl.ds(start, SUB, stride=sources * height), :]
                value = part if value is None else value + part
            sum_ref[item, group * SUB : (group + 1) * SUB, :] = value

    rowpos = (
        lax.broadcasted_iota(jnp.int32, (steps, rows), 0) * rows
        + lax.broadcasted_iota(jnp.int32, (steps, rows), 1)
    ).astype(jnp.float32)
    polys = legendre_list(rowpos, total_rows)
    for order in range(K):
        poly_ref[order * steps : (order + 1) * steps, :] = polys[order]
        poly_ref[(K + order) * steps : (K + order + 1) * steps, :] = polys[order]
    poly_ref[RHS * steps : (RHS + 1) * steps, :] = jnp.ones((steps, rows), jnp.float32)
    poly_ref[(RHS + 1) * steps :, :] = jnp.zeros((steps, rows), jnp.float32)
    for step in range(steps):
        stack = poly_ref[pl.ds(step, KROWS, stride=steps), :]
        pairs = jnp.concatenate([stack * stack[i : i + 1] for i in range(K)], axis=0)
        high = pairs.astype(jnp.bfloat16)
        high_ref[:, step * rows : (step + 1) * rows] = high
        low_ref[:, step * rows : (step + 1) * rows] = (pairs - high.astype(jnp.float32)).astype(
            jnp.bfloat16
        )

    square_ref[...] = jnp.zeros_like(square_ref)
    square_ref[0:owned, 0:K] = trace_ref[...]
    square_ref[0:owned, K : 2 * K] = width_ref[...]
    coef_ref[...] = square_ref[...].T[0:KROWS]
    weight_ref[...] = jnp.zeros_like(weight_ref)

    inverse_base = []
    for fiber in range(owned):
        base = bundle_ref[which_ref[me * owned + fiber]]
        inverse_base.append(1.0 / jnp.full((1, rows), base, jnp.float32))

    def newton_step(index, carry):
        for fiber in range(owned):
            splat_ref[fiber] = jnp.broadcast_to(
                coef_ref[:, fiber : fiber + 1], (KROWS, rows)
            )
        for group in range(steps // SUB):
            here = slice(group * SUB, (group + 1) * SUB)
            for fiber in range(owned):
                centre = jnp.zeros((SUB, rows), jnp.float32)
                spread = jnp.zeros((SUB, rows), jnp.float32)
                for order in range(K):
                    poly = poly_ref[order * steps + group * SUB : order * steps + (group + 1) * SUB, :]
                    centre = centre + splat_ref[fiber, order : order + 1, :] * poly
                    spread = spread + splat_ref[fiber, K + order : K + order + 1, :] * poly
                inverse = jnp.exp(-spread) * inverse_base[fiber]
                power = sum_ref[wide + fiber, here, :]
                sums = [jnp.zeros((SUB, rows), jnp.float32) for _ in range(5)]
                for pixel in range(PIX):
                    scaled = ((pixel - (PIX - 1) / 2.0) - centre) * inverse
                    shape = jnp.exp(-0.5 * scaled * scaled)
                    bend = shape * scaled
                    slope = bend * inverse
                    widen = bend * scaled
                    resid = sum_ref[fiber * PIX + pixel, here, :] - power * shape
                    sums[0] = sums[0] + slope * slope
                    sums[1] = sums[1] + slope * widen
                    sums[2] = sums[2] + widen * widen
                    sums[3] = sums[3] + resid * slope
                    sums[4] = sums[4] + resid * widen
                for kind in range(5):
                    value = sums[kind] * power if kind < 3 else sums[kind]
                    at = (kind * owned + fiber) * steps + group * SUB
                    weight_ref[at : at + SUB, :] = value
        count = weight_ref.shape[0] // steps
        weights = jnp.concatenate(
            [weight_ref[pl.ds(step, count, stride=steps), :] for step in range(steps)], axis=1
        )
        upper = weights.astype(jnp.bfloat16).astype(jnp.float32)
        both = jnp.concatenate([upper, weights - upper], axis=0).astype(jnp.bfloat16)
        dims = (((1,), (1,)), ((), ()))
        moments = lax.dot_general(
            high_ref[...], both, dims, preferred_element_type=jnp.float32
        ) + lax.dot_general(low_ref[...], both, dims, preferred_element_type=jnp.float32)
        lanes = moments.shape[1]
        moments = jnp.concatenate(
            [moments, jnp.zeros((moments.shape[0], LANE - lanes), jnp.float32)], axis=1
        )
        moments = moments + pltpu.roll(moments, LANE - count, 1)
        aligned = [moments] + [
            pltpu.roll(moments, LANE - kind * owned, 1) for kind in range(1, 5)
        ]
        row = lax.broadcasted_iota(jnp.int32, (KROWS, LANE), 0)

        def matrix_row(i, second):
            block = [item[i * KROWS : (i + 1) * KROWS] for item in aligned]
            left, right, side = (block[1], block[2], block[4]) if second else (
                block[0],
                block[1],
                block[3],
            )
            value = jnp.where(row < K, left, jnp.where(row < 2 * K, right, side))
            at = i + K if second else i
            return jnp.where(row == at, 1.5 * value + 1.0, value)

        matrix = [matrix_row(i, False) for i in range(K)] + [matrix_row(i, True) for i in range(K)]
        for pivot in range(2 * K):
            cut = KROWS - matrix[pivot].shape[0]
            inverse = 1.0 / matrix[pivot][pivot - cut : pivot - cut + 1]
            chosen = matrix[pivot] * inverse
            for i in range(2 * K):
                if i != pivot:
                    scale = matrix[i][pivot - cut : pivot - cut + 1]
                    matrix[i] = matrix[i] - scale * chosen
            matrix[pivot] = chosen
            if (pivot + 1) % SUB == 0:
                matrix = [item[SUB:] for item in matrix]
        for i in range(2 * K):
            cut = KROWS - matrix[i].shape[0]
            coef_ref[i : i + 1, :] = coef_ref[i : i + 1, :] + matrix[i][RHS - cut : RHS - cut + 1]
        return carry

    lax.fori_loop(0, ITERS, newton_step, 0)

    square_ref[...] = jnp.zeros_like(square_ref)
    lane = lax.broadcasted_iota(jnp.int32, (KROWS, LANE), 1)
    square_ref[0:KROWS, :] = jnp.where(lane < owned, coef_ref[...], 0.0)
    result = square_ref[...].T[0:owned]
    trace_out[...] = result[:, 0:K]
    width_out[...] = result[:, K : 2 * K]
    for device in range(send_ref.shape[0]):
        send_ref[device] = result


def fit(got, bundle_width, fiber_bundle, trace_coef, width_coef, devices, height, sources):
    owned = trace_coef.shape[0]
    rows = got.shape[1]
    steps = devices // sources
    count = -(-5 * owned // SUB) * SUB
    vmem = pl.BlockSpec(memory_space=pltpu.VMEM)
    smem = pl.BlockSpec(memory_space=pltpu.SMEM)
    return pl.pallas_call(
        functools.partial(fit_kernel, height, sources),
        out_shape=(
            jax.ShapeDtypeStruct((owned, K), jnp.float32),
            jax.ShapeDtypeStruct((owned, K), jnp.float32),
            jax.ShapeDtypeStruct((devices, owned, LANE), jnp.float32),
        ),
        in_specs=[smem, smem, vmem, vmem, vmem],
        out_specs=(vmem, vmem, vmem),
        scratch_shapes=[
            pltpu.VMEM((owned * PIX + owned, steps, rows), jnp.float32),
            pltpu.VMEM((KROWS * steps, rows), jnp.float32),
            pltpu.VMEM((K * KROWS, steps * rows), jnp.bfloat16),
            pltpu.VMEM((K * KROWS, steps * rows), jnp.bfloat16),
            pltpu.VMEM((count * steps, rows), jnp.float32),
            pltpu.VMEM((KROWS, LANE), jnp.float32),
            pltpu.VMEM((owned, KROWS, rows), jnp.float32),
            pltpu.VMEM((LANE, LANE), jnp.float32),
        ],
        compiler_params=pltpu.CompilerParams(vmem_limit_bytes=VMEM_BYTES),
        name="fit",
    )(bundle_width, fiber_bundle, got, trace_coef, width_coef)


def residual_kernel(
    bundle_ref, which_ref, coef_ref, frames_ref, amp_ref, start_ref, out_ref, lit_ref
):
    lamps, rows, cols = frames_ref.shape
    total_rows = rows * lax.axis_size("rows")
    fibers = coef_ref.shape[0]
    first = lax.axis_index("rows") * rows
    lit_ref[...] = lit_columns(lit_by_lamp(start_ref[...], first, rows))
    which = which_ref[...]
    base = jnp.zeros((1, fibers), jnp.float32)
    for bundle in range(bundle_ref.shape[0]):
        base = jnp.where(which == bundle, bundle_ref[bundle], base)

    rowpos = (first + lax.broadcasted_iota(jnp.int32, (1, rows), 1)).astype(jnp.float32)
    stack = stacked_legendre(rowpos, total_rows)
    row = lax.broadcasted_iota(jnp.int32, (KROWS, rows), 0)
    tables = jnp.concatenate(
        [jnp.where(row < K, stack, 0.0), jnp.where((row >= K) & (row < 2 * K), stack, 0.0)], axis=1
    )
    coef = coef_ref[...].T[0:KROWS]
    curves = lax.dot_general(
        tables, coef, (((0,), (0,)), ((), ())), precision=HIGH, preferred_element_type=jnp.float32
    )
    centre = curves[0:rows]
    inverse = jnp.exp(-curves[rows : 2 * rows]) * (1.0 / base)
    amp = amp_ref[...]
    pixel = (lax.broadcasted_iota(jnp.int32, (rows, LANE), 1) % PIX).astype(jnp.float32)
    offset = pixel - (PIX - 1) / 2.0
    for tile in range(cols // LANE):
        here = slice(tile * LANE, (tile + 1) * LANE)
        scaled = (offset - per_column(centre, tile)) * per_column(inverse, tile)
        shape = jnp.exp(-0.5 * scaled * scaled)
        amp_cols = per_column(amp, tile)
        for lamp in range(lamps):
            weight = lit_ref[:, lamp * LANE : (lamp + 1) * LANE] * amp_cols[lamp : lamp + 1]
            frame = frames_ref[lamp, :, here].astype(jnp.float32)
            out_ref[lamp, :, here] = (frame - weight * shape).astype(jnp.bfloat16)


def residual(bundle_width, fiber_bundle, coef, frames, amplitude, line_start):
    lamps, rows, cols = frames.shape
    vmem = pl.BlockSpec(memory_space=pltpu.VMEM)
    smem = pl.BlockSpec(memory_space=pltpu.SMEM)
    return pl.pallas_call(
        residual_kernel,
        out_shape=jax.ShapeDtypeStruct(frames.shape, jnp.bfloat16),
        in_specs=[smem, vmem, vmem, vmem, vmem, vmem],
        out_specs=vmem,
        scratch_shapes=[pltpu.VMEM((rows, lamps * LANE), jnp.float32)],
        compiler_params=pltpu.CompilerParams(vmem_limit_bytes=VMEM_BYTES),
        name="residual",
    )(bundle_width, fiber_bundle.reshape(1, -1), coef, frames, amplitude, line_start)


def body(frames, amplitude, line_start, bundle_width, fiber_bundle, trace_coef, width_coef):
    sources = lax.axis_size("fib")
    devices = lax.axis_size("rows") * sources
    rows = frames.shape[1]
    owned = trace_coef.shape[0]
    height = -(-(owned * PIX + owned) // SUB) * SUB
    partial = collapse(frames, amplitude, line_start, owned, height, devices)
    got = lax.all_to_all(partial, BOTH, 0, 0, tiled=True).reshape(devices * height, rows)
    trace_fit, width_fit, send = fit(
        got, bundle_width, fiber_bundle, trace_coef, width_coef, devices, height, sources
    )
    coef = lax.all_to_all(send, BOTH, 0, 0, tiled=True).reshape(devices * owned, LANE)
    image = residual(bundle_width, fiber_bundle, coef, frames, amplitude, line_start)
    return (trace_fit, width_fit, image)


def solution(mesh):
    return jax.shard_map(
        body,
        mesh=mesh,
        in_specs=(
            P("fib", "rows", None),
            P("fib", None),
            P("fib", None),
            P(),
            P(),
            P(BOTH, None),
            P(BOTH, None),
        ),
        out_specs=(P(BOTH, None), P(BOTH, None), P("fib", "rows", None)),
        check_vma=False,
    )
```

```python
import functools

import jax
import jax.numpy as jnp
from jax import lax
from jax.experimental import pallas as pl
from jax.experimental.pallas import tpu as pltpu
from jax.sharding import PartitionSpec as P

K = 11
PIX = 8
WIN = 8
ITERS = 3
SUB = 8
LANE = 128
KROWS = 24
RHS = 2 * K
VMEM_BYTES = 20 << 20
CHUNK = 256

HIGH = lax.Precision.HIGHEST
BOTH = ("rows", "fib")


def legendre_list(rowpos, total):
    tvals = (2.0 * rowpos + 1.0) / total - 1.0
    polys = [jnp.ones_like(tvals), tvals]
    for order in range(1, K - 1):
        polys.append(
            ((2 * order + 1) * tvals * polys[order] - order * polys[order - 1]) / (order + 1)
        )
    return polys


def stacked_legendre(rowpos, total):
    polys = legendre_list(rowpos, total)
    row = lax.broadcasted_iota(jnp.int32, (KROWS, rowpos.shape[1]), 0)
    table = jnp.zeros((KROWS, rowpos.shape[1]), jnp.float32)
    for order in range(K):
        table = jnp.where((row == order) | (row == K + order), polys[order], table)
    return jnp.where(row == RHS, 1.0, table)


def lit_by_lamp(start, first, rows):
    lamps, lines = start.shape
    rowid = first + lax.broadcasted_iota(jnp.int32, (lamps, rows), 1)
    lit = jnp.zeros((lamps, rows), jnp.float32)
    for line in range(lines):
        away = rowid - start[:, line : line + 1]
        lit = jnp.where((away >= 0) & (away < WIN), 1.0, lit)
    return lit


def lit_columns(lit):
    lamps, rows = lit.shape
    which = lax.broadcasted_iota(jnp.int32, (lamps, lamps * LANE), 1) // LANE
    own = lax.broadcasted_iota(jnp.int32, (lamps, lamps * LANE), 0)
    spread = jnp.where(which == own, 1.0, 0.0)
    return lax.dot_general(
        lit, spread, (((0,), (0,)), ((), ())), preferred_element_type=jnp.float32
    )


def per_column(values, tile):
    each = LANE // PIX
    part = (tile * each) // LANE
    lane = lax.broadcasted_iota(jnp.int32, (values.shape[0], LANE), 1)
    index = (tile * each) % LANE + lane // PIX
    block = values[:, part * LANE : (part + 1) * LANE]
    return jnp.take_along_axis(block, index, axis=1, mode="promise_in_bounds")


def start_copies(sources, targets, sems):
    copies = [
        pltpu.make_async_copy(source, target, sems.at[index])
        for index, (source, target) in enumerate(zip(sources, targets))
    ]
    for copy in copies:
        copy.start()
    return copies


def collapse_kernel(
    frames_hbm,
    amp_hbm,
    start_hbm,
    bundle_hbm,
    which_hbm,
    trace_hbm,
    width_hbm,
    keep_ref,
    send_ref,
    lit_ref,
    table_ref,
    base_ref,
    own_base_ref,
    coef_ref,
    poly_ref,
    high_ref,
    low_ref,
    frames_ref,
    amp_ref,
    start_ref,
    bundle_ref,
    which_ref,
    trace_ref,
    width_ref,
    square_ref,
    small_sems,
    frame_sems,
):
    lamps, rows, cols = frames_ref.shape
    owned = trace_ref.shape[0]
    fibers = which_ref.shape[1]
    steps = lax.axis_size("rows")
    total_rows = steps * rows
    me = lax.axis_index("rows") * lax.axis_size("fib") + lax.axis_index("fib")
    first = lax.axis_index("rows") * rows
    odd = lax.axis_index("fib") % 2 == 1

    small = start_copies(
        [amp_hbm, start_hbm, bundle_hbm, which_hbm, trace_hbm, width_hbm],
        [amp_ref, start_ref, bundle_ref, which_ref, trace_ref, width_ref],
        small_sems,
    )
    chunk = min(CHUNK, cols)
    spans = [slice(at, at + chunk) for at in range(0, cols, chunk)]
    arriving = start_copies(
        [frames_hbm.at[:, :, span] for span in spans],
        [frames_ref.at[:, :, span] for span in spans],
        frame_sems,
    )

    rowpos = (
        lax.broadcasted_iota(jnp.int32, (steps, rows), 0) * rows
        + lax.broadcasted_iota(jnp.int32, (steps, rows), 1)
    ).astype(jnp.float32)
    polys = legendre_list(rowpos, total_rows)
    for order in range(K):
        poly_ref[order * steps : (order + 1) * steps, :] = polys[order]
        poly_ref[(K + order) * steps : (K + order + 1) * steps, :] = polys[order]
    poly_ref[RHS * steps : (RHS + 1) * steps, :] = jnp.ones((steps, rows), jnp.float32)
    poly_ref[(RHS + 1) * steps :, :] = jnp.zeros((steps, rows), jnp.float32)
    for step in range(steps):
        stack = poly_ref[pl.ds(step, KROWS, stride=steps), :]
        pairs = jnp.concatenate([stack * stack[i : i + 1] for i in range(K)], axis=0)
        high = pairs.astype(jnp.bfloat16)
        high_ref[:, step * rows : (step + 1) * rows] = high
        low_ref[:, step * rows : (step + 1) * rows] = (pairs - high.astype(jnp.float32)).astype(
            jnp.bfloat16
        )
    here = (first + lax.broadcasted_iota(jnp.int32, (1, rows), 1)).astype(jnp.float32)
    stack = stacked_legendre(here, total_rows)
    row = lax.broadcasted_iota(jnp.int32, (KROWS, rows), 0)
    table_ref[:, 0:rows] = jnp.where(row < K, stack, 0.0)
    table_ref[:, rows : 2 * rows] = jnp.where((row >= K) & (row < 2 * K), stack, 0.0)

    for copy in small:
        copy.wait()
    amp = amp_ref[...]
    lit = lit_by_lamp(start_ref[...], first, rows)
    lit_ref[...] = lit_columns(lit)
    which = which_ref[...]
    bundles = bundle_ref[...]
    base = jnp.zeros((1, fibers), jnp.float32)
    for bundle in range(bundles.shape[1]):
        base = jnp.where(which == bundle, bundles[:, bundle : bundle + 1], base)
    inverse = 1.0 / base
    base_ref[...] = inverse
    lane = lax.broadcasted_iota(jnp.int32, (1, fibers), 1)
    for fiber in range(owned):
        own = jnp.sum(jnp.where(lane == me * owned + fiber, inverse, 0.0), axis=1, keepdims=True)
        own_base_ref[fiber : fiber + 1, :] = jnp.broadcast_to(own, (1, rows))

    square_ref[...] = jnp.zeros_like(square_ref)
    square_ref[0:owned, 0:K] = trace_ref[...]
    square_ref[0:owned, K : 2 * K] = width_ref[...]
    coef_ref[...] = square_ref[...].T[0:KROWS]

    square = lax.dot_general(
        amp * amp, lit, (((0,), (0,)), ((), ())), precision=HIGH, preferred_element_type=jnp.float32
    )
    wide = owned * PIX

    def place(block, at, even_value, odd_value):
        keep_ref[block, at, :] = jnp.where(odd, odd_value, even_value)
        send_ref[block, at, :] = jnp.where(odd, even_value, odd_value)

    for block in range(fibers // (2 * owned)):
        low = 2 * block * owned
        place(
            block,
            slice(wide, wide + owned),
            square[low : low + owned],
            square[low + owned : low + 2 * owned],
        )
    for tile in range(cols // LANE):
        if (tile * LANE) % chunk == 0:
            arriving[tile * LANE // chunk].wait()
        amp_cols = per_column(amp, tile)
        total = jnp.zeros((rows, LANE), jnp.float32)
        for lamp in range(lamps):
            frame = frames_ref[lamp, :, tile * LANE : (tile + 1) * LANE].astype(jnp.float32)
            weight = lit_ref[:, lamp * LANE : (lamp + 1) * LANE] * amp_cols[lamp : lamp + 1]
            total = total + weight * frame
        flipped = total.T
        for pair in range(LANE // (2 * wide)):
            low = 2 * pair * wide
            place(
                tile * (LANE // (2 * wide)) + pair,
                slice(0, wide),
                flipped[low : low + wide],
                flipped[low + wide : low + 2 * wide],
            )


def collapse(
    frames, amplitude, line_start, bundle_width, fiber_bundle, trace_coef, width_coef, height
):
    lamps, rows, cols = frames.shape
    owned = trace_coef.shape[0]
    steps = lax.axis_size("rows")
    blocks = steps * lax.axis_size("fib") // 2
    args = (
        frames,
        amplitude,
        line_start,
        bundle_width.reshape(1, -1),
        fiber_bundle.reshape(1, -1),
        trace_coef,
        width_coef,
    )
    shape = jax.ShapeDtypeStruct
    outs = (
        shape((blocks, height, rows), jnp.float32),
        shape((blocks, height, rows), jnp.float32),
        shape((rows, lamps * LANE), jnp.float32),
        shape((KROWS, 2 * rows), jnp.float32),
        shape((1, fiber_bundle.shape[0]), jnp.float32),
        shape((owned, rows), jnp.float32),
        shape((KROWS, LANE), jnp.float32),
        shape((KROWS * steps, rows), jnp.float32),
        shape((K * KROWS, steps * rows), jnp.bfloat16),
        shape((K * KROWS, steps * rows), jnp.bfloat16),
    )
    return pl.pallas_call(
        collapse_kernel,
        out_shape=outs,
        in_specs=[pl.BlockSpec(memory_space=pltpu.HBM)] * len(args),
        out_specs=[pl.BlockSpec(memory_space=pltpu.VMEM)] * len(outs),
        scratch_shapes=[pltpu.VMEM(arg.shape, arg.dtype) for arg in args]
        + [
            pltpu.VMEM((LANE, LANE), jnp.float32),
            pltpu.SemaphoreType.DMA((len(args) - 1,)),
            pltpu.SemaphoreType.DMA((cols // min(CHUNK, cols),)),
        ],
        compiler_params=pltpu.CompilerParams(vmem_limit_bytes=VMEM_BYTES),
        name="collapse",
    )(*args)


def fit_kernel(
    height,
    sources,
    owned,
    got_ref,
    start_ref,
    base_ref,
    poly_ref,
    high_ref,
    low_ref,
    send_ref,
    sum_ref,
    weight_ref,
    coef_ref,
    splat_ref,
    square_ref,
):
    wide = owned * PIX
    steps = got_ref.shape[0] // (height * sources)
    rows = got_ref.shape[1]
    used = wide + owned

    for group in range(steps // SUB):
        for item in range(used):
            value = None
            for source in range(sources):
                start = (group * SUB * sources + source) * height + item
                part = got_ref[pl.ds(start, SUB, stride=sources * height), :]
                value = part if value is None else value + part
            sum_ref[item, group * SUB : (group + 1) * SUB, :] = value

    coef_ref[...] = start_ref[...]
    inverse_base = [base_ref[fiber : fiber + 1, :] for fiber in range(owned)]
    weight_ref[...] = jnp.zeros_like(weight_ref)

    def newton_step(index, carry):
        for fiber in range(owned):
            splat_ref[fiber] = jnp.broadcast_to(
                coef_ref[:, fiber : fiber + 1], (KROWS, rows)
            )
        for group in range(steps // SUB):
            here = slice(group * SUB, (group + 1) * SUB)
            for fiber in range(owned):
                centre = jnp.zeros((SUB, rows), jnp.float32)
                spread = jnp.zeros((SUB, rows), jnp.float32)
                for order in range(K):
                    poly = poly_ref[order * steps + group * SUB : order * steps + (group + 1) * SUB, :]
                    centre = centre + splat_ref[fiber, order : order + 1, :] * poly
                    spread = spread + splat_ref[fiber, K + order : K + order + 1, :] * poly
                inverse = jnp.exp(-spread) * inverse_base[fiber]
                power = sum_ref[wide + fiber, here, :]
                sums = [jnp.zeros((SUB, rows), jnp.float32) for _ in range(5)]
                for pixel in range(PIX):
                    scaled = ((pixel - (PIX - 1) / 2.0) - centre) * inverse
                    shape = jnp.exp(-0.5 * scaled * scaled)
                    bend = shape * scaled
                    slope = bend * inverse
                    widen = bend * scaled
                    resid = sum_ref[fiber * PIX + pixel, here, :] - power * shape
                    sums[0] = sums[0] + slope * slope
                    sums[1] = sums[1] + slope * widen
                    sums[2] = sums[2] + widen * widen
                    sums[3] = sums[3] + resid * slope
                    sums[4] = sums[4] + resid * widen
                for kind in range(5):
                    value = sums[kind] * power if kind < 3 else sums[kind]
                    at = (kind * owned + fiber) * steps + group * SUB
                    weight_ref[at : at + SUB, :] = value
        count = weight_ref.shape[0] // steps
        weights = jnp.concatenate(
            [weight_ref[pl.ds(step, count, stride=steps), :] for step in range(steps)], axis=1
        )
        upper = weights.astype(jnp.bfloat16).astype(jnp.float32)
        both = jnp.concatenate([upper, weights - upper], axis=0).astype(jnp.bfloat16)
        dims = (((1,), (1,)), ((), ()))
        moments = lax.dot_general(
            high_ref[...], both, dims, preferred_element_type=jnp.float32
        ) + lax.dot_general(low_ref[...], both, dims, preferred_element_type=jnp.float32)
        lanes = moments.shape[1]
        moments = jnp.concatenate(
            [moments, jnp.zeros((moments.shape[0], LANE - lanes), jnp.float32)], axis=1
        )
        moments = moments + pltpu.roll(moments, LANE - count, 1)
        aligned = [moments] + [
            pltpu.roll(moments, LANE - kind * owned, 1) for kind in range(1, 5)
        ]
        row = lax.broadcasted_iota(jnp.int32, (KROWS, LANE), 0)

        def matrix_row(i, second):
            block = [item[i * KROWS : (i + 1) * KROWS] for item in aligned]
            left, right, side = (block[1], block[2], block[4]) if second else (
                block[0],
                block[1],
                block[3],
            )
            value = jnp.where(row < K, left, jnp.where(row < 2 * K, right, side))
            at = i + K if second else i
            return jnp.where(row == at, 1.5 * value + 1.0, value)

        matrix = [matrix_row(i, False) for i in range(K)] + [matrix_row(i, True) for i in range(K)]
        for pivot in range(2 * K):
            cut = KROWS - matrix[pivot].shape[0]
            inverse = 1.0 / matrix[pivot][pivot - cut : pivot - cut + 1]
            chosen = matrix[pivot] * inverse
            for i in range(2 * K):
                if i != pivot:
                    scale = matrix[i][pivot - cut : pivot - cut + 1]
                    matrix[i] = matrix[i] - scale * chosen
            matrix[pivot] = chosen
            if (pivot + 1) % SUB == 0:
                matrix = [item[SUB:] for item in matrix]
        for i in range(2 * K):
            cut = KROWS - matrix[i].shape[0]
            coef_ref[i : i + 1, :] = coef_ref[i : i + 1, :] + matrix[i][RHS - cut : RHS - cut + 1]
        return carry

    lax.fori_loop(0, ITERS, newton_step, 0)

    square_ref[...] = jnp.zeros_like(square_ref)
    lane = lax.broadcasted_iota(jnp.int32, (KROWS, LANE), 1)
    square_ref[0:KROWS, :] = jnp.where(lane < owned, coef_ref[...], 0.0)
    result = square_ref[...].T[0:owned]
    for device in range(send_ref.shape[0]):
        send_ref[device] = result


def fit(got, start, base, poly, high, low, devices, height, sources):
    owned, rows = base.shape
    steps = got.shape[0] // (height * sources)
    count = -(-5 * owned // SUB) * SUB
    vmem = pl.BlockSpec(memory_space=pltpu.VMEM)
    return pl.pallas_call(
        functools.partial(fit_kernel, height, sources, owned),
        out_shape=jax.ShapeDtypeStruct((devices, owned, LANE), jnp.float32),
        in_specs=[vmem] * 6,
        out_specs=vmem,
        scratch_shapes=[
            pltpu.VMEM((owned * PIX + owned, steps, rows), jnp.float32),
            pltpu.VMEM((count * steps, rows), jnp.float32),
            pltpu.VMEM((KROWS, LANE), jnp.float32),
            pltpu.VMEM((owned, KROWS, rows), jnp.float32),
            pltpu.VMEM((LANE, LANE), jnp.float32),
        ],
        compiler_params=pltpu.CompilerParams(vmem_limit_bytes=VMEM_BYTES),
        name="fit",
    )(got, start, base, poly, high, low)


def residual_kernel(
    owned,
    coef_ref,
    table_ref,
    base_ref,
    lit_ref,
    amp_ref,
    frames_ref,
    trace_hbm,
    width_hbm,
    image_hbm,
    trace_ref,
    width_ref,
    image_ref,
    small_sems,
    image_sems,
):
    lamps, rows, cols = frames_ref.shape
    me = lax.axis_index("rows") * lax.axis_size("fib") + lax.axis_index("fib")
    own = coef_ref[pl.ds(me * owned, owned), :]
    trace_ref[...] = own[:, 0:K]
    width_ref[...] = own[:, K : 2 * K]
    leaving = start_copies([trace_ref, width_ref], [trace_hbm, width_hbm], small_sems)

    coef = coef_ref[...].T[0:KROWS]
    curves = lax.dot_general(
        table_ref[...],
        coef,
        (((0,), (0,)), ((), ())),
        precision=HIGH,
        preferred_element_type=jnp.float32,
    )
    centre = curves[0:rows]
    inverse = jnp.exp(-curves[rows : 2 * rows]) * base_ref[...]
    amp = amp_ref[...]
    pixel = (lax.broadcasted_iota(jnp.int32, (rows, LANE), 1) % PIX).astype(jnp.float32)
    offset = pixel - (PIX - 1) / 2.0
    chunk = min(CHUNK, cols)
    for tile in range(cols // LANE):
        here = slice(tile * LANE, (tile + 1) * LANE)
        scaled = (offset - per_column(centre, tile)) * per_column(inverse, tile)
        shape = jnp.exp(-0.5 * scaled * scaled)
        amp_cols = per_column(amp, tile)
        for lamp in range(lamps):
            weight = lit_ref[:, lamp * LANE : (lamp + 1) * LANE] * amp_cols[lamp : lamp + 1]
            frame = frames_ref[lamp, :, here].astype(jnp.float32)
            image_ref[lamp, :, here] = (frame - weight * shape).astype(jnp.bfloat16)
        if ((tile + 1) * LANE) % chunk == 0:
            span = slice((tile + 1) * LANE - chunk, (tile + 1) * LANE)
            copy = pltpu.make_async_copy(
                image_ref.at[:, :, span],
                image_hbm.at[:, :, span],
                image_sems.at[tile * LANE // chunk],
            )
            copy.start()
            leaving.append(copy)
    for copy in leaving:
        copy.wait()


def residual(owned, coef, table, base, lit, amplitude, frames):
    cols = frames.shape[2]
    vmem = pl.BlockSpec(memory_space=pltpu.VMEM)
    hbm = pl.BlockSpec(memory_space=pltpu.HBM)
    fitted = jax.ShapeDtypeStruct((owned, K), jnp.float32)
    return pl.pallas_call(
        functools.partial(residual_kernel, owned),
        out_shape=(fitted, fitted, jax.ShapeDtypeStruct(frames.shape, jnp.bfloat16)),
        in_specs=[vmem] * 6,
        out_specs=[hbm] * 3,
        scratch_shapes=[
            pltpu.VMEM((owned, K), jnp.float32),
            pltpu.VMEM((owned, K), jnp.float32),
            pltpu.VMEM(frames.shape, jnp.bfloat16),
            pltpu.SemaphoreType.DMA((2,)),
            pltpu.SemaphoreType.DMA((cols // min(CHUNK, cols),)),
        ],
        compiler_params=pltpu.CompilerParams(vmem_limit_bytes=VMEM_BYTES),
        name="residual",
    )(coef, table, base, lit, amplitude, frames)


def body(frames, amplitude, line_start, bundle_width, fiber_bundle, trace_coef, width_coef):
    sources = lax.axis_size("fib")
    devices = lax.axis_size("rows") * sources
    rows = frames.shape[1]
    owned = trace_coef.shape[0]
    height = -(-(owned * PIX + owned) // SUB) * SUB
    keep, send, lit, table, base, own_base, start, poly, high, low = collapse(
        frames, amplitude, line_start, bundle_width, fiber_bundle, trace_coef, width_coef, height
    )
    came = lax.ppermute(send, "fib", [(index, index ^ 1) for index in range(sources)])
    alike = [[index for index in range(devices) if index % 2 == odd] for odd in range(2)]
    got = lax.all_to_all(keep + came, BOTH, 0, 0, axis_index_groups=alike, tiled=True)
    got = got.reshape(devices // 2 * height, rows)
    reply = fit(got, start, own_base, poly, high, low, devices, height, sources // 2)
    coef = lax.all_to_all(reply, BOTH, 0, 0, tiled=True).reshape(devices * owned, LANE)
    return residual(owned, coef, table, base, lit, amplitude, frames)


def solution(mesh):
    return jax.shard_map(
        body,
        mesh=mesh,
        in_specs=(
            P("fib", "rows", None),
            P("fib", None),
            P("fib", None),
            P(),
            P(),
            P(BOTH, None),
            P(BOTH, None),
        ),
        out_specs=(P(BOTH, None), P(BOTH, None), P("fib", "rows", None)),
        check_vma=False,
    )
```

```python
import functools

import jax
import jax.numpy as jnp
from jax import lax
from jax.experimental import pallas as pl
from jax.experimental.pallas import tpu as pltpu
from jax.sharding import PartitionSpec as P

K = 11
PIX = 8
WIN = 8
ITERS = 3
SUB = 8
LANE = 128
KROWS = 24
RHS = 2 * K
VMEM_BYTES = 20 << 20
CHUNK = 256

HIGH = lax.Precision.HIGHEST
BOTH = ("rows", "fib")


def legendre_list(rowpos, total):
    tvals = (2.0 * rowpos + 1.0) / total - 1.0
    polys = [jnp.ones_like(tvals), tvals]
    for order in range(1, K - 1):
        polys.append(
            ((2 * order + 1) * tvals * polys[order] - order * polys[order - 1]) / (order + 1)
        )
    return polys


def stacked_legendre(rowpos, total):
    polys = legendre_list(rowpos, total)
    row = lax.broadcasted_iota(jnp.int32, (KROWS, rowpos.shape[1]), 0)
    table = jnp.zeros((KROWS, rowpos.shape[1]), jnp.float32)
    for order in range(K):
        table = jnp.where((row == order) | (row == K + order), polys[order], table)
    return jnp.where(row == RHS, 1.0, table)


def lit_by_lamp(start, first, rows):
    lamps, lines = start.shape
    rowid = first + lax.broadcasted_iota(jnp.int32, (lamps, rows), 1)
    lit = jnp.zeros((lamps, rows), jnp.float32)
    for line in range(lines):
        away = rowid - start[:, line : line + 1]
        lit = jnp.where((away >= 0) & (away < WIN), 1.0, lit)
    return lit


def lit_columns(lit):
    lamps, rows = lit.shape
    which = lax.broadcasted_iota(jnp.int32, (lamps, lamps * LANE), 1) // LANE
    own = lax.broadcasted_iota(jnp.int32, (lamps, lamps * LANE), 0)
    spread = jnp.where(which == own, 1.0, 0.0)
    return lax.dot_general(
        lit, spread, (((0,), (0,)), ((), ())), preferred_element_type=jnp.float32
    )


def per_column(values, tile):
    each = LANE // PIX
    part = (tile * each) // LANE
    lane = lax.broadcasted_iota(jnp.int32, (values.shape[0], LANE), 1)
    index = (tile * each) % LANE + lane // PIX
    block = values[:, part * LANE : (part + 1) * LANE]
    return jnp.take_along_axis(block, index, axis=1, mode="promise_in_bounds")


def start_copies(sources, targets, sems):
    copies = [
        pltpu.make_async_copy(source, target, sems.at[index])
        for index, (source, target) in enumerate(zip(sources, targets))
    ]
    for copy in copies:
        copy.start()
    return copies


def collapse_kernel(
    frames_hbm,
    amp_hbm,
    start_hbm,
    bundle_hbm,
    which_hbm,
    trace_hbm,
    width_hbm,
    keep_ref,
    send_ref,
    lit_ref,
    table_ref,
    base_ref,
    own_base_ref,
    coef_ref,
    poly_ref,
    high_ref,
    low_ref,
    frames_ref,
    amp_ref,
    start_ref,
    bundle_ref,
    which_ref,
    trace_ref,
    width_ref,
    square_ref,
    small_sems,
    frame_sems,
):
    lamps, rows, cols = frames_ref.shape
    owned = trace_ref.shape[0]
    fibers = which_ref.shape[1]
    steps = lax.axis_size("rows")
    total_rows = steps * rows
    me = lax.axis_index("rows") * lax.axis_size("fib") + lax.axis_index("fib")
    first = lax.axis_index("rows") * rows
    odd = lax.axis_index("fib") % 2 == 1

    small = start_copies(
        [amp_hbm, start_hbm, bundle_hbm, which_hbm, trace_hbm, width_hbm],
        [amp_ref, start_ref, bundle_ref, which_ref, trace_ref, width_ref],
        small_sems,
    )
    chunk = min(CHUNK, cols)
    spans = [slice(at, at + chunk) for at in range(0, cols, chunk)]
    arriving = start_copies(
        [frames_hbm.at[:, :, span] for span in spans],
        [frames_ref.at[:, :, span] for span in spans],
        frame_sems,
    )

    rowpos = (
        lax.broadcasted_iota(jnp.int32, (steps, rows), 0) * rows
        + lax.broadcasted_iota(jnp.int32, (steps, rows), 1)
    ).astype(jnp.float32)
    polys = legendre_list(rowpos, total_rows)
    for order in range(K):
        poly_ref[order * steps : (order + 1) * steps, :] = polys[order]
        poly_ref[(K + order) * steps : (K + order + 1) * steps, :] = polys[order]
    poly_ref[RHS * steps : (RHS + 1) * steps, :] = jnp.ones((steps, rows), jnp.float32)
    poly_ref[(RHS + 1) * steps :, :] = jnp.zeros((steps, rows), jnp.float32)
    for step in range(steps):
        stack = poly_ref[pl.ds(step, KROWS, stride=steps), :]
        pairs = jnp.concatenate([stack * stack[i : i + 1] for i in range(K)], axis=0)
        high = pairs.astype(jnp.bfloat16)
        high_ref[:, step * rows : (step + 1) * rows] = high
        low_ref[:, step * rows : (step + 1) * rows] = (pairs - high.astype(jnp.float32)).astype(
            jnp.bfloat16
        )
    here = (first + lax.broadcasted_iota(jnp.int32, (1, rows), 1)).astype(jnp.float32)
    stack = stacked_legendre(here, total_rows)
    row = lax.broadcasted_iota(jnp.int32, (KROWS, rows), 0)
    table_ref[:, 0:rows] = jnp.where(row < K, stack, 0.0)
    table_ref[:, rows : 2 * rows] = jnp.where((row >= K) & (row < 2 * K), stack, 0.0)

    for copy in small:
        copy.wait()
    amp = amp_ref[...]
    lit = lit_by_lamp(start_ref[...], first, rows)
    lit_ref[...] = lit_columns(lit)
    which = which_ref[...]
    bundles = bundle_ref[...]
    base = jnp.zeros((1, fibers), jnp.float32)
    for bundle in range(bundles.shape[1]):
        base = jnp.where(which == bundle, bundles[:, bundle : bundle + 1], base)
    inverse = 1.0 / base
    base_ref[...] = inverse
    lane = lax.broadcasted_iota(jnp.int32, (1, fibers), 1)
    for fiber in range(owned):
        own = jnp.sum(jnp.where(lane == me * owned + fiber, inverse, 0.0), axis=1, keepdims=True)
        own_base_ref[fiber : fiber + 1, :] = jnp.broadcast_to(own, (1, rows))

    square_ref[...] = jnp.zeros_like(square_ref)
    square_ref[0:owned, 0:K] = trace_ref[...]
    square_ref[0:owned, K : 2 * K] = width_ref[...]
    coef_ref[...] = square_ref[...].T[0:KROWS]

    square = lax.dot_general(
        amp * amp, lit, (((0,), (0,)), ((), ())), precision=HIGH, preferred_element_type=jnp.float32
    )
    wide = owned * PIX

    def place(block, at, even_value, odd_value):
        keep_ref[block, at, :] = jnp.where(odd, odd_value, even_value)
        send_ref[block, at, :] = jnp.where(odd, even_value, odd_value)

    for block in range(fibers // (2 * owned)):
        low = 2 * block * owned
        place(
            block,
            slice(wide, wide + owned),
            square[low : low + owned],
            square[low + owned : low + 2 * owned],
        )
    for tile in range(cols // LANE):
        if (tile * LANE) % chunk == 0:
            arriving[tile * LANE // chunk].wait()
        amp_cols = per_column(amp, tile)
        total = jnp.zeros((rows, LANE), jnp.float32)
        for lamp in range(lamps):
            frame = frames_ref[lamp, :, tile * LANE : (tile + 1) * LANE].astype(jnp.float32)
            weight = lit_ref[:, lamp * LANE : (lamp + 1) * LANE] * amp_cols[lamp : lamp + 1]
            total = total + weight * frame
        flipped = total.T
        for pair in range(LANE // (2 * wide)):
            low = 2 * pair * wide
            place(
                tile * (LANE // (2 * wide)) + pair,
                slice(0, wide),
                flipped[low : low + wide],
                flipped[low + wide : low + 2 * wide],
            )


def collapse(
    frames, amplitude, line_start, bundle_width, fiber_bundle, trace_coef, width_coef, height
):
    lamps, rows, cols = frames.shape
    owned = trace_coef.shape[0]
    steps = lax.axis_size("rows")
    blocks = steps * lax.axis_size("fib") // 2
    args = (
        frames,
        amplitude,
        line_start,
        bundle_width.reshape(1, -1),
        fiber_bundle.reshape(1, -1),
        trace_coef,
        width_coef,
    )
    shape = jax.ShapeDtypeStruct
    outs = (
        shape((blocks, height, rows), jnp.float32),
        shape((blocks, height, rows), jnp.float32),
        shape((rows, lamps * LANE), jnp.float32),
        shape((KROWS, 2 * rows), jnp.float32),
        shape((1, fiber_bundle.shape[0]), jnp.float32),
        shape((owned, rows), jnp.float32),
        shape((KROWS, LANE), jnp.float32),
        shape((KROWS * steps, rows), jnp.float32),
        shape((K * KROWS, steps * rows), jnp.bfloat16),
        shape((K * KROWS, steps * rows), jnp.bfloat16),
    )
    return pl.pallas_call(
        collapse_kernel,
        out_shape=outs,
        in_specs=[pl.BlockSpec(memory_space=pltpu.HBM)] * len(args),
        out_specs=[pl.BlockSpec(memory_space=pltpu.VMEM)] * len(outs),
        scratch_shapes=[pltpu.VMEM(arg.shape, arg.dtype) for arg in args]
        + [
            pltpu.VMEM((LANE, LANE), jnp.float32),
            pltpu.SemaphoreType.DMA((len(args) - 1,)),
            pltpu.SemaphoreType.DMA((cols // min(CHUNK, cols),)),
        ],
        compiler_params=pltpu.CompilerParams(vmem_limit_bytes=VMEM_BYTES),
        name="collapse",
    )(*[pltpu.with_memory_space_constraint(arg, pltpu.HBM) for arg in args])


def fit_kernel(
    height,
    sources,
    owned,
    got_ref,
    start_ref,
    base_ref,
    poly_ref,
    high_ref,
    low_ref,
    send_ref,
    sum_ref,
    weight_ref,
    coef_ref,
    splat_ref,
    square_ref,
):
    wide = owned * PIX
    steps = got_ref.shape[0] // (height * sources)
    rows = got_ref.shape[1]
    used = wide + owned

    for group in range(steps // SUB):
        for item in range(used):
            value = None
            for source in range(sources):
                start = (group * SUB * sources + source) * height + item
                part = got_ref[pl.ds(start, SUB, stride=sources * height), :]
                value = part if value is None else value + part
            sum_ref[item, group * SUB : (group + 1) * SUB, :] = value

    coef_ref[...] = start_ref[...]
    inverse_base = [base_ref[fiber : fiber + 1, :] for fiber in range(owned)]
    weight_ref[...] = jnp.zeros_like(weight_ref)

    def newton_step(index, carry):
        for fiber in range(owned):
            splat_ref[fiber] = jnp.broadcast_to(
                coef_ref[:, fiber : fiber + 1], (KROWS, rows)
            )
        for group in range(steps // SUB):
            here = slice(group * SUB, (group + 1) * SUB)
            for fiber in range(owned):
                centre = jnp.zeros((SUB, rows), jnp.float32)
                spread = jnp.zeros((SUB, rows), jnp.float32)
                for order in range(K):
                    poly = poly_ref[order * steps + group * SUB : order * steps + (group + 1) * SUB, :]
                    centre = centre + splat_ref[fiber, order : order + 1, :] * poly
                    spread = spread + splat_ref[fiber, K + order : K + order + 1, :] * poly
                inverse = jnp.exp(-spread) * inverse_base[fiber]
                power = sum_ref[wide + fiber, here, :]
                sums = [jnp.zeros((SUB, rows), jnp.float32) for _ in range(5)]
                for pixel in range(PIX):
                    scaled = ((pixel - (PIX - 1) / 2.0) - centre) * inverse
                    shape = jnp.exp(-0.5 * scaled * scaled)
                    bend = shape * scaled
                    slope = bend * inverse
                    widen = bend * scaled
                    resid = sum_ref[fiber * PIX + pixel, here, :] - power * shape
                    sums[0] = sums[0] + slope * slope
                    sums[1] = sums[1] + slope * widen
                    sums[2] = sums[2] + widen * widen
                    sums[3] = sums[3] + resid * slope
                    sums[4] = sums[4] + resid * widen
                for kind in range(5):
                    value = sums[kind] * power if kind < 3 else sums[kind]
                    at = (kind * owned + fiber) * steps + group * SUB
                    weight_ref[at : at + SUB, :] = value
        count = weight_ref.shape[0] // steps
        weights = jnp.concatenate(
            [weight_ref[pl.ds(step, count, stride=steps), :] for step in range(steps)], axis=1
        )
        upper = weights.astype(jnp.bfloat16).astype(jnp.float32)
        both = jnp.concatenate([upper, weights - upper], axis=0).astype(jnp.bfloat16)
        dims = (((1,), (1,)), ((), ()))
        moments = lax.dot_general(
            high_ref[...], both, dims, preferred_element_type=jnp.float32
        ) + lax.dot_general(low_ref[...], both, dims, preferred_element_type=jnp.float32)
        lanes = moments.shape[1]
        moments = jnp.concatenate(
            [moments, jnp.zeros((moments.shape[0], LANE - lanes), jnp.float32)], axis=1
        )
        moments = moments + pltpu.roll(moments, LANE - count, 1)
        aligned = [moments] + [
            pltpu.roll(moments, LANE - kind * owned, 1) for kind in range(1, 5)
        ]
        row = lax.broadcasted_iota(jnp.int32, (KROWS, LANE), 0)

        def matrix_row(i, second):
            block = [item[i * KROWS : (i + 1) * KROWS] for item in aligned]
            left, right, side = (block[1], block[2], block[4]) if second else (
                block[0],
                block[1],
                block[3],
            )
            value = jnp.where(row < K, left, jnp.where(row < 2 * K, right, side))
            at = i + K if second else i
            return jnp.where(row == at, 1.5 * value + 1.0, value)

        matrix = [matrix_row(i, False) for i in range(K)] + [matrix_row(i, True) for i in range(K)]
        for pivot in range(2 * K):
            cut = KROWS - matrix[pivot].shape[0]
            inverse = 1.0 / matrix[pivot][pivot - cut : pivot - cut + 1]
            chosen = matrix[pivot] * inverse
            for i in range(2 * K):
                if i != pivot:
                    scale = matrix[i][pivot - cut : pivot - cut + 1]
                    matrix[i] = matrix[i] - scale * chosen
            matrix[pivot] = chosen
            if (pivot + 1) % SUB == 0:
                matrix = [item[SUB:] for item in matrix]
        for i in range(2 * K):
            cut = KROWS - matrix[i].shape[0]
            coef_ref[i : i + 1, :] = coef_ref[i : i + 1, :] + matrix[i][RHS - cut : RHS - cut + 1]
        return carry

    lax.fori_loop(0, ITERS, newton_step, 0)

    square_ref[...] = jnp.zeros_like(square_ref)
    lane = lax.broadcasted_iota(jnp.int32, (KROWS, LANE), 1)
    square_ref[0:KROWS, :] = jnp.where(lane < owned, coef_ref[...], 0.0)
    result = square_ref[...].T[0:owned]
    for device in range(send_ref.shape[0]):
        send_ref[device] = result


def fit(got, start, base, poly, high, low, devices, height, sources):
    owned, rows = base.shape
    steps = got.shape[0] // (height * sources)
    count = -(-5 * owned // SUB) * SUB
    vmem = pl.BlockSpec(memory_space=pltpu.VMEM)
    return pl.pallas_call(
        functools.partial(fit_kernel, height, sources, owned),
        out_shape=jax.ShapeDtypeStruct((devices, owned, LANE), jnp.float32),
        in_specs=[vmem] * 6,
        out_specs=vmem,
        scratch_shapes=[
            pltpu.VMEM((owned * PIX + owned, steps, rows), jnp.float32),
            pltpu.VMEM((count * steps, rows), jnp.float32),
            pltpu.VMEM((KROWS, LANE), jnp.float32),
            pltpu.VMEM((owned, KROWS, rows), jnp.float32),
            pltpu.VMEM((LANE, LANE), jnp.float32),
        ],
        compiler_params=pltpu.CompilerParams(vmem_limit_bytes=VMEM_BYTES),
        name="fit",
    )(got, start, base, poly, high, low)


def residual_kernel(
    owned,
    coef_ref,
    table_ref,
    base_ref,
    lit_ref,
    amp_ref,
    frames_ref,
    trace_hbm,
    width_hbm,
    image_hbm,
    trace_ref,
    width_ref,
    image_ref,
    small_sems,
    image_sems,
):
    lamps, rows, cols = frames_ref.shape
    me = lax.axis_index("rows") * lax.axis_size("fib") + lax.axis_index("fib")
    own = coef_ref[pl.ds(me * owned, owned), :]
    trace_ref[...] = own[:, 0:K]
    width_ref[...] = own[:, K : 2 * K]
    leaving = start_copies([trace_ref, width_ref], [trace_hbm, width_hbm], small_sems)

    coef = coef_ref[...].T[0:KROWS]
    curves = lax.dot_general(
        table_ref[...],
        coef,
        (((0,), (0,)), ((), ())),
        precision=HIGH,
        preferred_element_type=jnp.float32,
    )
    centre = curves[0:rows]
    inverse = jnp.exp(-curves[rows : 2 * rows]) * base_ref[...]
    amp = amp_ref[...]
    pixel = (lax.broadcasted_iota(jnp.int32, (rows, LANE), 1) % PIX).astype(jnp.float32)
    offset = pixel - (PIX - 1) / 2.0
    chunk = min(CHUNK, cols)
    for tile in range(cols // LANE):
        here = slice(tile * LANE, (tile + 1) * LANE)
        scaled = (offset - per_column(centre, tile)) * per_column(inverse, tile)
        shape = jnp.exp(-0.5 * scaled * scaled)
        amp_cols = per_column(amp, tile)
        for lamp in range(lamps):
            weight = lit_ref[:, lamp * LANE : (lamp + 1) * LANE] * amp_cols[lamp : lamp + 1]
            frame = frames_ref[lamp, :, here].astype(jnp.float32)
            image_ref[lamp, :, here] = (frame - weight * shape).astype(jnp.bfloat16)
        if ((tile + 1) * LANE) % chunk == 0:
            span = slice((tile + 1) * LANE - chunk, (tile + 1) * LANE)
            copy = pltpu.make_async_copy(
                image_ref.at[:, :, span],
                image_hbm.at[:, :, span],
                image_sems.at[tile * LANE // chunk],
            )
            copy.start()
            leaving.append(copy)
    for copy in leaving:
        copy.wait()


def residual(owned, coef, table, base, lit, amplitude, frames):
    cols = frames.shape[2]
    vmem = pl.BlockSpec(memory_space=pltpu.VMEM)
    hbm = pl.BlockSpec(memory_space=pltpu.HBM)
    fitted = jax.ShapeDtypeStruct((owned, K), jnp.float32)
    return pl.pallas_call(
        functools.partial(residual_kernel, owned),
        out_shape=(fitted, fitted, jax.ShapeDtypeStruct(frames.shape, jnp.bfloat16)),
        in_specs=[vmem] * 6,
        out_specs=[hbm] * 3,
        scratch_shapes=[
            pltpu.VMEM((owned, K), jnp.float32),
            pltpu.VMEM((owned, K), jnp.float32),
            pltpu.VMEM(frames.shape, jnp.bfloat16),
            pltpu.SemaphoreType.DMA((2,)),
            pltpu.SemaphoreType.DMA((cols // min(CHUNK, cols),)),
        ],
        compiler_params=pltpu.CompilerParams(vmem_limit_bytes=VMEM_BYTES),
        name="residual",
    )(coef, table, base, lit, amplitude, frames)


def body(frames, amplitude, line_start, bundle_width, fiber_bundle, trace_coef, width_coef):
    sources = lax.axis_size("fib")
    devices = lax.axis_size("rows") * sources
    rows = frames.shape[1]
    owned = trace_coef.shape[0]
    height = -(-(owned * PIX + owned) // SUB) * SUB
    keep, send, lit, table, base, own_base, start, poly, high, low = collapse(
        frames, amplitude, line_start, bundle_width, fiber_bundle, trace_coef, width_coef, height
    )
    came = lax.ppermute(send, "fib", [(index, index ^ 1) for index in range(sources)])
    alike = [[index for index in range(devices) if index % 2 == odd] for odd in range(2)]
    got = lax.all_to_all(keep + came, BOTH, 0, 0, axis_index_groups=alike, tiled=True)
    got = got.reshape(devices // 2 * height, rows)
    reply = fit(got, start, own_base, poly, high, low, devices, height, sources // 2)
    coef = lax.all_to_all(reply, BOTH, 0, 0, tiled=True).reshape(devices * owned, LANE)
    return residual(owned, coef, table, base, lit, amplitude, frames)


def solution(mesh):
    return jax.shard_map(
        body,
        mesh=mesh,
        in_specs=(
            P("fib", "rows", None),
            P("fib", None),
            P("fib", None),
            P(),
            P(),
            P(BOTH, None),
            P(BOTH, None),
        ),
        out_specs=(P(BOTH, None), P(BOTH, None), P("fib", "rows", None)),
        check_vma=False,
    )
```

```python
import functools

import jax
import jax.numpy as jnp
import numpy as np
from jax import lax
from jax.experimental import pallas as pl
from jax.experimental.pallas import tpu as pltpu
from jax.sharding import PartitionSpec as P

K = 11
PIX = 8
WIN = 8
ITERS = 3
SUB = 8
LANE = 128
KROWS = 24
RHS = 2 * K
PARTS = 9 * KROWS + 8
VMEM_BYTES = 20 << 20

HIGH = lax.Precision.HIGHEST
BOTH = ("rows", "fib")


def adams_factor(order):
    value = 1.0
    for index in range(1, order + 1):
        value = value * (2.0 * index - 1.0) / index
    return value


def system_map():
    table = np.zeros((K * KROWS, 3 * KROWS))
    for i in range(K):
        table[i * KROWS + RHS, 2 * KROWS + i] = 1.0
        for j in range(K):
            for inner in range(min(i, j) + 1):
                target = i + j - 2 * inner
                value = adams_factor(inner) * adams_factor(i - inner) * adams_factor(j - inner)
                value = value / adams_factor(i + j - inner)
                value = value * (2.0 * target + 1.0) / (2.0 * (i + j - inner) + 1.0)
                table[i * KROWS + j, target] += value
                table[i * KROWS + K + j, KROWS + target] += value
    high = table.astype(jnp.bfloat16)
    low = (table - high.astype(np.float64)).astype(jnp.bfloat16)
    spare = np.zeros((K * KROWS, PARTS - 9 * KROWS), jnp.bfloat16)
    return np.concatenate([high, high, low, spare], axis=1)


def legendre_list(rowpos, total, count):
    tvals = (2.0 * rowpos + 1.0) / total - 1.0
    polys = [jnp.ones_like(tvals), tvals]
    for order in range(1, count - 1):
        polys.append(
            ((2 * order + 1) * tvals * polys[order] - order * polys[order - 1]) / (order + 1)
        )
    return polys


def stacked_legendre(rowpos, total):
    polys = legendre_list(rowpos, total, K)
    row = lax.broadcasted_iota(jnp.int32, (KROWS, rowpos.shape[1]), 0)
    table = jnp.zeros((KROWS, rowpos.shape[1]), jnp.float32)
    for order in range(K):
        table = jnp.where((row == order) | (row == K + order), polys[order], table)
    return jnp.where(row == RHS, 1.0, table)


def lit_by_lamp(start, first, rows):
    lamps, lines = start.shape
    rowid = first + lax.broadcasted_iota(jnp.int32, (lamps, rows), 1)
    lit = jnp.zeros((lamps, rows), jnp.float32)
    for line in range(lines):
        away = rowid - start[:, line : line + 1]
        lit = jnp.where((away >= 0) & (away < WIN), 1.0, lit)
    return lit


def lit_columns(lit):
    lamps, rows = lit.shape
    which = lax.broadcasted_iota(jnp.int32, (lamps, lamps * LANE), 1) // LANE
    own = lax.broadcasted_iota(jnp.int32, (lamps, lamps * LANE), 0)
    spread = jnp.where(which == own, 1.0, 0.0)
    return lax.dot_general(
        lit, spread, (((0,), (0,)), ((), ())), preferred_element_type=jnp.float32
    )


def take_lanes(values, index):
    parts = values.shape[1] // LANE
    result = None
    for part in range(parts):
        block = values[:, part * LANE : (part + 1) * LANE]
        taken = jnp.take_along_axis(block, index % LANE, axis=1, mode="promise_in_bounds")
        result = taken if result is None else jnp.where(index // LANE == part, taken, result)
    return result


def per_column(values, tile, owned, grouped):
    fiber = tile * (LANE // PIX) + (
        lax.broadcasted_iota(jnp.int32, (values.shape[0], LANE), 1) // PIX
    )
    if grouped:
        fiber = (fiber % owned) * (values.shape[1] // owned) + fiber // owned
    else:
        part = tile * (LANE // PIX) // LANE
        values = values[:, part * LANE : (part + 1) * LANE]
        fiber = fiber % LANE
    return take_lanes(values, fiber)


def start_copies(sources, targets, sems):
    copies = [
        pltpu.make_async_copy(source, target, sems.at[index])
        for index, (source, target) in enumerate(zip(sources, targets))
    ]
    for copy in copies:
        copy.start()
    return copies


def collapse_kernel(
    frames_hbm,
    amp_hbm,
    start_hbm,
    bundle_hbm,
    which_hbm,
    trace_hbm,
    width_hbm,
    keep_ref,
    send_ref,
    lit_ref,
    table_ref,
    coef_ref,
    poly_ref,
    split_ref,
    frames_ref,
    amp_ref,
    start_ref,
    bundle_ref,
    which_ref,
    trace_ref,
    width_ref,
    square_ref,
    small_sems,
    frame_sems,
):
    lamps, rows, cols = frames_ref.shape
    owned = trace_ref.shape[0]
    fibers = which_ref.shape[1]
    steps = lax.axis_size("rows")
    total_rows = steps * rows
    me = lax.axis_index("rows") * lax.axis_size("fib") + lax.axis_index("fib")
    first = lax.axis_index("rows") * rows
    odd = lax.axis_index("fib") % 2 == 1

    small = start_copies(
        [amp_hbm, start_hbm, bundle_hbm, which_hbm, trace_hbm, width_hbm],
        [amp_ref, start_ref, bundle_ref, which_ref, trace_ref, width_ref],
        small_sems,
    )
    arriving = start_copies([frames_hbm], [frames_ref], frame_sems)

    rowpos = (
        lax.broadcasted_iota(jnp.int32, (steps, rows), 0) * rows
        + lax.broadcasted_iota(jnp.int32, (steps, rows), 1)
    ).astype(jnp.float32)
    polys = legendre_list(rowpos, total_rows, 2 * K - 1)
    for order in range(KROWS):
        poly_ref[order * steps : (order + 1) * steps, :] = (
            polys[order] if order < 2 * K - 1 else jnp.zeros((steps, rows), jnp.float32)
        )
    for step in range(steps):
        stack = poly_ref[pl.ds(step, KROWS, stride=steps), :]
        high = stack.astype(jnp.bfloat16).astype(jnp.float32)
        split_ref[:, step * rows : (step + 1) * rows] = jnp.concatenate(
            [high, stack - high], axis=0
        ).astype(jnp.bfloat16)

    here = (first + lax.broadcasted_iota(jnp.int32, (1, rows), 1)).astype(jnp.float32)
    stack = stacked_legendre(here, total_rows)
    row = lax.broadcasted_iota(jnp.int32, (KROWS, rows), 0)
    table_ref[:, 0:rows] = jnp.where(row < K, stack, 0.0)
    table_ref[:, rows : 2 * rows] = jnp.where((row >= K) & (row < 2 * K), stack, 0.0)

    for copy in small:
        copy.wait()
    amp = amp_ref[...]
    lit = lit_by_lamp(start_ref[...], first, rows)
    lit_ref[...] = lit_columns(lit)
    which = which_ref[...]
    bundles = bundle_ref[...]
    base = jnp.zeros((1, fibers), jnp.float32)
    for bundle in range(bundles.shape[1]):
        base = jnp.where(which == bundle, bundles[:, bundle : bundle + 1], base)
    inverse = 1.0 / base
    lane = lax.broadcasted_iota(jnp.int32, (1, fibers), 1)

    square_ref[...] = jnp.zeros_like(square_ref)
    square_ref[0:owned, 0:K] = trace_ref[...]
    square_ref[0:owned, K : 2 * K] = width_ref[...]
    for fiber in range(owned):
        square_ref[fiber : fiber + 1, RHS : RHS + 1] = jnp.sum(
            jnp.where(lane == me * owned + fiber, inverse, 0.0), axis=1, keepdims=True
        )
    coef_ref[...] = square_ref[...].T[0:KROWS]

    square = lax.dot_general(
        amp * amp, lit, (((0,), (0,)), ((), ())), precision=HIGH, preferred_element_type=jnp.float32
    )
    wide = owned * PIX

    height = wide + owned

    def place(block, offset, even_value, odd_value):
        at = slice(block * height + offset, block * height + offset + even_value.shape[0])
        keep_ref[at, :] = jnp.where(odd, odd_value, even_value)
        send_ref[at, :] = jnp.where(odd, even_value, odd_value)

    for block in range(fibers // (2 * owned)):
        low = 2 * block * owned
        place(
            block,
            wide,
            square[low : low + owned],
            square[low + owned : low + 2 * owned],
        )
    for copy in arriving:
        copy.wait()
    for tile in range(cols // LANE):
        amp_cols = per_column(amp, tile, owned, False)
        total = jnp.zeros((rows, LANE), jnp.float32)
        for lamp in range(lamps):
            frame = frames_ref[lamp, :, tile * LANE : (tile + 1) * LANE].astype(jnp.float32)
            weight = lit_ref[:, lamp * LANE : (lamp + 1) * LANE] * amp_cols[lamp : lamp + 1]
            total = total + weight * frame
        flipped = total.T
        for pair in range(LANE // (2 * wide)):
            low = 2 * pair * wide
            place(
                tile * (LANE // (2 * wide)) + pair,
                0,
                flipped[low : low + wide],
                flipped[low + wide : low + 2 * wide],
            )


def collapse(
    frames, amplitude, line_start, bundle_width, fiber_bundle, trace_coef, width_coef, height
):
    lamps, rows, cols = frames.shape
    steps = lax.axis_size("rows")
    blocks = steps * lax.axis_size("fib") // 2
    args = (
        frames,
        amplitude,
        line_start,
        bundle_width.reshape(1, -1),
        fiber_bundle.reshape(1, -1),
        trace_coef,
        width_coef,
    )
    shape = jax.ShapeDtypeStruct
    outs = (
        shape((blocks * height, rows), jnp.float32),
        shape((blocks * height, rows), jnp.float32),
        shape((rows, lamps * LANE), jnp.float32),
        shape((KROWS, 2 * rows), jnp.float32),
        shape((KROWS, LANE), jnp.float32),
        shape((KROWS * steps, rows), jnp.float32),
        shape((2 * KROWS, steps * rows), jnp.bfloat16),
    )
    return pl.pallas_call(
        collapse_kernel,
        out_shape=outs,
        in_specs=[pl.BlockSpec(memory_space=pltpu.HBM)] * len(args),
        out_specs=[pl.BlockSpec(memory_space=pltpu.VMEM)] * len(outs),
        scratch_shapes=[pltpu.VMEM(arg.shape, arg.dtype) for arg in args]
        + [
            pltpu.VMEM((LANE, LANE), jnp.float32),
            pltpu.SemaphoreType.DMA((len(args) - 1,)),
            pltpu.SemaphoreType.DMA((1,)),
        ],
        compiler_params=pltpu.CompilerParams(vmem_limit_bytes=VMEM_BYTES),
        name="collapse",
    )(*[pltpu.with_memory_space_constraint(arg, pltpu.HBM) for arg in args])


def fit_kernel(
    height,
    sources,
    owned,
    got_ref,
    start_ref,
    poly_ref,
    split_ref,
    map_ref,
    send_ref,
    sum_ref,
    weight_ref,
    coef_ref,
    splat_ref,
    square_ref,
):
    wide = owned * PIX
    steps = got_ref.shape[0] // (height * sources)
    rows = got_ref.shape[1]
    used = wide + owned

    for group in range(steps // SUB):
        for item in range(used):
            value = None
            for source in range(sources):
                start = (group * SUB * sources + source) * height + item
                part = got_ref[pl.ds(start, SUB, stride=sources * height), :]
                value = part if value is None else value + part
            sum_ref[item, group * SUB : (group + 1) * SUB, :] = value

    coef_ref[...] = start_ref[...]
    weight_ref[...] = jnp.zeros_like(weight_ref)

    def newton_step(index, carry):
        for fiber in range(owned):
            splat_ref[fiber] = jnp.broadcast_to(
                coef_ref[:, fiber : fiber + 1], (KROWS, rows)
            )
        for group in range(steps // SUB):
            here = slice(group * SUB, (group + 1) * SUB)
            for fiber in range(owned):
                centre = jnp.zeros((SUB, rows), jnp.float32)
                spread = jnp.zeros((SUB, rows), jnp.float32)
                for order in range(K):
                    poly = poly_ref[order * steps + group * SUB : order * steps + (group + 1) * SUB, :]
                    centre = centre + splat_ref[fiber, order : order + 1, :] * poly
                    spread = spread + splat_ref[fiber, K + order : K + order + 1, :] * poly
                inverse = jnp.exp(-spread) * splat_ref[fiber, RHS : RHS + 1, :]
                power = sum_ref[wide + fiber, here, :]
                sums = [jnp.zeros((SUB, rows), jnp.float32) for _ in range(5)]
                for pixel in range(PIX):
                    scaled = ((pixel - (PIX - 1) / 2.0) - centre) * inverse
                    shape = jnp.exp(-0.5 * scaled * scaled)
                    bend = shape * scaled
                    slope = bend * inverse
                    widen = bend * scaled
                    resid = sum_ref[fiber * PIX + pixel, here, :] - power * shape
                    sums[0] = sums[0] + slope * slope
                    sums[1] = sums[1] + slope * widen
                    sums[2] = sums[2] + widen * widen
                    sums[3] = sums[3] + resid * slope
                    sums[4] = sums[4] + resid * widen
                for kind in range(5):
                    value = sums[kind] * power if kind < 3 else sums[kind]
                    at = (kind * owned + fiber) * steps + group * SUB
                    weight_ref[at : at + SUB, :] = value
        count = weight_ref.shape[0] // steps
        weights = jnp.concatenate(
            [weight_ref[pl.ds(step, count, stride=steps), :] for step in range(steps)], axis=1
        )
        upper = weights.astype(jnp.bfloat16).astype(jnp.float32)
        both = jnp.concatenate([upper, weights - upper], axis=0).astype(jnp.bfloat16)
        moments = lax.dot_general(
            split_ref[...], both, (((1,), (1,)), ((), ())), preferred_element_type=jnp.float32
        )
        moments = moments[0:KROWS] + moments[KROWS:]
        moments = jnp.concatenate(
            [moments, jnp.zeros((KROWS, LANE - 2 * count), jnp.float32)], axis=1
        )
        moments = moments + pltpu.roll(moments, LANE - count, 1)
        kinds = [moments] + [
            pltpu.roll(moments, LANE - kind * owned, 1) for kind in range(1, 5)
        ]
        stacked = jnp.concatenate(
            [
                jnp.concatenate([kinds[0], kinds[1], kinds[3]], axis=0),
                jnp.concatenate([kinds[1], kinds[2], kinds[4]], axis=0),
            ],
            axis=1,
        )
        high = stacked.astype(jnp.bfloat16).astype(jnp.float32)
        spare = jnp.zeros((PARTS - 9 * KROWS, 2 * LANE), jnp.float32)
        system = jnp.dot(
            map_ref[...],
            jnp.concatenate([high, stacked - high, high, spare], axis=0).astype(jnp.bfloat16),
            preferred_element_type=jnp.float32,
        )
        row = lax.broadcasted_iota(jnp.int32, (KROWS, LANE), 0)
        matrix = []
        for i in range(2 * K):
            second, at = divmod(i, K)
            value = system[at * KROWS : (at + 1) * KROWS, second * LANE : (second + 1) * LANE]
            matrix.append(jnp.where(row == i, 1.5 * value + 1.0, value))
        for pivot in range(2 * K):
            cut = KROWS - matrix[pivot].shape[0]
            inverse = 1.0 / matrix[pivot][pivot - cut : pivot - cut + 1]
            chosen = matrix[pivot] * inverse
            for i in range(2 * K):
                if i != pivot:
                    scale = matrix[i][pivot - cut : pivot - cut + 1]
                    matrix[i] = matrix[i] - scale * chosen
            matrix[pivot] = chosen
            if (pivot + 1) % SUB == 0:
                matrix = [item[SUB:] for item in matrix]
        for i in range(2 * K):
            cut = KROWS - matrix[i].shape[0]
            coef_ref[i : i + 1, :] = coef_ref[i : i + 1, :] + matrix[i][RHS - cut : RHS - cut + 1]
        return carry

    lax.fori_loop(0, ITERS, newton_step, 0)

    square_ref[...] = jnp.zeros_like(square_ref)
    lane = lax.broadcasted_iota(jnp.int32, (KROWS, LANE), 1)
    square_ref[0:KROWS, :] = jnp.where(lane < owned, coef_ref[...], 0.0)
    result = square_ref[...].T[0:owned]
    packed = result[0:1]
    for fiber in range(1, owned):
        packed = packed + pltpu.roll(result[fiber : fiber + 1], fiber * (LANE // owned), 1)
    send_ref[...] = jnp.broadcast_to(packed, send_ref.shape)


def fit(got, start, poly, split, owned, devices, height, sources):
    rows = got.shape[1]
    steps = got.shape[0] // (height * sources)
    count = -(-5 * owned // SUB) * SUB
    vmem = pl.BlockSpec(memory_space=pltpu.VMEM)
    return pl.pallas_call(
        functools.partial(fit_kernel, height, sources, owned),
        out_shape=jax.ShapeDtypeStruct((devices, LANE), jnp.float32),
        in_specs=[vmem] * 5,
        out_specs=vmem,
        scratch_shapes=[
            pltpu.VMEM((owned * PIX + owned, steps, rows), jnp.float32),
            pltpu.VMEM((count * steps, rows), jnp.float32),
            pltpu.VMEM((KROWS, LANE), jnp.float32),
            pltpu.VMEM((owned, KROWS, rows), jnp.float32),
            pltpu.VMEM((LANE, LANE), jnp.float32),
        ],
        compiler_params=pltpu.CompilerParams(vmem_limit_bytes=VMEM_BYTES),
        name="fit",
    )(got, start, poly, split, jnp.asarray(system_map()))


def residual_kernel(
    owned,
    coef_ref,
    table_ref,
    lit_ref,
    amp_ref,
    frames_ref,
    trace_hbm,
    width_hbm,
    image_hbm,
    trace_ref,
    width_ref,
    image_ref,
    shape_ref,
    bright_ref,
    small_sems,
    image_sems,
):
    lamps, rows, cols = frames_ref.shape
    me = lax.axis_index("rows") * lax.axis_size("fib") + lax.axis_index("fib")
    own = coef_ref[pl.ds(me, 1), :]
    each = LANE // owned
    for fiber in range(owned):
        at = fiber * each
        trace_ref[fiber : fiber + 1, :] = own[:, at : at + K]
        width_ref[fiber : fiber + 1, :] = own[:, at + K : at + 2 * K]
    leaving = start_copies([trace_ref, width_ref], [trace_hbm, width_hbm], small_sems)

    flipped = coef_ref[...].T
    coef = jnp.concatenate(
        [flipped[fiber * each : fiber * each + KROWS] for fiber in range(owned)], axis=1
    )
    curves = lax.dot_general(
        table_ref[...],
        coef,
        (((0,), (0,)), ((), ())),
        precision=HIGH,
        preferred_element_type=jnp.float32,
    )
    centre = curves[0:rows]
    inverse = jnp.exp(-curves[rows : 2 * rows]) * coef[RHS : RHS + 1]
    amp = amp_ref[...]
    pixel = (lax.broadcasted_iota(jnp.int32, (rows, LANE), 1) % PIX).astype(jnp.float32)
    offset = pixel - (PIX - 1) / 2.0
    for tile in range(cols // LANE):
        here = slice(tile * LANE, (tile + 1) * LANE)
        scaled = (offset - per_column(centre, tile, owned, True)) * per_column(
            inverse, tile, owned, True
        )
        shape_ref[:, here] = jnp.exp(-0.5 * scaled * scaled)
        bright = per_column(amp, tile, owned, False)
        for lamp in range(lamps):
            bright_ref[lamp, :, here] = bright[lamp : lamp + 1]

    def leave(lamp):
        return pltpu.make_async_copy(
            image_ref.at[lamp], image_hbm.at[lamp], image_sems.at[lamp]
        )

    def one_lamp(lamp, carry):
        lit = lit_ref[:, pl.ds(pl.multiple_of(lamp * LANE, LANE), LANE)]
        for tile in range(cols // LANE):
            here = slice(tile * LANE, (tile + 1) * LANE)
            weight = lit * bright_ref[lamp, :, here]
            frame = frames_ref[lamp, :, here].astype(jnp.float32)
            image_ref[lamp, :, here] = (frame - weight * shape_ref[:, here]).astype(jnp.bfloat16)
        leave(lamp).start()
        return carry

    lax.fori_loop(0, lamps, one_lamp, 0)
    for lamp in range(lamps):
        leave(lamp).wait()
    for copy in leaving:
        copy.wait()


def residual(owned, coef, table, lit, amplitude, frames):
    lamps, rows, cols = frames.shape
    vmem = pl.BlockSpec(memory_space=pltpu.VMEM)
    hbm = pl.BlockSpec(memory_space=pltpu.HBM)
    fitted = jax.ShapeDtypeStruct((owned, K), jnp.float32)
    return pl.pallas_call(
        functools.partial(residual_kernel, owned),
        out_shape=(fitted, fitted, jax.ShapeDtypeStruct(frames.shape, jnp.bfloat16)),
        in_specs=[vmem] * 5,
        out_specs=[hbm] * 3,
        scratch_shapes=[
            pltpu.VMEM((owned, K), jnp.float32),
            pltpu.VMEM((owned, K), jnp.float32),
            pltpu.VMEM(frames.shape, jnp.bfloat16),
            pltpu.VMEM((rows, cols), jnp.float32),
            pltpu.VMEM((lamps, 1, cols), jnp.float32),
            pltpu.SemaphoreType.DMA((2,)),
            pltpu.SemaphoreType.DMA((lamps,)),
        ],
        compiler_params=pltpu.CompilerParams(vmem_limit_bytes=VMEM_BYTES),
        name="residual",
    )(coef, table, lit, amplitude, frames)


def body(frames, amplitude, line_start, bundle_width, fiber_bundle, trace_coef, width_coef):
    sources = lax.axis_size("fib")
    devices = lax.axis_size("rows") * sources
    rows = frames.shape[1]
    owned = trace_coef.shape[0]
    height = owned * PIX + owned
    keep, send, lit, table, start, poly, split = collapse(
        frames, amplitude, line_start, bundle_width, fiber_bundle, trace_coef, width_coef, height
    )
    came = lax.ppermute(send, "fib", [(index, index ^ 1) for index in range(sources)])
    alike = [[index for index in range(devices) if index % 2 == odd] for odd in range(2)]
    unit = 4 if height % 4 == 0 else 1
    got = lax.all_to_all(
        (keep + came).reshape(devices // 2, height // unit, unit, rows),
        BOTH,
        0,
        0,
        axis_index_groups=alike,
        tiled=True,
    ).reshape(devices // 2 * height, rows)
    reply = fit(got, start, poly, split, owned, devices, height, sources // 2)
    coef = lax.all_to_all(reply, BOTH, 0, 0, tiled=True)
    return residual(owned, coef, table, lit, amplitude, frames)


def solution(mesh):
    return jax.shard_map(
        body,
        mesh=mesh,
        in_specs=(
            P("fib", "rows", None),
            P("fib", None),
            P("fib", None),
            P(),
            P(),
            P(BOTH, None),
            P(BOTH, None),
        ),
        out_specs=(P(BOTH, None), P(BOTH, None), P("fib", "rows", None)),
        check_vma=False,
    )
```

```python
import functools

import jax
import jax.numpy as jnp
import numpy as np
from jax import lax
from jax.experimental import pallas as pl
from jax.experimental.pallas import tpu as pltpu
from jax.sharding import PartitionSpec as P

K = 11
PIX = 8
WIN = 8
ITERS = 3
SUB = 8
LANE = 128
KROWS = 24
RHS = 2 * K
WIDTH = RHS + 1
VMEM_BYTES = 20 << 20

HIGH = lax.Precision.HIGHEST
BOTH = ("rows", "fib")


def adams_factor(order):
    value = 1.0
    for index in range(1, order + 1):
        value = value * (2.0 * index - 1.0) / index
    return value


def system_map():
    table = np.zeros((LANE, 2 * LANE))
    for i in range(K):
        table[2 * KROWS + i, i * WIDTH + RHS] = 1.0
        for j in range(K):
            for inner in range(min(i, j) + 1):
                target = i + j - 2 * inner
                value = adams_factor(inner) * adams_factor(i - inner) * adams_factor(j - inner)
                value = value / adams_factor(i + j - inner)
                value = value * (2.0 * target + 1.0) / (2.0 * (i + j - inner) + 1.0)
                table[target, i * WIDTH + j] += value
                table[KROWS + target, i * WIDTH + K + j] += value
    high = table.astype(jnp.bfloat16)
    low = (table - high.astype(np.float64)).astype(jnp.bfloat16)
    return np.concatenate([high, low], axis=0)


def legendre_list(rowpos, total, count):
    tvals = (2.0 * rowpos + 1.0) / total - 1.0
    polys = [jnp.ones_like(tvals), tvals]
    for order in range(1, count - 1):
        polys.append(
            ((2 * order + 1) * tvals * polys[order] - order * polys[order - 1]) / (order + 1)
        )
    return polys


def lit_by_lamp(start, first, rows):
    lamps, lines = start.shape
    rowid = first + lax.broadcasted_iota(jnp.int32, (lamps, rows), 1)
    lit = jnp.zeros((lamps, rows), jnp.float32)
    for line in range(lines):
        away = rowid - start[:, line : line + 1]
        lit = jnp.where((away >= 0) & (away < WIN), 1.0, lit)
    return lit


def lit_columns(lit):
    lamps, rows = lit.shape
    which = lax.broadcasted_iota(jnp.int32, (lamps, lamps * LANE), 1) // LANE
    own = lax.broadcasted_iota(jnp.int32, (lamps, lamps * LANE), 0)
    spread = jnp.where(which == own, 1.0, 0.0)
    return lax.dot_general(
        lit, spread, (((0,), (0,)), ((), ())), preferred_element_type=jnp.float32
    )


def take_lanes(values, index):
    parts = values.shape[1] // LANE
    result = None
    for part in range(parts):
        block = values[:, part * LANE : (part + 1) * LANE]
        taken = jnp.take_along_axis(block, index % LANE, axis=1, mode="promise_in_bounds")
        result = taken if result is None else jnp.where(index // LANE == part, taken, result)
    return result


def per_column(values, tile, owned, grouped):
    fiber = tile * (LANE // PIX) + (
        lax.broadcasted_iota(jnp.int32, (values.shape[0], LANE), 1) // PIX
    )
    if grouped:
        fiber = (fiber % owned) * (values.shape[1] // owned) + fiber // owned
    else:
        part = tile * (LANE // PIX) // LANE
        values = values[:, part * LANE : (part + 1) * LANE]
        fiber = fiber % LANE
    return take_lanes(values, fiber)


def start_copies(sources, targets, sems):
    copies = [
        pltpu.make_async_copy(source, target, sems.at[index])
        for index, (source, target) in enumerate(zip(sources, targets))
    ]
    for copy in copies:
        copy.start()
    return copies


def tables_kernel(after_ref, poly_ref, split_ref, local_ref):
    rows = poly_ref.shape[1]
    steps = poly_ref.shape[0] // KROWS

    rowpos = (
        lax.broadcasted_iota(jnp.int32, (steps, rows), 0) * rows
        + lax.broadcasted_iota(jnp.int32, (steps, rows), 1)
    ).astype(jnp.float32)
    polys = legendre_list(rowpos, steps * rows, 2 * K - 1)
    for order in range(KROWS):
        poly_ref[order * steps : (order + 1) * steps, :] = (
            polys[order] if order < 2 * K - 1 else jnp.zeros((steps, rows), jnp.float32)
        )

    spare = jnp.zeros((LANE - 3 * KROWS, rows), jnp.float32)
    for step in range(steps):
        stack = poly_ref[pl.ds(step, KROWS, stride=steps), :]
        high = stack.astype(jnp.bfloat16).astype(jnp.float32)
        for half, part in enumerate([high, stack - high]):
            split_ref[step * rows : (step + 1) * rows, half * LANE : (half + 1) * LANE] = (
                jnp.concatenate([part, part, part, spare], axis=0).T.astype(jnp.bfloat16)
            )

    first = lax.axis_index("rows") * rows
    here = (first + lax.broadcasted_iota(jnp.int32, (rows, LANE), 0)).astype(jnp.float32)
    for order, poly in enumerate(legendre_list(here, steps * rows, K)):
        local_ref[order] = poly


def tables(after, rows):
    steps = lax.axis_size("rows")
    shape = jax.ShapeDtypeStruct
    vmem = pl.BlockSpec(memory_space=pltpu.VMEM)
    size = 2 * LANE * steps * rows
    return pl.pallas_call(
        tables_kernel,
        out_shape=(
            shape((KROWS * steps, rows), jnp.float32),
            shape((steps * rows, 2 * LANE), jnp.bfloat16),
            shape((K, rows, LANE), jnp.float32),
        ),
        in_specs=[vmem],
        out_specs=[vmem] * 3,
        compiler_params=pltpu.CompilerParams(vmem_limit_bytes=VMEM_BYTES),
        cost_estimate=pl.CostEstimate(flops=8 * size, bytes_accessed=4 * size, transcendentals=0),
        name="tables",
    )(after)


def collapse_kernel(
    frames_hbm,
    amp_hbm,
    start_hbm,
    bundle_hbm,
    which_hbm,
    trace_hbm,
    width_hbm,
    keep_ref,
    send_ref,
    lit_ref,
    coef_ref,
    frames_ref,
    amp_ref,
    start_ref,
    bundle_ref,
    which_ref,
    trace_ref,
    width_ref,
    square_ref,
    small_sems,
    frame_sems,
):
    lamps, rows, cols = frames_ref.shape
    owned = trace_ref.shape[0]
    fibers = which_ref.shape[1]
    me = lax.axis_index("rows") * lax.axis_size("fib") + lax.axis_index("fib")
    first = lax.axis_index("rows") * rows
    odd = lax.axis_index("fib") % 2 == 1

    small = start_copies(
        [amp_hbm, start_hbm, bundle_hbm, which_hbm, trace_hbm, width_hbm],
        [amp_ref, start_ref, bundle_ref, which_ref, trace_ref, width_ref],
        small_sems,
    )
    arriving = start_copies([frames_hbm], [frames_ref], frame_sems)

    for copy in small:
        copy.wait()
    amp = amp_ref[...]
    lit = lit_by_lamp(start_ref[...], first, rows)
    lit_ref[...] = lit_columns(lit)
    which = which_ref[...]
    bundles = bundle_ref[...]
    base = jnp.zeros((1, fibers), jnp.float32)
    for bundle in range(bundles.shape[1]):
        base = jnp.where(which == bundle, bundles[:, bundle : bundle + 1], base)
    inverse = 1.0 / base
    lane = lax.broadcasted_iota(jnp.int32, (1, fibers), 1)

    square_ref[...] = jnp.zeros_like(square_ref)
    square_ref[0:owned, 0:K] = trace_ref[...]
    square_ref[0:owned, K : 2 * K] = width_ref[...]
    for fiber in range(owned):
        square_ref[fiber : fiber + 1, RHS : RHS + 1] = jnp.sum(
            jnp.where(lane == me * owned + fiber, inverse, 0.0), axis=1, keepdims=True
        )
    coef_ref[...] = square_ref[...].T[0:KROWS]

    square = lax.dot_general(
        amp * amp, lit, (((0,), (0,)), ((), ())), precision=HIGH, preferred_element_type=jnp.float32
    )
    wide = owned * PIX

    height = wide + owned

    def place(block, offset, even_value, odd_value):
        at = slice(block * height + offset, block * height + offset + even_value.shape[0])
        keep_ref[at, :] = jnp.where(odd, odd_value, even_value)
        send_ref[at, :] = jnp.where(odd, even_value, odd_value)

    for block in range(fibers // (2 * owned)):
        low = 2 * block * owned
        place(
            block,
            wide,
            square[low : low + owned],
            square[low + owned : low + 2 * owned],
        )
    for copy in arriving:
        copy.wait()
    for tile in range(cols // LANE):
        amp_cols = per_column(amp, tile, owned, False)
        total = jnp.zeros((rows, LANE), jnp.float32)
        for lamp in range(lamps):
            frame = frames_ref[lamp, :, tile * LANE : (tile + 1) * LANE].astype(jnp.float32)
            weight = lit_ref[:, lamp * LANE : (lamp + 1) * LANE] * amp_cols[lamp : lamp + 1]
            total = total + weight * frame
        flipped = total.T
        for pair in range(LANE // (2 * wide)):
            low = 2 * pair * wide
            place(
                tile * (LANE // (2 * wide)) + pair,
                0,
                flipped[low : low + wide],
                flipped[low + wide : low + 2 * wide],
            )


def collapse(
    frames, amplitude, line_start, bundle_width, fiber_bundle, trace_coef, width_coef, height
):
    lamps, rows, cols = frames.shape
    steps = lax.axis_size("rows")
    blocks = steps * lax.axis_size("fib") // 2
    args = (
        frames,
        amplitude,
        line_start,
        bundle_width.reshape(1, -1),
        fiber_bundle.reshape(1, -1),
        trace_coef,
        width_coef,
    )
    shape = jax.ShapeDtypeStruct
    outs = (
        shape((blocks * height, rows), jnp.float32),
        shape((blocks * height, rows), jnp.float32),
        shape((rows, lamps * LANE), jnp.float32),
        shape((KROWS, LANE), jnp.float32),
    )
    return pl.pallas_call(
        collapse_kernel,
        out_shape=outs,
        in_specs=[pl.BlockSpec(memory_space=pltpu.HBM)] * len(args),
        out_specs=[pl.BlockSpec(memory_space=pltpu.VMEM)] * len(outs),
        scratch_shapes=[pltpu.VMEM(arg.shape, arg.dtype) for arg in args]
        + [
            pltpu.VMEM((LANE, LANE), jnp.float32),
            pltpu.SemaphoreType.DMA((len(args) - 1,)),
            pltpu.SemaphoreType.DMA((1,)),
        ],
        compiler_params=pltpu.CompilerParams(vmem_limit_bytes=VMEM_BYTES),
        name="collapse",
    )(*[pltpu.with_memory_space_constraint(arg, pltpu.HBM) for arg in args])


def fit_kernel(
    height,
    sources,
    owned,
    got_ref,
    start_ref,
    poly_ref,
    split_ref,
    map_ref,
    send_ref,
    sum_ref,
    weight_ref,
    coef_ref,
    splat_ref,
    square_ref,
    moment_ref,
    system_ref,
):
    wide = owned * PIX
    steps = got_ref.shape[0] // (height * sources)
    rows = got_ref.shape[1]
    used = wide + owned

    for group in range(steps // SUB):
        for item in range(used):
            value = None
            for source in range(sources):
                start = (group * SUB * sources + source) * height + item
                part = got_ref[pl.ds(start, SUB, stride=sources * height), :]
                value = part if value is None else value + part
            sum_ref[item, group * SUB : (group + 1) * SUB, :] = value

    coef_ref[...] = start_ref[...]
    weight_ref[...] = jnp.zeros_like(weight_ref)
    moment_ref[...] = jnp.zeros_like(moment_ref)
    system_ref[...] = jnp.zeros_like(system_ref)

    def newton_step(index, carry):
        for fiber in range(owned):
            splat_ref[fiber] = jnp.broadcast_to(
                coef_ref[:, fiber : fiber + 1], (KROWS, rows)
            )
        for group in range(steps // SUB):
            here = slice(group * SUB, (group + 1) * SUB)
            for fiber in range(owned):
                centre = jnp.zeros((SUB, rows), jnp.float32)
                spread = jnp.zeros((SUB, rows), jnp.float32)
                for order in range(K):
                    poly = poly_ref[order * steps + group * SUB : order * steps + (group + 1) * SUB, :]
                    centre = centre + splat_ref[fiber, order : order + 1, :] * poly
                    spread = spread + splat_ref[fiber, K + order : K + order + 1, :] * poly
                inverse = jnp.exp(-spread) * splat_ref[fiber, RHS : RHS + 1, :]
                power = sum_ref[wide + fiber, here, :]
                sums = [jnp.zeros((SUB, rows), jnp.float32) for _ in range(5)]
                for pixel in range(PIX):
                    scaled = ((pixel - (PIX - 1) / 2.0) - centre) * inverse
                    shape = jnp.exp(-0.5 * scaled * scaled)
                    bend = shape * scaled
                    slope = bend * inverse
                    widen = bend * scaled
                    resid = sum_ref[fiber * PIX + pixel, here, :] - power * shape
                    sums[0] = sums[0] + slope * slope
                    sums[1] = sums[1] + slope * widen
                    sums[2] = sums[2] + widen * widen
                    sums[3] = sums[3] + resid * slope
                    sums[4] = sums[4] + resid * widen
                for kind in range(5):
                    value = sums[kind] * power if kind < 3 else sums[kind]
                    at = (kind * owned + fiber) * steps + group * SUB
                    weight_ref[at : at + SUB, :] = value
        count = weight_ref.shape[0] // steps
        weights = jnp.concatenate(
            [weight_ref[pl.ds(step, count, stride=steps), :] for step in range(steps)], axis=1
        )
        upper = weights.astype(jnp.bfloat16).astype(jnp.float32)
        both = jnp.concatenate([upper, weights - upper], axis=0).astype(jnp.bfloat16)
        moments = jnp.dot(both, split_ref[...], preferred_element_type=jnp.float32)
        moments = moments[:, 0:LANE] + moments[:, LANE:]
        moment_ref[0:count, :] = moments[0:count] + moments[count:]
        kinds = [moment_ref[kind * owned : kind * owned + SUB, :] for kind in range(5)]
        lane = lax.broadcasted_iota(jnp.int32, (SUB, LANE), 1)

        def three_kinds(one, two, three):
            return jnp.where(lane < KROWS, one, jnp.where(lane < 2 * KROWS, two, three))

        values = jnp.concatenate(
            [three_kinds(kinds[0], kinds[1], kinds[3]), three_kinds(kinds[1], kinds[2], kinds[4])],
            axis=0,
        )
        high = values.astype(jnp.bfloat16).astype(jnp.float32)
        values = jnp.concatenate([high, values - high], axis=0)
        system = jnp.dot(
            jnp.concatenate([values, values], axis=1).astype(jnp.bfloat16),
            map_ref[...],
            preferred_element_type=jnp.float32,
        )
        system = system[0 : 2 * SUB] + system[2 * SUB :]
        for second in range(2):
            for part in range(2):
                turned = system[second * SUB : (second + 1) * SUB, part * LANE : (part + 1) * LANE].T
                system_ref[second, part * LANE : (part + 1) * LANE, 0:SUB] = turned
        row = lax.broadcasted_iota(jnp.int32, (KROWS, LANE), 0)
        matrix = []
        for i in range(2 * K):
            second, at = divmod(i, K)
            value = system_ref[second, at * WIDTH : at * WIDTH + KROWS, :]
            matrix.append(jnp.where(row == i, 1.5 * value + 1.0, value))
        for pivot in range(2 * K):
            cut = KROWS - matrix[pivot].shape[0]
            inverse = 1.0 / matrix[pivot][pivot - cut : pivot - cut + 1]
            chosen = matrix[pivot] * inverse
            for i in range(2 * K):
                if i != pivot:
                    scale = matrix[i][pivot - cut : pivot - cut + 1]
                    matrix[i] = matrix[i] - scale * chosen
            matrix[pivot] = chosen
            if (pivot + 1) % SUB == 0:
                matrix = [item[SUB:] for item in matrix]
        for i in range(2 * K):
            cut = KROWS - matrix[i].shape[0]
            coef_ref[i : i + 1, :] = coef_ref[i : i + 1, :] + matrix[i][RHS - cut : RHS - cut + 1]
        return carry

    lax.fori_loop(0, ITERS, newton_step, 0)

    square_ref[...] = jnp.zeros_like(square_ref)
    lane = lax.broadcasted_iota(jnp.int32, (KROWS, LANE), 1)
    square_ref[0:KROWS, :] = jnp.where(lane < owned, coef_ref[...], 0.0)
    result = square_ref[...].T[0:owned]
    packed = result[0:1]
    for fiber in range(1, owned):
        packed = packed + pltpu.roll(result[fiber : fiber + 1], fiber * (LANE // owned), 1)
    send_ref[...] = jnp.broadcast_to(packed, send_ref.shape)


def fit(got, start, poly, split, owned, devices, height, sources):
    rows = got.shape[1]
    steps = got.shape[0] // (height * sources)
    count = -(-5 * owned // SUB) * SUB
    vmem = pl.BlockSpec(memory_space=pltpu.VMEM)
    return pl.pallas_call(
        functools.partial(fit_kernel, height, sources, owned),
        out_shape=jax.ShapeDtypeStruct((devices, LANE), jnp.float32),
        in_specs=[vmem] * 5,
        out_specs=vmem,
        scratch_shapes=[
            pltpu.VMEM((owned * PIX + owned, steps, rows), jnp.float32),
            pltpu.VMEM((count * steps, rows), jnp.float32),
            pltpu.VMEM((KROWS, LANE), jnp.float32),
            pltpu.VMEM((owned, KROWS, rows), jnp.float32),
            pltpu.VMEM((LANE, LANE), jnp.float32),
            pltpu.VMEM((count + SUB, LANE), jnp.float32),
            pltpu.VMEM((2, 2 * LANE, LANE), jnp.float32),
        ],
        compiler_params=pltpu.CompilerParams(vmem_limit_bytes=VMEM_BYTES),
        name="fit",
    )(got, start, poly, split, jnp.asarray(system_map()))


def residual_kernel(
    owned,
    coef_ref,
    local_ref,
    lit_ref,
    amp_ref,
    frames_ref,
    trace_hbm,
    width_hbm,
    image_hbm,
    trace_ref,
    width_ref,
    image_ref,
    shape_ref,
    bright_ref,
    small_sems,
    image_sems,
):
    lamps, rows, cols = frames_ref.shape
    me = lax.axis_index("rows") * lax.axis_size("fib") + lax.axis_index("fib")
    own = coef_ref[pl.ds(me, 1), :]
    each = LANE // owned
    for fiber in range(owned):
        at = fiber * each
        trace_ref[fiber : fiber + 1, :] = own[:, at : at + K]
        width_ref[fiber : fiber + 1, :] = own[:, at + K : at + 2 * K]
    leaving = start_copies([trace_ref, width_ref], [trace_hbm, width_hbm], small_sems)

    flipped = coef_ref[...].T
    coef = jnp.concatenate(
        [flipped[fiber * each : fiber * each + KROWS] for fiber in range(owned)], axis=1
    )
    centre = jnp.zeros((rows, coef.shape[1]), jnp.float32)
    spread = jnp.zeros((rows, coef.shape[1]), jnp.float32)
    for order in range(K):
        poly = jnp.concatenate([local_ref[order]] * (coef.shape[1] // LANE), axis=1)
        centre = centre + poly * coef[order : order + 1]
        spread = spread + poly * coef[K + order : K + order + 1]
    inverse = jnp.exp(-spread) * coef[RHS : RHS + 1]
    amp = amp_ref[...]
    pixel = (lax.broadcasted_iota(jnp.int32, (rows, LANE), 1) % PIX).astype(jnp.float32)
    offset = pixel - (PIX - 1) / 2.0
    for tile in range(cols // LANE):
        here = slice(tile * LANE, (tile + 1) * LANE)
        scaled = (offset - per_column(centre, tile, owned, True)) * per_column(
            inverse, tile, owned, True
        )
        shape_ref[:, here] = jnp.exp(-0.5 * scaled * scaled)
        bright = per_column(amp, tile, owned, False)
        for lamp in range(lamps):
            bright_ref[lamp, :, here] = bright[lamp : lamp + 1]

    def leave(lamp):
        return pltpu.make_async_copy(
            image_ref.at[lamp], image_hbm.at[lamp], image_sems.at[lamp]
        )

    def one_lamp(lamp, carry):
        lit = lit_ref[:, pl.ds(pl.multiple_of(lamp * LANE, LANE), LANE)]
        for tile in range(cols // LANE):
            here = slice(tile * LANE, (tile + 1) * LANE)
            weight = lit * bright_ref[lamp, :, here]
            frame = frames_ref[lamp, :, here].astype(jnp.float32)
            image_ref[lamp, :, here] = (frame - weight * shape_ref[:, here]).astype(jnp.bfloat16)
        leave(lamp).start()
        return carry

    lax.fori_loop(0, lamps, one_lamp, 0)
    for lamp in range(lamps):
        leave(lamp).wait()
    for copy in leaving:
        copy.wait()


def residual(owned, coef, local, lit, amplitude, frames):
    lamps, rows, cols = frames.shape
    vmem = pl.BlockSpec(memory_space=pltpu.VMEM)
    hbm = pl.BlockSpec(memory_space=pltpu.HBM)
    fitted = jax.ShapeDtypeStruct((owned, K), jnp.float32)
    return pl.pallas_call(
        functools.partial(residual_kernel, owned),
        out_shape=(fitted, fitted, jax.ShapeDtypeStruct(frames.shape, jnp.bfloat16)),
        in_specs=[vmem] * 5,
        out_specs=[hbm] * 3,
        scratch_shapes=[
            pltpu.VMEM((owned, K), jnp.float32),
            pltpu.VMEM((owned, K), jnp.float32),
            pltpu.VMEM(frames.shape, jnp.bfloat16),
            pltpu.VMEM((rows, cols), jnp.float32),
            pltpu.VMEM((lamps, 1, cols), jnp.float32),
            pltpu.SemaphoreType.DMA((2,)),
            pltpu.SemaphoreType.DMA((lamps,)),
        ],
        compiler_params=pltpu.CompilerParams(vmem_limit_bytes=VMEM_BYTES),
        name="residual",
    )(coef, local, lit, amplitude, frames)


def body(frames, amplitude, line_start, bundle_width, fiber_bundle, trace_coef, width_coef):
    sources = lax.axis_size("fib")
    devices = lax.axis_size("rows") * sources
    rows = frames.shape[1]
    owned = trace_coef.shape[0]
    height = owned * PIX + owned
    keep, send, lit, start = collapse(
        frames, amplitude, line_start, bundle_width, fiber_bundle, trace_coef, width_coef, height
    )
    came = lax.ppermute(send, "fib", [(index, index ^ 1) for index in range(sources)])
    poly, split, local = tables(start, rows)
    came, poly, split, local = lax.optimization_barrier((came, poly, split, local))
    alike = [[index for index in range(devices) if index % 2 == odd] for odd in range(2)]
    unit = 4 if height % 4 == 0 else 1
    got = lax.all_to_all(
        (keep + came).reshape(devices // 2, height // unit, unit, rows),
        BOTH,
        0,
        0,
        axis_index_groups=alike,
        tiled=True,
    ).reshape(devices // 2 * height, rows)
    reply = fit(got, start, poly, split, owned, devices, height, sources // 2)
    coef = lax.all_to_all(reply, BOTH, 0, 0, tiled=True)
    return residual(owned, coef, local, lit, amplitude, frames)


def solution(mesh):
    return jax.shard_map(
        body,
        mesh=mesh,
        in_specs=(
            P("fib", "rows", None),
            P("fib", None),
            P("fib", None),
            P(),
            P(),
            P(BOTH, None),
            P(BOTH, None),
        ),
        out_specs=(P(BOTH, None), P(BOTH, None), P("fib", "rows", None)),
        check_vma=False,
    )
```

```python
import functools
import math

import jax
import jax.numpy as jnp
import numpy as np
from jax import lax
from jax.experimental import pallas as pl
from jax.experimental.pallas import tpu as pltpu
from jax.sharding import PartitionSpec as P

K = 11
PIX = 8
WIN = 8
ITERS = 3
SUB = 8
LANE = 128
KROWS = 24
RHS = 2 * K
WIDTH = RHS + 1
ROOT = math.sqrt(0.5 / math.log(2.0))
VMEM_BYTES = 20 << 20

HIGH = lax.Precision.HIGHEST
BOTH = ("rows", "fib")


def adams_factor(order):
    value = 1.0
    for index in range(1, order + 1):
        value = value * (2.0 * index - 1.0) / index
    return value


def system_map():
    table = np.zeros((LANE, 2 * LANE))
    for i in range(K):
        table[2 * KROWS + i, i * WIDTH + RHS] = 1.0
        for j in range(K):
            for inner in range(min(i, j) + 1):
                target = i + j - 2 * inner
                value = adams_factor(inner) * adams_factor(i - inner) * adams_factor(j - inner)
                value = value / adams_factor(i + j - inner)
                value = value * (2.0 * target + 1.0) / (2.0 * (i + j - inner) + 1.0)
                table[target, i * WIDTH + j] += value
                table[KROWS + target, i * WIDTH + K + j] += value
    high = table.astype(jnp.bfloat16)
    low = (table - high.astype(np.float64)).astype(jnp.bfloat16)
    return np.concatenate([high, low], axis=0)


def legendre_list(rowpos, total, count):
    tvals = (2.0 * rowpos + 1.0) / total - 1.0
    polys = [jnp.ones_like(tvals), tvals]
    for order in range(1, count - 1):
        polys.append(
            ((2 * order + 1) * tvals * polys[order] - order * polys[order - 1]) / (order + 1)
        )
    return polys


def lit_by_lamp(start, first, rows):
    lamps, lines = start.shape
    rowid = first + lax.broadcasted_iota(jnp.int32, (lamps, rows), 1)
    lit = jnp.zeros((lamps, rows), jnp.float32)
    for line in range(lines):
        away = rowid - start[:, line : line + 1]
        lit = jnp.where((away >= 0) & (away < WIN), 1.0, lit)
    return lit


def lit_columns(lit):
    lamps, rows = lit.shape
    which = lax.broadcasted_iota(jnp.int32, (lamps, lamps * LANE), 1) // LANE
    own = lax.broadcasted_iota(jnp.int32, (lamps, lamps * LANE), 0)
    spread = jnp.where(which == own, 1.0, 0.0)
    return lax.dot_general(
        lit, spread, (((0,), (0,)), ((), ())), preferred_element_type=jnp.float32
    )


def take_lanes(values, index):
    parts = values.shape[1] // LANE
    result = None
    for part in range(parts):
        block = values[:, part * LANE : (part + 1) * LANE]
        taken = jnp.take_along_axis(block, index % LANE, axis=1, mode="promise_in_bounds")
        result = taken if result is None else jnp.where(index // LANE == part, taken, result)
    return result


def per_column(values, tile, owned, grouped):
    fiber = tile * (LANE // PIX) + (
        lax.broadcasted_iota(jnp.int32, (values.shape[0], LANE), 1) // PIX
    )
    if grouped:
        fiber = (fiber % owned) * (values.shape[1] // owned) + fiber // owned
    else:
        part = tile * (LANE // PIX) // LANE
        values = values[:, part * LANE : (part + 1) * LANE]
        fiber = fiber % LANE
    return take_lanes(values, fiber)


def start_copies(sources, targets, sems):
    copies = [
        pltpu.make_async_copy(source, target, sems.at[index])
        for index, (source, target) in enumerate(zip(sources, targets))
    ]
    for copy in copies:
        copy.start()
    return copies


def tables_kernel(after_ref, poly_ref, split_ref, local_ref):
    rows = poly_ref.shape[1]
    steps = poly_ref.shape[0] // KROWS

    rowpos = (
        lax.broadcasted_iota(jnp.int32, (steps, rows), 0) * rows
        + lax.broadcasted_iota(jnp.int32, (steps, rows), 1)
    ).astype(jnp.float32)
    polys = legendre_list(rowpos, steps * rows, 2 * K - 1)
    for order in range(KROWS):
        poly_ref[order * steps : (order + 1) * steps, :] = (
            polys[order] if order < 2 * K - 1 else jnp.zeros((steps, rows), jnp.float32)
        )

    spare = jnp.zeros((LANE - 3 * KROWS, rows), jnp.float32)
    for step in range(steps):
        stack = poly_ref[pl.ds(step, KROWS, stride=steps), :]
        high = stack.astype(jnp.bfloat16).astype(jnp.float32)
        for half, part in enumerate([high, stack - high]):
            split_ref[step * rows : (step + 1) * rows, half * LANE : (half + 1) * LANE] = (
                jnp.concatenate([part, part, part, spare], axis=0).T.astype(jnp.bfloat16)
            )

    first = lax.axis_index("rows") * rows
    here = (first + lax.broadcasted_iota(jnp.int32, (rows, LANE), 0)).astype(jnp.float32)
    for order, poly in enumerate(legendre_list(here, steps * rows, K)):
        local_ref[order] = poly


def tables(after, rows):
    steps = lax.axis_size("rows")
    shape = jax.ShapeDtypeStruct
    vmem = pl.BlockSpec(memory_space=pltpu.VMEM)
    size = 2 * LANE * steps * rows
    return pl.pallas_call(
        tables_kernel,
        out_shape=(
            shape((KROWS * steps, rows), jnp.float32),
            shape((steps * rows, 2 * LANE), jnp.bfloat16),
            shape((K, rows, LANE), jnp.float32),
        ),
        in_specs=[vmem],
        out_specs=[vmem] * 3,
        compiler_params=pltpu.CompilerParams(vmem_limit_bytes=VMEM_BYTES),
        cost_estimate=pl.CostEstimate(flops=8 * size, bytes_accessed=4 * size, transcendentals=0),
        name="tables",
    )(after)


def collapse_kernel(
    frames_hbm,
    amp_hbm,
    start_hbm,
    bundle_hbm,
    which_hbm,
    trace_hbm,
    width_hbm,
    keep_ref,
    send_ref,
    weight_ref,
    coef_ref,
    frames_ref,
    amp_ref,
    start_ref,
    bundle_ref,
    which_ref,
    trace_ref,
    width_ref,
    square_ref,
    small_sems,
    frame_sems,
):
    lamps, rows, cols = frames_ref.shape
    owned = trace_ref.shape[0]
    fibers = which_ref.shape[1]
    me = lax.axis_index("rows") * lax.axis_size("fib") + lax.axis_index("fib")
    first = lax.axis_index("rows") * rows
    odd = lax.axis_index("fib") % 2 == 1

    small = start_copies(
        [amp_hbm, start_hbm, bundle_hbm, which_hbm, trace_hbm, width_hbm],
        [amp_ref, start_ref, bundle_ref, which_ref, trace_ref, width_ref],
        small_sems,
    )
    arriving = start_copies([frames_hbm], [frames_ref], frame_sems)

    for copy in small:
        copy.wait()
    amp = amp_ref[...]
    lit = lit_by_lamp(start_ref[...], first, rows)
    columns = lit_columns(lit)
    for tile in range(cols // LANE):
        amp_cols = per_column(amp, tile, owned, False)
        for lamp in range(lamps):
            weight_ref[lamp, :, tile * LANE : (tile + 1) * LANE] = (
                columns[:, lamp * LANE : (lamp + 1) * LANE] * amp_cols[lamp : lamp + 1]
            )
    which = which_ref[...]
    bundles = bundle_ref[...]
    base = jnp.zeros((1, fibers), jnp.float32)
    for bundle in range(bundles.shape[1]):
        base = jnp.where(which == bundle, bundles[:, bundle : bundle + 1], base)
    inverse = 1.0 / base
    lane = lax.broadcasted_iota(jnp.int32, (1, fibers), 1)

    square_ref[...] = jnp.zeros_like(square_ref)
    square_ref[0:owned, 0:K] = trace_ref[...]
    square_ref[0:owned, K : 2 * K] = width_ref[...]
    for fiber in range(owned):
        square_ref[fiber : fiber + 1, RHS : RHS + 1] = jnp.sum(
            jnp.where(lane == me * owned + fiber, inverse, 0.0), axis=1, keepdims=True
        )
    coef_ref[...] = square_ref[...].T[0:KROWS]

    square = lax.dot_general(
        amp * amp, lit, (((0,), (0,)), ((), ())), precision=HIGH, preferred_element_type=jnp.float32
    )
    wide = owned * PIX

    height = wide + owned

    def place(block, offset, even_value, odd_value):
        at = slice(block * height + offset, block * height + offset + even_value.shape[0])
        keep_ref[at, :] = jnp.where(odd, odd_value, even_value)
        send_ref[at, :] = jnp.where(odd, even_value, odd_value)

    for block in range(fibers // (2 * owned)):
        low = 2 * block * owned
        place(
            block,
            wide,
            square[low : low + owned],
            square[low + owned : low + 2 * owned],
        )
    for copy in arriving:
        copy.wait()
    for tile in range(cols // LANE):
        at = slice(tile * LANE, (tile + 1) * LANE)
        total = jnp.zeros((rows, LANE), jnp.float32)
        for lamp in range(lamps):
            total = total + weight_ref[lamp, :, at] * frames_ref[lamp, :, at].astype(jnp.float32)
        flipped = total.T
        for pair in range(LANE // (2 * wide)):
            low = 2 * pair * wide
            place(
                tile * (LANE // (2 * wide)) + pair,
                0,
                flipped[low : low + wide],
                flipped[low + wide : low + 2 * wide],
            )


def collapse(
    frames, amplitude, line_start, bundle_width, fiber_bundle, trace_coef, width_coef, height
):
    lamps, rows, cols = frames.shape
    steps = lax.axis_size("rows")
    blocks = steps * lax.axis_size("fib") // 2
    args = (
        frames,
        amplitude,
        line_start,
        bundle_width.reshape(1, -1),
        fiber_bundle.reshape(1, -1),
        trace_coef,
        width_coef,
    )
    shape = jax.ShapeDtypeStruct
    outs = (
        shape((blocks * height, rows), jnp.float32),
        shape((blocks * height, rows), jnp.float32),
        shape((lamps, rows, cols), jnp.float32),
        shape((KROWS, LANE), jnp.float32),
    )
    return pl.pallas_call(
        collapse_kernel,
        out_shape=outs,
        in_specs=[pl.BlockSpec(memory_space=pltpu.HBM)] * len(args),
        out_specs=[pl.BlockSpec(memory_space=pltpu.VMEM)] * len(outs),
        scratch_shapes=[pltpu.VMEM(arg.shape, arg.dtype) for arg in args]
        + [
            pltpu.VMEM((LANE, LANE), jnp.float32),
            pltpu.SemaphoreType.DMA((len(args) - 1,)),
            pltpu.SemaphoreType.DMA((1,)),
        ],
        compiler_params=pltpu.CompilerParams(vmem_limit_bytes=VMEM_BYTES),
        name="collapse",
    )(*[pltpu.with_memory_space_constraint(arg, pltpu.HBM) for arg in args])


def fit_kernel(
    height,
    sources,
    owned,
    got_ref,
    start_ref,
    poly_ref,
    split_ref,
    map_ref,
    send_ref,
    sum_ref,
    weight_ref,
    coef_ref,
    splat_ref,
    square_ref,
    moment_ref,
    system_ref,
):
    wide = owned * PIX
    steps = got_ref.shape[0] // (height * sources)
    rows = got_ref.shape[1]
    used = wide + owned

    for group in range(steps // SUB):
        for item in range(used):
            value = None
            for source in range(sources):
                start = (group * SUB * sources + source) * height + item
                part = got_ref[pl.ds(start, SUB, stride=sources * height), :]
                value = part if value is None else value + part
            sum_ref[item, group * SUB : (group + 1) * SUB, :] = value

    coef_ref[...] = start_ref[...]
    weight_ref[...] = jnp.zeros_like(weight_ref)
    moment_ref[...] = jnp.zeros_like(moment_ref)
    system_ref[...] = jnp.zeros_like(system_ref)

    def newton_step(index, carry):
        for fiber in range(owned):
            splat_ref[fiber] = jnp.broadcast_to(
                coef_ref[:, fiber : fiber + 1], (KROWS, rows)
            )
        for group in range(steps // SUB):
            here = slice(group * SUB, (group + 1) * SUB)
            for fiber in range(owned):
                centre = jnp.zeros((SUB, rows), jnp.float32)
                spread = jnp.zeros((SUB, rows), jnp.float32)
                for order in range(K):
                    poly = poly_ref[order * steps + group * SUB : order * steps + (group + 1) * SUB, :]
                    centre = centre + splat_ref[fiber, order : order + 1, :] * poly
                    spread = spread + splat_ref[fiber, K + order : K + order + 1, :] * poly
                inverse = jnp.exp(-spread) * splat_ref[fiber, RHS : RHS + 1, :]
                reach = inverse * ROOT
                power = sum_ref[wide + fiber, here, :]
                sums = [jnp.zeros((SUB, rows), jnp.float32) for _ in range(5)]
                for pixel in range(PIX):
                    scaled = ((pixel - (PIX - 1) / 2.0) - centre) * reach
                    shape = jnp.exp2(-(scaled * scaled))
                    bend = shape * scaled
                    widen = bend * scaled
                    resid = sum_ref[fiber * PIX + pixel, here, :] - power * shape
                    sums[0] = sums[0] + bend * bend
                    sums[1] = sums[1] + bend * widen
                    sums[2] = sums[2] + widen * widen
                    sums[3] = sums[3] + resid * bend
                    sums[4] = sums[4] + resid * widen
                slant = inverse * (1.0 / ROOT)
                grow = 1.0 / (ROOT * ROOT)
                values = [
                    sums[0] * power * slant * slant,
                    sums[1] * power * slant * grow,
                    sums[2] * power * (grow * grow),
                    sums[3] * slant,
                    sums[4] * grow,
                ]
                for kind in range(5):
                    at = (kind * owned + fiber) * steps + group * SUB
                    weight_ref[at : at + SUB, :] = values[kind]
        count = weight_ref.shape[0] // steps
        weights = jnp.concatenate(
            [weight_ref[pl.ds(step, count, stride=steps), :] for step in range(steps)], axis=1
        )
        upper = weights.astype(jnp.bfloat16).astype(jnp.float32)
        both = jnp.concatenate([upper, weights - upper], axis=0).astype(jnp.bfloat16)
        moments = jnp.dot(both, split_ref[...], preferred_element_type=jnp.float32)
        moments = moments[:, 0:LANE] + moments[:, LANE:]
        moment_ref[0:count, :] = moments[0:count] + moments[count:]
        kinds = [moment_ref[kind * owned : kind * owned + SUB, :] for kind in range(5)]
        lane = lax.broadcasted_iota(jnp.int32, (SUB, LANE), 1)

        def three_kinds(one, two, three):
            return jnp.where(lane < KROWS, one, jnp.where(lane < 2 * KROWS, two, three))

        values = jnp.concatenate(
            [three_kinds(kinds[0], kinds[1], kinds[3]), three_kinds(kinds[1], kinds[2], kinds[4])],
            axis=0,
        )
        high = values.astype(jnp.bfloat16).astype(jnp.float32)
        values = jnp.concatenate([high, values - high], axis=0)
        system = jnp.dot(
            jnp.concatenate([values, values], axis=1).astype(jnp.bfloat16),
            map_ref[...],
            preferred_element_type=jnp.float32,
        )
        system = system[0 : 2 * SUB] + system[2 * SUB :]
        for second in range(2):
            for part in range(2):
                turned = system[second * SUB : (second + 1) * SUB, part * LANE : (part + 1) * LANE].T
                system_ref[second, part * LANE : (part + 1) * LANE, 0:SUB] = turned
        row = lax.broadcasted_iota(jnp.int32, (SUB, LANE), 0)
        matrix = []
        for i in range(2 * K):
            second, at = divmod(i, K)
            tiles = {}
            for tile in range(i // SUB, KROWS // SUB):
                start = at * WIDTH + tile * SUB
                tiles[tile] = system_ref[second, start : start + SUB, :]
            value = tiles[i // SUB]
            tiles[i // SUB] = jnp.where(row == i % SUB, 1.5 * value + 1.0, value)
            matrix.append(tiles)

        def entry(i, column):
            return matrix[i][column // SUB][column % SUB : column % SUB + 1]

        for pivot in range(2 * K):
            inverse = 1.0 / entry(pivot, pivot)
            chosen = {tile: value * inverse for tile, value in matrix[pivot].items()}
            for i in range(2 * K):
                if i == pivot:
                    continue
                scale = entry(pivot, i) if i > pivot else entry(i, pivot)
                for tile in range(max(i, pivot + 1) // SUB, KROWS // SUB):
                    matrix[i][tile] = matrix[i][tile] - scale * chosen[tile]
            matrix[pivot] = chosen
        for i in range(2 * K):
            coef_ref[i : i + 1, :] = coef_ref[i : i + 1, :] + entry(i, RHS)
        return carry

    lax.fori_loop(0, ITERS, newton_step, 0)

    square_ref[...] = jnp.zeros_like(square_ref)
    lane = lax.broadcasted_iota(jnp.int32, (KROWS, LANE), 1)
    square_ref[0:KROWS, :] = jnp.where(lane < owned, coef_ref[...], 0.0)
    result = square_ref[...].T[0:owned]
    packed = result[0:1]
    for fiber in range(1, owned):
        packed = packed + pltpu.roll(result[fiber : fiber + 1], fiber * (LANE // owned), 1)
    send_ref[...] = jnp.broadcast_to(packed, send_ref.shape)


def fit(got, start, poly, split, owned, devices, height, sources):
    rows = got.shape[1]
    steps = got.shape[0] // (height * sources)
    count = -(-5 * owned // SUB) * SUB
    vmem = pl.BlockSpec(memory_space=pltpu.VMEM)
    return pl.pallas_call(
        functools.partial(fit_kernel, height, sources, owned),
        out_shape=jax.ShapeDtypeStruct((devices, LANE), jnp.float32),
        in_specs=[vmem] * 5,
        out_specs=vmem,
        scratch_shapes=[
            pltpu.VMEM((owned * PIX + owned, steps, rows), jnp.float32),
            pltpu.VMEM((count * steps, rows), jnp.float32),
            pltpu.VMEM((KROWS, LANE), jnp.float32),
            pltpu.VMEM((owned, KROWS, rows), jnp.float32),
            pltpu.VMEM((LANE, LANE), jnp.float32),
            pltpu.VMEM((count + SUB, LANE), jnp.float32),
            pltpu.VMEM((2, 2 * LANE, LANE), jnp.float32),
        ],
        compiler_params=pltpu.CompilerParams(vmem_limit_bytes=VMEM_BYTES),
        name="fit",
    )(got, start, poly, split, jnp.asarray(system_map()))


def residual_kernel(
    owned,
    coef_ref,
    local_ref,
    weight_ref,
    frames_ref,
    trace_hbm,
    width_hbm,
    image_hbm,
    trace_ref,
    width_ref,
    image_ref,
    shape_ref,
    small_sems,
    image_sems,
):
    lamps, rows, cols = frames_ref.shape
    me = lax.axis_index("rows") * lax.axis_size("fib") + lax.axis_index("fib")
    own = coef_ref[pl.ds(me, 1), :]
    each = LANE // owned
    for fiber in range(owned):
        at = fiber * each
        trace_ref[fiber : fiber + 1, :] = own[:, at : at + K]
        width_ref[fiber : fiber + 1, :] = own[:, at + K : at + 2 * K]
    leaving = start_copies([trace_ref, width_ref], [trace_hbm, width_hbm], small_sems)

    flipped = coef_ref[...].T
    coef = jnp.concatenate(
        [flipped[fiber * each : fiber * each + KROWS] for fiber in range(owned)], axis=1
    )
    centre = jnp.zeros((rows, coef.shape[1]), jnp.float32)
    spread = jnp.zeros((rows, coef.shape[1]), jnp.float32)
    for order in range(K):
        poly = jnp.concatenate([local_ref[order]] * (coef.shape[1] // LANE), axis=1)
        centre = centre + poly * coef[order : order + 1]
        spread = spread + poly * coef[K + order : K + order + 1]
    inverse = jnp.exp(-spread) * coef[RHS : RHS + 1]
    pixel = (lax.broadcasted_iota(jnp.int32, (rows, LANE), 1) % PIX).astype(jnp.float32)
    offset = pixel - (PIX - 1) / 2.0
    for tile in range(cols // LANE):
        here = slice(tile * LANE, (tile + 1) * LANE)
        scaled = (offset - per_column(centre, tile, owned, True)) * per_column(
            inverse, tile, owned, True
        )
        shape_ref[:, here] = jnp.exp(-0.5 * scaled * scaled)

    def leave(lamp):
        return pltpu.make_async_copy(
            image_ref.at[lamp], image_hbm.at[lamp], image_sems.at[lamp]
        )

    def one_lamp(lamp, carry):
        for tile in range(cols // LANE):
            here = slice(tile * LANE, (tile + 1) * LANE)
            frame = frames_ref[lamp, :, here].astype(jnp.float32)
            model = weight_ref[lamp, :, here] * shape_ref[:, here]
            image_ref[lamp, :, here] = (frame - model).astype(jnp.bfloat16)
        leave(lamp).start()
        return carry

    lax.fori_loop(0, lamps, one_lamp, 0)
    for lamp in range(lamps):
        leave(lamp).wait()
    for copy in leaving:
        copy.wait()


def residual(owned, coef, local, weight, frames):
    lamps, rows, cols = frames.shape
    vmem = pl.BlockSpec(memory_space=pltpu.VMEM)
    hbm = pl.BlockSpec(memory_space=pltpu.HBM)
    fitted = jax.ShapeDtypeStruct((owned, K), jnp.float32)
    return pl.pallas_call(
        functools.partial(residual_kernel, owned),
        out_shape=(fitted, fitted, jax.ShapeDtypeStruct(frames.shape, jnp.bfloat16)),
        in_specs=[vmem] * 4,
        out_specs=[hbm] * 3,
        scratch_shapes=[
            pltpu.VMEM((owned, K), jnp.float32),
            pltpu.VMEM((owned, K), jnp.float32),
            pltpu.VMEM(frames.shape, jnp.bfloat16),
            pltpu.VMEM((rows, cols), jnp.float32),
            pltpu.SemaphoreType.DMA((2,)),
            pltpu.SemaphoreType.DMA((lamps,)),
        ],
        compiler_params=pltpu.CompilerParams(vmem_limit_bytes=VMEM_BYTES),
        name="residual",
    )(coef, local, weight, frames)


def body(frames, amplitude, line_start, bundle_width, fiber_bundle, trace_coef, width_coef):
    sources = lax.axis_size("fib")
    devices = lax.axis_size("rows") * sources
    rows = frames.shape[1]
    owned = trace_coef.shape[0]
    height = owned * PIX + owned
    keep, send, weight, start = collapse(
        frames, amplitude, line_start, bundle_width, fiber_bundle, trace_coef, width_coef, height
    )
    came = lax.ppermute(send, "fib", [(index, index ^ 1) for index in range(sources)])
    poly, split, local = tables(start, rows)
    came, poly, split, local = lax.optimization_barrier((came, poly, split, local))
    alike = [[index for index in range(devices) if index % 2 == odd] for odd in range(2)]
    unit = 4 if height % 4 == 0 else 1
    got = lax.all_to_all(
        (keep + came).reshape(devices // 2, height // unit, unit, rows),
        BOTH,
        0,
        0,
        axis_index_groups=alike,
        tiled=True,
    ).reshape(devices // 2 * height, rows)
    reply = fit(got, start, poly, split, owned, devices, height, sources // 2)
    coef = lax.all_to_all(reply, BOTH, 0, 0, tiled=True)
    return residual(owned, coef, local, weight, frames)


def solution(mesh):
    return jax.shard_map(
        body,
        mesh=mesh,
        in_specs=(
            P("fib", "rows", None),
            P("fib", None),
            P("fib", None),
            P(),
            P(),
            P(BOTH, None),
            P(BOTH, None),
        ),
        out_specs=(P(BOTH, None), P(BOTH, None), P("fib", "rows", None)),
        check_vma=False,
    )
```

```python
import functools
import math

import jax
import jax.numpy as jnp
import numpy as np
from jax import lax
from jax.experimental import pallas as pl
from jax.experimental.pallas import tpu as pltpu
from jax.sharding import PartitionSpec as P

K = 11
PIX = 8
WIN = 8
ITERS = 3
SUB = 8
LANE = 128
KROWS = 24
RHS = 2 * K
WIDTH = RHS + 1
READY = 2 * PIX + 6
ROOT = math.sqrt(0.5 / math.log(2.0))
VMEM_BYTES = 20 << 20

HIGH = lax.Precision.HIGHEST
BOTH = ("rows", "fib")


def adams_factor(order):
    value = 1.0
    for index in range(1, order + 1):
        value = value * (2.0 * index - 1.0) / index
    return value


def system_map():
    table = np.zeros((LANE, 2 * LANE))
    for i in range(K):
        table[2 * KROWS + i, i * WIDTH + RHS] = 1.0
        for j in range(K):
            for inner in range(min(i, j) + 1):
                target = i + j - 2 * inner
                value = adams_factor(inner) * adams_factor(i - inner) * adams_factor(j - inner)
                value = value / adams_factor(i + j - inner)
                value = value * (2.0 * target + 1.0) / (2.0 * (i + j - inner) + 1.0)
                table[target, i * WIDTH + j] += value
                table[KROWS + target, i * WIDTH + K + j] += value
    high = table.astype(jnp.bfloat16)
    low = (table - high.astype(np.float64)).astype(jnp.bfloat16)
    return np.concatenate([high, low], axis=0)


def legendre_list(rowpos, total, count):
    tvals = (2.0 * rowpos + 1.0) / total - 1.0
    polys = [jnp.ones_like(tvals), tvals]
    for order in range(1, count - 1):
        polys.append(
            ((2 * order + 1) * tvals * polys[order] - order * polys[order - 1]) / (order + 1)
        )
    return polys


def lit_by_lamp(start, first, rows):
    lamps, lines = start.shape
    rowid = first + lax.broadcasted_iota(jnp.int32, (lamps, rows), 1)
    lit = jnp.zeros((lamps, rows), jnp.float32)
    for line in range(lines):
        away = rowid - start[:, line : line + 1]
        lit = jnp.where((away >= 0) & (away < WIN), 1.0, lit)
    return lit


def lit_columns(lit):
    lamps, rows = lit.shape
    which = lax.broadcasted_iota(jnp.int32, (lamps, lamps * LANE), 1) // LANE
    own = lax.broadcasted_iota(jnp.int32, (lamps, lamps * LANE), 0)
    spread = jnp.where(which == own, 1.0, 0.0)
    return lax.dot_general(
        lit, spread, (((0,), (0,)), ((), ())), preferred_element_type=jnp.float32
    )


def take_lanes(values, index):
    parts = values.shape[1] // LANE
    result = None
    for part in range(parts):
        block = values[:, part * LANE : (part + 1) * LANE]
        taken = jnp.take_along_axis(block, index % LANE, axis=1, mode="promise_in_bounds")
        result = taken if result is None else jnp.where(index // LANE == part, taken, result)
    return result


def per_column(values, tile, owned, grouped):
    fiber = tile * (LANE // PIX) + (
        lax.broadcasted_iota(jnp.int32, (values.shape[0], LANE), 1) // PIX
    )
    if grouped:
        fiber = (fiber % owned) * (values.shape[1] // owned) + fiber // owned
    else:
        part = tile * (LANE // PIX) // LANE
        values = values[:, part * LANE : (part + 1) * LANE]
        fiber = fiber % LANE
    return take_lanes(values, fiber)


def start_copies(sources, targets, sems):
    copies = [
        pltpu.make_async_copy(source, target, sems.at[index])
        for index, (source, target) in enumerate(zip(sources, targets))
    ]
    for copy in copies:
        copy.start()
    return copies


def spread_coefficients(coef_ref, splat_ref):
    owned, _, rows = splat_ref.shape
    for fiber in range(owned):
        splat_ref[fiber] = jnp.broadcast_to(coef_ref[:, fiber : fiber + 1], (KROWS, rows))


def curves_of(poly_ref, splat_ref, fiber, group, steps):
    rows = poly_ref.shape[1]
    centre = jnp.zeros((SUB, rows), jnp.float32)
    spread = jnp.zeros((SUB, rows), jnp.float32)
    for order in range(K):
        poly = poly_ref[order * steps + group * SUB : order * steps + (group + 1) * SUB, :]
        centre = centre + splat_ref[fiber, order : order + 1, :] * poly
        spread = spread + splat_ref[fiber, K + order : K + order + 1, :] * poly
    return centre, jnp.exp(-spread) * splat_ref[fiber, RHS : RHS + 1, :]


def profile_at(pixel, centre, reach):
    scaled = ((pixel - (PIX - 1) / 2.0) - centre) * reach
    shape = jnp.exp2(-(scaled * scaled))
    bend = shape * scaled
    return shape, bend, bend * scaled


def store_weights(weight_ref, sums, power, slant, fiber, owned, group, steps):
    grow = 1.0 / (ROOT * ROOT)
    values = [
        sums[0] * power * slant * slant,
        sums[1] * power * slant * grow,
        sums[2] * power * (grow * grow),
        sums[3] * slant,
        sums[4] * grow,
    ]
    for kind in range(5):
        at = (kind * owned + fiber) * steps + group * SUB
        weight_ref[at : at + SUB, :] = values[kind]


def tables_kernel(coef_ref, poly_ref, split_ref, local_ref, ready_ref, splat_ref):
    rows = poly_ref.shape[1]
    steps = poly_ref.shape[0] // KROWS

    rowpos = (
        lax.broadcasted_iota(jnp.int32, (steps, rows), 0) * rows
        + lax.broadcasted_iota(jnp.int32, (steps, rows), 1)
    ).astype(jnp.float32)
    polys = legendre_list(rowpos, steps * rows, 2 * K - 1)
    for order in range(KROWS):
        poly_ref[order * steps : (order + 1) * steps, :] = (
            polys[order] if order < 2 * K - 1 else jnp.zeros((steps, rows), jnp.float32)
        )

    spare = jnp.zeros((LANE - 3 * KROWS, rows), jnp.float32)
    for step in range(steps):
        stack = poly_ref[pl.ds(step, KROWS, stride=steps), :]
        high = stack.astype(jnp.bfloat16).astype(jnp.float32)
        for half, part in enumerate([high, stack - high]):
            split_ref[step * rows : (step + 1) * rows, half * LANE : (half + 1) * LANE] = (
                jnp.concatenate([part, part, part, spare], axis=0).T.astype(jnp.bfloat16)
            )

    first = lax.axis_index("rows") * rows
    here = (first + lax.broadcasted_iota(jnp.int32, (rows, LANE), 0)).astype(jnp.float32)
    for order, poly in enumerate(legendre_list(here, steps * rows, K)):
        local_ref[order] = poly

    spread_coefficients(coef_ref, splat_ref)
    for group in range(steps // SUB):
        at = slice(group * SUB, (group + 1) * SUB)
        for fiber in range(splat_ref.shape[0]):
            centre, inverse = curves_of(poly_ref, splat_ref, fiber, group, steps)
            sums = [jnp.zeros((SUB, rows), jnp.float32) for _ in range(5)]
            for pixel in range(PIX):
                shape, bend, widen = profile_at(pixel, centre, inverse * ROOT)
                ready_ref[fiber, pixel, at, :] = bend
                ready_ref[fiber, PIX + pixel, at, :] = widen
                terms = [bend * bend, bend * widen, widen * widen, shape * bend, shape * widen]
                sums = [total + term for total, term in zip(sums, terms)]
            for index, total in enumerate(sums + [inverse * (1.0 / ROOT)]):
                ready_ref[fiber, 2 * PIX + index, at, :] = total


def tables(coef, owned, rows):
    steps = lax.axis_size("rows")
    shape = jax.ShapeDtypeStruct
    vmem = pl.BlockSpec(memory_space=pltpu.VMEM)
    size = 2 * LANE * steps * rows
    return pl.pallas_call(
        tables_kernel,
        out_shape=(
            shape((KROWS * steps, rows), jnp.float32),
            shape((steps * rows, 2 * LANE), jnp.bfloat16),
            shape((K, rows, LANE), jnp.float32),
            shape((owned, READY, steps, rows), jnp.float32),
        ),
        in_specs=[vmem],
        out_specs=[vmem] * 4,
        scratch_shapes=[pltpu.VMEM((owned, KROWS, rows), jnp.float32)],
        compiler_params=pltpu.CompilerParams(vmem_limit_bytes=VMEM_BYTES),
        cost_estimate=pl.CostEstimate(flops=8 * size, bytes_accessed=4 * size, transcendentals=0),
        name="tables",
    )(coef)


def collapse_kernel(
    frames_hbm,
    amp_hbm,
    start_hbm,
    bundle_hbm,
    which_hbm,
    trace_hbm,
    width_hbm,
    keep_ref,
    send_ref,
    weight_ref,
    coef_ref,
    frames_ref,
    amp_ref,
    start_ref,
    bundle_ref,
    which_ref,
    trace_ref,
    width_ref,
    square_ref,
    small_sems,
    frame_sems,
):
    lamps, rows, cols = frames_ref.shape
    owned = trace_ref.shape[0]
    fibers = which_ref.shape[1]
    me = lax.axis_index("rows") * lax.axis_size("fib") + lax.axis_index("fib")
    first = lax.axis_index("rows") * rows
    odd = lax.axis_index("fib") % 2 == 1

    small = start_copies(
        [amp_hbm, start_hbm, bundle_hbm, which_hbm, trace_hbm, width_hbm],
        [amp_ref, start_ref, bundle_ref, which_ref, trace_ref, width_ref],
        small_sems,
    )
    arriving = start_copies([frames_hbm], [frames_ref], frame_sems)

    for copy in small:
        copy.wait()
    amp = amp_ref[...]
    lit = lit_by_lamp(start_ref[...], first, rows)
    columns = lit_columns(lit)
    for tile in range(cols // LANE):
        amp_cols = per_column(amp, tile, owned, False)
        for lamp in range(lamps):
            weight_ref[lamp, :, tile * LANE : (tile + 1) * LANE] = (
                columns[:, lamp * LANE : (lamp + 1) * LANE] * amp_cols[lamp : lamp + 1]
            )
    which = which_ref[...]
    bundles = bundle_ref[...]
    base = jnp.zeros((1, fibers), jnp.float32)
    for bundle in range(bundles.shape[1]):
        base = jnp.where(which == bundle, bundles[:, bundle : bundle + 1], base)
    inverse = 1.0 / base
    lane = lax.broadcasted_iota(jnp.int32, (1, fibers), 1)

    square_ref[...] = jnp.zeros_like(square_ref)
    square_ref[0:owned, 0:K] = trace_ref[...]
    square_ref[0:owned, K : 2 * K] = width_ref[...]
    for fiber in range(owned):
        square_ref[fiber : fiber + 1, RHS : RHS + 1] = jnp.sum(
            jnp.where(lane == me * owned + fiber, inverse, 0.0), axis=1, keepdims=True
        )
    coef_ref[...] = square_ref[...].T[0:KROWS]

    square = lax.dot_general(
        amp * amp, lit, (((0,), (0,)), ((), ())), precision=HIGH, preferred_element_type=jnp.float32
    )
    wide = owned * PIX

    height = wide + owned

    def place(block, offset, even_value, odd_value):
        at = slice(block * height + offset, block * height + offset + even_value.shape[0])
        keep_ref[at, :] = jnp.where(odd, odd_value, even_value)
        send_ref[at, :] = jnp.where(odd, even_value, odd_value)

    for block in range(fibers // (2 * owned)):
        low = 2 * block * owned
        place(
            block,
            wide,
            square[low : low + owned],
            square[low + owned : low + 2 * owned],
        )
    for copy in arriving:
        copy.wait()
    for tile in range(cols // LANE):
        at = slice(tile * LANE, (tile + 1) * LANE)
        total = jnp.zeros((rows, LANE), jnp.float32)
        for lamp in range(lamps):
            total = total + weight_ref[lamp, :, at] * frames_ref[lamp, :, at].astype(jnp.float32)
        flipped = total.T
        for pair in range(LANE // (2 * wide)):
            low = 2 * pair * wide
            place(
                tile * (LANE // (2 * wide)) + pair,
                0,
                flipped[low : low + wide],
                flipped[low + wide : low + 2 * wide],
            )


def collapse(
    frames, amplitude, line_start, bundle_width, fiber_bundle, trace_coef, width_coef, height
):
    lamps, rows, cols = frames.shape
    steps = lax.axis_size("rows")
    blocks = steps * lax.axis_size("fib") // 2
    args = (
        frames,
        amplitude,
        line_start,
        bundle_width.reshape(1, -1),
        fiber_bundle.reshape(1, -1),
        trace_coef,
        width_coef,
    )
    shape = jax.ShapeDtypeStruct
    outs = (
        shape((blocks * height, rows), jnp.float32),
        shape((blocks * height, rows), jnp.float32),
        shape((lamps, rows, cols), jnp.float32),
        shape((KROWS, LANE), jnp.float32),
    )
    return pl.pallas_call(
        collapse_kernel,
        out_shape=outs,
        in_specs=[pl.BlockSpec(memory_space=pltpu.HBM)] * len(args),
        out_specs=[pl.BlockSpec(memory_space=pltpu.VMEM)] * len(outs),
        scratch_shapes=[pltpu.VMEM(arg.shape, arg.dtype) for arg in args]
        + [
            pltpu.VMEM((LANE, LANE), jnp.float32),
            pltpu.SemaphoreType.DMA((len(args) - 1,)),
            pltpu.SemaphoreType.DMA((1,)),
        ],
        compiler_params=pltpu.CompilerParams(vmem_limit_bytes=VMEM_BYTES),
        name="collapse",
    )(*[pltpu.with_memory_space_constraint(arg, pltpu.HBM) for arg in args])


def fit_kernel(
    height,
    sources,
    owned,
    got_ref,
    start_ref,
    poly_ref,
    split_ref,
    ready_ref,
    map_ref,
    send_ref,
    sum_ref,
    weight_ref,
    coef_ref,
    splat_ref,
    square_ref,
    moment_ref,
    system_ref,
):
    wide = owned * PIX
    steps = got_ref.shape[0] // (height * sources)
    rows = got_ref.shape[1]
    used = wide + owned

    for group in range(steps // SUB):
        for item in range(used):
            value = None
            for source in range(sources):
                start = (group * SUB * sources + source) * height + item
                part = got_ref[pl.ds(start, SUB, stride=sources * height), :]
                value = part if value is None else value + part
            sum_ref[item, group * SUB : (group + 1) * SUB, :] = value

    coef_ref[...] = start_ref[...]
    weight_ref[...] = jnp.zeros_like(weight_ref)
    moment_ref[...] = jnp.zeros_like(moment_ref)
    system_ref[...] = jnp.zeros_like(system_ref)

    def first_weights():
        for group in range(steps // SUB):
            here = slice(group * SUB, (group + 1) * SUB)
            for fiber in range(owned):
                power = sum_ref[wide + fiber, here, :]
                last = [ready_ref[fiber, 2 * PIX + index, here, :] for index in range(6)]
                sums = last[0:3] + [-(power * last[3]), -(power * last[4])]
                for pixel in range(PIX):
                    image = sum_ref[fiber * PIX + pixel, here, :]
                    sums[3] = sums[3] + image * ready_ref[fiber, pixel, here, :]
                    sums[4] = sums[4] + image * ready_ref[fiber, PIX + pixel, here, :]
                store_weights(weight_ref, sums, power, last[5], fiber, owned, group, steps)

    def later_weights():
        spread_coefficients(coef_ref, splat_ref)
        for group in range(steps // SUB):
            here = slice(group * SUB, (group + 1) * SUB)
            for fiber in range(owned):
                centre, inverse = curves_of(poly_ref, splat_ref, fiber, group, steps)
                power = sum_ref[wide + fiber, here, :]
                sums = [jnp.zeros((SUB, rows), jnp.float32) for _ in range(5)]
                for pixel in range(PIX):
                    shape, bend, widen = profile_at(pixel, centre, inverse * ROOT)
                    resid = sum_ref[fiber * PIX + pixel, here, :] - power * shape
                    terms = [bend * bend, bend * widen, widen * widen, resid * bend, resid * widen]
                    sums = [total + term for total, term in zip(sums, terms)]
                slant = inverse * (1.0 / ROOT)
                store_weights(weight_ref, sums, power, slant, fiber, owned, group, steps)

    def solve_step():
        count = weight_ref.shape[0] // steps
        weights = jnp.concatenate(
            [weight_ref[pl.ds(step, count, stride=steps), :] for step in range(steps)], axis=1
        )
        upper = weights.astype(jnp.bfloat16).astype(jnp.float32)
        both = jnp.concatenate([upper, weights - upper], axis=0).astype(jnp.bfloat16)
        moments = jnp.dot(both, split_ref[...], preferred_element_type=jnp.float32)
        moments = moments[:, 0:LANE] + moments[:, LANE:]
        moment_ref[0:count, :] = moments[0:count] + moments[count:]
        kinds = [moment_ref[kind * owned : kind * owned + SUB, :] for kind in range(5)]
        lane = lax.broadcasted_iota(jnp.int32, (SUB, LANE), 1)

        def three_kinds(one, two, three):
            return jnp.where(lane < KROWS, one, jnp.where(lane < 2 * KROWS, two, three))

        values = jnp.concatenate(
            [three_kinds(kinds[0], kinds[1], kinds[3]), three_kinds(kinds[1], kinds[2], kinds[4])],
            axis=0,
        )
        high = values.astype(jnp.bfloat16).astype(jnp.float32)
        values = jnp.concatenate([high, values - high], axis=0)
        system = jnp.dot(
            jnp.concatenate([values, values], axis=1).astype(jnp.bfloat16),
            map_ref[...],
            preferred_element_type=jnp.float32,
        )
        system = system[0 : 2 * SUB] + system[2 * SUB :]
        for second in range(2):
            for part in range(2):
                turned = system[second * SUB : (second + 1) * SUB, part * LANE : (part + 1) * LANE].T
                system_ref[second, part * LANE : (part + 1) * LANE, 0:SUB] = turned
        row = lax.broadcasted_iota(jnp.int32, (SUB, LANE), 0)
        matrix = []
        for i in range(2 * K):
            second, at = divmod(i, K)
            tiles = {}
            for tile in range(i // SUB, KROWS // SUB):
                start = at * WIDTH + tile * SUB
                tiles[tile] = system_ref[second, start : start + SUB, :]
            value = tiles[i // SUB]
            tiles[i // SUB] = jnp.where(row == i % SUB, 1.5 * value + 1.0, value)
            matrix.append(tiles)

        def entry(i, column):
            return matrix[i][column // SUB][column % SUB : column % SUB + 1]

        for pivot in range(2 * K):
            inverse = 1.0 / entry(pivot, pivot)
            chosen = {tile: value * inverse for tile, value in matrix[pivot].items()}
            for i in range(2 * K):
                if i == pivot:
                    continue
                scale = entry(pivot, i) if i > pivot else entry(i, pivot)
                for tile in range(max(i, pivot + 1) // SUB, KROWS // SUB):
                    matrix[i][tile] = matrix[i][tile] - scale * chosen[tile]
            matrix[pivot] = chosen
        for i in range(2 * K):
            coef_ref[i : i + 1, :] = coef_ref[i : i + 1, :] + entry(i, RHS)

    first_weights()
    solve_step()

    def later_step(index, carry):
        later_weights()
        solve_step()
        return carry

    lax.fori_loop(1, ITERS, later_step, 0)

    square_ref[...] = jnp.zeros_like(square_ref)
    lane = lax.broadcasted_iota(jnp.int32, (KROWS, LANE), 1)
    square_ref[0:KROWS, :] = jnp.where(lane < owned, coef_ref[...], 0.0)
    result = square_ref[...].T[0:owned]
    packed = result[0:1]
    for fiber in range(1, owned):
        packed = packed + pltpu.roll(result[fiber : fiber + 1], fiber * (LANE // owned), 1)
    send_ref[...] = jnp.broadcast_to(packed, send_ref.shape)


def fit(got, start, poly, split, ready, owned, devices, height, sources):
    rows = got.shape[1]
    steps = got.shape[0] // (height * sources)
    count = -(-5 * owned // SUB) * SUB
    vmem = pl.BlockSpec(memory_space=pltpu.VMEM)
    return pl.pallas_call(
        functools.partial(fit_kernel, height, sources, owned),
        out_shape=jax.ShapeDtypeStruct((devices, LANE), jnp.float32),
        in_specs=[vmem] * 6,
        out_specs=vmem,
        scratch_shapes=[
            pltpu.VMEM((owned * PIX + owned, steps, rows), jnp.float32),
            pltpu.VMEM((count * steps, rows), jnp.float32),
            pltpu.VMEM((KROWS, LANE), jnp.float32),
            pltpu.VMEM((owned, KROWS, rows), jnp.float32),
            pltpu.VMEM((LANE, LANE), jnp.float32),
            pltpu.VMEM((count + SUB, LANE), jnp.float32),
            pltpu.VMEM((2, 2 * LANE, LANE), jnp.float32),
        ],
        compiler_params=pltpu.CompilerParams(vmem_limit_bytes=VMEM_BYTES),
        name="fit",
    )(got, start, poly, split, ready, jnp.asarray(system_map()))


def residual_kernel(
    owned,
    coef_ref,
    local_ref,
    weight_ref,
    frames_ref,
    trace_hbm,
    width_hbm,
    image_hbm,
    trace_ref,
    width_ref,
    image_ref,
    shape_ref,
    small_sems,
    image_sems,
):
    lamps, rows, cols = frames_ref.shape
    me = lax.axis_index("rows") * lax.axis_size("fib") + lax.axis_index("fib")
    own = coef_ref[pl.ds(me, 1), :]
    each = LANE // owned
    for fiber in range(owned):
        at = fiber * each
        trace_ref[fiber : fiber + 1, :] = own[:, at : at + K]
        width_ref[fiber : fiber + 1, :] = own[:, at + K : at + 2 * K]
    leaving = start_copies([trace_ref, width_ref], [trace_hbm, width_hbm], small_sems)

    flipped = coef_ref[...].T
    coef = jnp.concatenate(
        [flipped[fiber * each : fiber * each + KROWS] for fiber in range(owned)], axis=1
    )
    centre = jnp.zeros((rows, coef.shape[1]), jnp.float32)
    spread = jnp.zeros((rows, coef.shape[1]), jnp.float32)
    for order in range(K):
        poly = jnp.concatenate([local_ref[order]] * (coef.shape[1] // LANE), axis=1)
        centre = centre + poly * coef[order : order + 1]
        spread = spread + poly * coef[K + order : K + order + 1]
    inverse = jnp.exp(-spread) * coef[RHS : RHS + 1]
    pixel = (lax.broadcasted_iota(jnp.int32, (rows, LANE), 1) % PIX).astype(jnp.float32)
    offset = pixel - (PIX - 1) / 2.0
    for tile in range(cols // LANE):
        here = slice(tile * LANE, (tile + 1) * LANE)
        scaled = (offset - per_column(centre, tile, owned, True)) * per_column(
            inverse, tile, owned, True
        )
        shape_ref[:, here] = jnp.exp(-0.5 * scaled * scaled)

    def leave(lamp):
        return pltpu.make_async_copy(
            image_ref.at[lamp], image_hbm.at[lamp], image_sems.at[lamp]
        )

    def one_lamp(lamp, carry):
        for tile in range(cols // LANE):
            here = slice(tile * LANE, (tile + 1) * LANE)
            frame = frames_ref[lamp, :, here].astype(jnp.float32)
            model = weight_ref[lamp, :, here] * shape_ref[:, here]
            image_ref[lamp, :, here] = (frame - model).astype(jnp.bfloat16)
        leave(lamp).start()
        return carry

    lax.fori_loop(0, lamps, one_lamp, 0)
    for lamp in range(lamps):
        leave(lamp).wait()
    for copy in leaving:
        copy.wait()


def residual(owned, coef, local, weight, frames):
    lamps, rows, cols = frames.shape
    vmem = pl.BlockSpec(memory_space=pltpu.VMEM)
    hbm = pl.BlockSpec(memory_space=pltpu.HBM)
    fitted = jax.ShapeDtypeStruct((owned, K), jnp.float32)
    return pl.pallas_call(
        functools.partial(residual_kernel, owned),
        out_shape=(fitted, fitted, jax.ShapeDtypeStruct(frames.shape, jnp.bfloat16)),
        in_specs=[vmem] * 4,
        out_specs=[hbm] * 3,
        scratch_shapes=[
            pltpu.VMEM((owned, K), jnp.float32),
            pltpu.VMEM((owned, K), jnp.float32),
            pltpu.VMEM(frames.shape, jnp.bfloat16),
            pltpu.VMEM((rows, cols), jnp.float32),
            pltpu.SemaphoreType.DMA((2,)),
            pltpu.SemaphoreType.DMA((lamps,)),
        ],
        compiler_params=pltpu.CompilerParams(vmem_limit_bytes=VMEM_BYTES),
        name="residual",
    )(coef, local, weight, frames)


def body(frames, amplitude, line_start, bundle_width, fiber_bundle, trace_coef, width_coef):
    sources = lax.axis_size("fib")
    devices = lax.axis_size("rows") * sources
    rows = frames.shape[1]
    owned = trace_coef.shape[0]
    height = owned * PIX + owned
    keep, send, weight, start = collapse(
        frames, amplitude, line_start, bundle_width, fiber_bundle, trace_coef, width_coef, height
    )
    came = lax.ppermute(send, "fib", [(index, index ^ 1) for index in range(sources)])
    poly, split, local, ready = tables(start, owned, rows)
    came, poly, split, local, ready = lax.optimization_barrier((came, poly, split, local, ready))
    alike = [[index for index in range(devices) if index % 2 == odd] for odd in range(2)]
    unit = 4 if height % 4 == 0 else 1
    got = lax.all_to_all(
        (keep + came).reshape(devices // 2, height // unit, unit, rows),
        BOTH,
        0,
        0,
        axis_index_groups=alike,
        tiled=True,
    ).reshape(devices // 2 * height, rows)
    reply = fit(got, start, poly, split, ready, owned, devices, height, sources // 2)
    coef = lax.all_to_all(reply, BOTH, 0, 0, tiled=True)
    return residual(owned, coef, local, weight, frames)


def solution(mesh):
    return jax.shard_map(
        body,
        mesh=mesh,
        in_specs=(
            P("fib", "rows", None),
            P("fib", None),
            P("fib", None),
            P(),
            P(),
            P(BOTH, None),
            P(BOTH, None),
        ),
        out_specs=(P(BOTH, None), P(BOTH, None), P("fib", "rows", None)),
        check_vma=False,
    )
```

```python
import functools
import math

import jax
import jax.numpy as jnp
import numpy as np
from jax import lax
from jax.experimental import pallas as pl
from jax.experimental.pallas import tpu as pltpu
from jax.sharding import PartitionSpec as P

K = 11
PIX = 8
WIN = 8
ITERS = 3
SUB = 8
LANE = 128
KROWS = 24
RHS = 2 * K
WIDTH = RHS + 1
EARLY = 2
READY = 2 * PIX + 6
ROOT = math.sqrt(0.5 / math.log(2.0))
VMEM_BYTES = 20 << 20

HIGH = lax.Precision.HIGHEST
BOTH = ("rows", "fib")


def adams_factor(order):
    value = 1.0
    for index in range(1, order + 1):
        value = value * (2.0 * index - 1.0) / index
    return value


def system_map():
    table = np.zeros((LANE, 2 * LANE))
    for i in range(K):
        table[2 * KROWS + i, i * WIDTH + RHS] = 1.0
        for j in range(K):
            for inner in range(min(i, j) + 1):
                target = i + j - 2 * inner
                value = adams_factor(inner) * adams_factor(i - inner) * adams_factor(j - inner)
                value = value / adams_factor(i + j - inner)
                value = value * (2.0 * target + 1.0) / (2.0 * (i + j - inner) + 1.0)
                table[target, i * WIDTH + j] += value
                table[KROWS + target, i * WIDTH + K + j] += value
    high = table.astype(jnp.bfloat16)
    low = (table - high.astype(np.float64)).astype(jnp.bfloat16)
    return np.concatenate([high, low], axis=0)


def legendre_list(rowpos, total, count):
    tvals = (2.0 * rowpos + 1.0) / total - 1.0
    polys = [jnp.ones_like(tvals), tvals]
    for order in range(1, count - 1):
        polys.append(
            ((2 * order + 1) * tvals * polys[order] - order * polys[order - 1]) / (order + 1)
        )
    return polys


def lit_by_lamp(start, first, rows):
    lamps, lines = start.shape
    rowid = first + lax.broadcasted_iota(jnp.int32, (lamps, rows), 1)
    lit = jnp.zeros((lamps, rows), jnp.float32)
    for line in range(lines):
        away = rowid - start[:, line : line + 1]
        lit = jnp.where((away >= 0) & (away < WIN), 1.0, lit)
    return lit


def lit_columns(lit):
    lamps, rows = lit.shape
    which = lax.broadcasted_iota(jnp.int32, (lamps, lamps * LANE), 1) // LANE
    own = lax.broadcasted_iota(jnp.int32, (lamps, lamps * LANE), 0)
    spread = jnp.where(which == own, 1.0, 0.0)
    return lax.dot_general(
        lit, spread, (((0,), (0,)), ((), ())), preferred_element_type=jnp.float32
    )


def take_lanes(values, index):
    parts = values.shape[1] // LANE
    result = None
    for part in range(parts):
        block = values[:, part * LANE : (part + 1) * LANE]
        taken = jnp.take_along_axis(block, index % LANE, axis=1, mode="promise_in_bounds")
        result = taken if result is None else jnp.where(index // LANE == part, taken, result)
    return result


def per_column(values, tile, owned, grouped):
    fiber = tile * (LANE // PIX) + (
        lax.broadcasted_iota(jnp.int32, (values.shape[0], LANE), 1) // PIX
    )
    if grouped:
        fiber = (fiber % owned) * (values.shape[1] // owned) + fiber // owned
    else:
        part = tile * (LANE // PIX) // LANE
        values = values[:, part * LANE : (part + 1) * LANE]
        fiber = fiber % LANE
    return take_lanes(values, fiber)


def start_copies(sources, targets, sems):
    copies = [
        pltpu.make_async_copy(source, target, sems.at[index])
        for index, (source, target) in enumerate(zip(sources, targets))
    ]
    for copy in copies:
        copy.start()
    return copies


def spread_coefficients(coef_ref, splat_ref):
    owned, _, rows = splat_ref.shape
    for fiber in range(owned):
        splat_ref[fiber] = jnp.broadcast_to(coef_ref[:, fiber : fiber + 1], (KROWS, rows))


def curves_of(poly_ref, splat_ref, fiber, group, steps):
    rows = poly_ref.shape[1]
    centre = jnp.zeros((SUB, rows), jnp.float32)
    spread = jnp.zeros((SUB, rows), jnp.float32)
    for order in range(K):
        poly = poly_ref[order * steps + group * SUB : order * steps + (group + 1) * SUB, :]
        centre = centre + splat_ref[fiber, order : order + 1, :] * poly
        spread = spread + splat_ref[fiber, K + order : K + order + 1, :] * poly
    return centre, jnp.exp(-spread) * splat_ref[fiber, RHS : RHS + 1, :]


def profile_at(pixel, centre, reach):
    scaled = ((pixel - (PIX - 1) / 2.0) - centre) * reach
    shape = jnp.exp2(-(scaled * scaled))
    bend = shape * scaled
    return shape, bend, bend * scaled


def store_weights(weight_ref, sums, power, slant, fiber, owned, group, steps):
    grow = 1.0 / (ROOT * ROOT)
    values = [
        sums[0] * power * slant * slant,
        sums[1] * power * slant * grow,
        sums[2] * power * (grow * grow),
        sums[3] * slant,
        sums[4] * grow,
    ]
    for kind in range(5):
        at = (kind * owned + fiber) * steps + group * SUB
        weight_ref[at : at + SUB, :] = values[kind]


def tables_kernel(coef_ref, poly_ref, split_ref, local_ref, ready_ref, splat_ref):
    rows = poly_ref.shape[1]
    steps = poly_ref.shape[0] // KROWS

    rowpos = (
        lax.broadcasted_iota(jnp.int32, (steps, rows), 0) * rows
        + lax.broadcasted_iota(jnp.int32, (steps, rows), 1)
    ).astype(jnp.float32)
    polys = legendre_list(rowpos, steps * rows, 2 * K - 1)
    for order in range(KROWS):
        poly_ref[order * steps : (order + 1) * steps, :] = (
            polys[order] if order < 2 * K - 1 else jnp.zeros((steps, rows), jnp.float32)
        )

    spare = jnp.zeros((LANE - 3 * KROWS, rows), jnp.float32)
    for step in range(steps):
        stack = poly_ref[pl.ds(step, KROWS, stride=steps), :]
        high = stack.astype(jnp.bfloat16).astype(jnp.float32)
        for half, part in enumerate([high, stack - high]):
            split_ref[step * rows : (step + 1) * rows, half * LANE : (half + 1) * LANE] = (
                jnp.concatenate([part, part, part, spare], axis=0).T.astype(jnp.bfloat16)
            )

    first = lax.axis_index("rows") * rows
    here = (first + lax.broadcasted_iota(jnp.int32, (rows, LANE), 0)).astype(jnp.float32)
    for order, poly in enumerate(legendre_list(here, steps * rows, K)):
        local_ref[order] = poly

    spread_coefficients(coef_ref, splat_ref)
    for group in range(steps // SUB):
        at = slice(group * SUB, (group + 1) * SUB)
        for fiber in range(splat_ref.shape[0]):
            centre, inverse = curves_of(poly_ref, splat_ref, fiber, group, steps)
            sums = [jnp.zeros((SUB, rows), jnp.float32) for _ in range(5)]
            for pixel in range(PIX):
                shape, bend, widen = profile_at(pixel, centre, inverse * ROOT)
                ready_ref[fiber, pixel, at, :] = bend
                ready_ref[fiber, PIX + pixel, at, :] = widen
                terms = [bend * bend, bend * widen, widen * widen, shape * bend, shape * widen]
                sums = [total + term for total, term in zip(sums, terms)]
            for index, total in enumerate(sums + [inverse * (1.0 / ROOT)]):
                ready_ref[fiber, 2 * PIX + index, at, :] = total


def tables(coef, owned, rows):
    steps = lax.axis_size("rows")
    shape = jax.ShapeDtypeStruct
    vmem = pl.BlockSpec(memory_space=pltpu.VMEM)
    size = 2 * LANE * steps * rows
    return pl.pallas_call(
        tables_kernel,
        out_shape=(
            shape((KROWS * steps, rows), jnp.float32),
            shape((steps * rows, 2 * LANE), jnp.bfloat16),
            shape((K, rows, LANE), jnp.float32),
            shape((owned, READY, steps, rows), jnp.float32),
        ),
        in_specs=[vmem],
        out_specs=[vmem] * 4,
        scratch_shapes=[pltpu.VMEM((owned, KROWS, rows), jnp.float32)],
        compiler_params=pltpu.CompilerParams(vmem_limit_bytes=VMEM_BYTES),
        cost_estimate=pl.CostEstimate(flops=8 * size, bytes_accessed=4 * size, transcendentals=0),
        name="tables",
    )(coef)


def collapse_kernel(
    frames_hbm,
    amp_hbm,
    start_hbm,
    bundle_hbm,
    which_hbm,
    trace_hbm,
    width_hbm,
    keep_ref,
    send_ref,
    weight_ref,
    coef_ref,
    frames_ref,
    amp_ref,
    start_ref,
    bundle_ref,
    which_ref,
    trace_ref,
    width_ref,
    square_ref,
    small_sems,
    frame_sems,
):
    lamps, rows, cols = frames_ref.shape
    owned = trace_ref.shape[0]
    fibers = which_ref.shape[1]
    me = lax.axis_index("rows") * lax.axis_size("fib") + lax.axis_index("fib")
    first = lax.axis_index("rows") * rows
    odd = lax.axis_index("fib") % 2 == 1

    small = start_copies(
        [amp_hbm, start_hbm, bundle_hbm, which_hbm, trace_hbm, width_hbm],
        [amp_ref, start_ref, bundle_ref, which_ref, trace_ref, width_ref],
        small_sems,
    )
    arriving = start_copies([frames_hbm], [frames_ref], frame_sems)

    for copy in small:
        copy.wait()
    amp = amp_ref[...]
    lit = lit_by_lamp(start_ref[...], first, rows)
    columns = lit_columns(lit)
    for tile in range(cols // LANE):
        amp_cols = per_column(amp, tile, owned, False)
        for lamp in range(lamps):
            weight_ref[lamp, :, tile * LANE : (tile + 1) * LANE] = (
                columns[:, lamp * LANE : (lamp + 1) * LANE] * amp_cols[lamp : lamp + 1]
            )
    which = which_ref[...]
    bundles = bundle_ref[...]
    base = jnp.zeros((1, fibers), jnp.float32)
    for bundle in range(bundles.shape[1]):
        base = jnp.where(which == bundle, bundles[:, bundle : bundle + 1], base)
    inverse = 1.0 / base
    lane = lax.broadcasted_iota(jnp.int32, (1, fibers), 1)

    square_ref[...] = jnp.zeros_like(square_ref)
    square_ref[0:owned, 0:K] = trace_ref[...]
    square_ref[0:owned, K : 2 * K] = width_ref[...]
    for fiber in range(owned):
        square_ref[fiber : fiber + 1, RHS : RHS + 1] = jnp.sum(
            jnp.where(lane == me * owned + fiber, inverse, 0.0), axis=1, keepdims=True
        )
    coef_ref[...] = square_ref[...].T[0:KROWS]

    square = lax.dot_general(
        amp * amp, lit, (((0,), (0,)), ((), ())), precision=HIGH, preferred_element_type=jnp.float32
    )
    wide = owned * PIX

    height = wide + owned

    def place(block, offset, even_value, odd_value):
        at = slice(block * height + offset, block * height + offset + even_value.shape[0])
        keep_ref[at, :] = jnp.where(odd, odd_value, even_value)
        send_ref[at, :] = jnp.where(odd, even_value, odd_value)

    for block in range(fibers // (2 * owned)):
        low = 2 * block * owned
        place(
            block,
            wide,
            square[low : low + owned],
            square[low + owned : low + 2 * owned],
        )
    for copy in arriving:
        copy.wait()
    for tile in range(cols // LANE):
        at = slice(tile * LANE, (tile + 1) * LANE)
        total = jnp.zeros((rows, LANE), jnp.float32)
        for lamp in range(lamps):
            total = total + weight_ref[lamp, :, at] * frames_ref[lamp, :, at].astype(jnp.float32)
        flipped = total.T
        for pair in range(LANE // (2 * wide)):
            low = 2 * pair * wide
            place(
                tile * (LANE // (2 * wide)) + pair,
                0,
                flipped[low : low + wide],
                flipped[low + wide : low + 2 * wide],
            )


def collapse(
    frames, amplitude, line_start, bundle_width, fiber_bundle, trace_coef, width_coef, height
):
    lamps, rows, cols = frames.shape
    steps = lax.axis_size("rows")
    blocks = steps * lax.axis_size("fib") // 2
    args = (
        frames,
        amplitude,
        line_start,
        bundle_width.reshape(1, -1),
        fiber_bundle.reshape(1, -1),
        trace_coef,
        width_coef,
    )
    shape = jax.ShapeDtypeStruct
    outs = (
        shape((blocks * height, rows), jnp.float32),
        shape((blocks * height, rows), jnp.float32),
        shape((lamps, rows, cols), jnp.float32),
        shape((KROWS, LANE), jnp.float32),
    )
    return pl.pallas_call(
        collapse_kernel,
        out_shape=outs,
        in_specs=[pl.BlockSpec(memory_space=pltpu.HBM)] * len(args),
        out_specs=[pl.BlockSpec(memory_space=pltpu.VMEM)] * len(outs),
        scratch_shapes=[pltpu.VMEM(arg.shape, arg.dtype) for arg in args]
        + [
            pltpu.VMEM((LANE, LANE), jnp.float32),
            pltpu.SemaphoreType.DMA((len(args) - 1,)),
            pltpu.SemaphoreType.DMA((1,)),
        ],
        compiler_params=pltpu.CompilerParams(vmem_limit_bytes=VMEM_BYTES),
        name="collapse",
    )(*[pltpu.with_memory_space_constraint(arg, pltpu.HBM) for arg in args])


def fit_kernel(
    height,
    sources,
    owned,
    got_ref,
    start_ref,
    poly_ref,
    split_ref,
    ready_ref,
    map_ref,
    send_ref,
    sum_ref,
    weight_ref,
    coef_ref,
    splat_ref,
    square_ref,
    moment_ref,
    system_ref,
):
    wide = owned * PIX
    steps = got_ref.shape[0] // (height * sources)
    rows = got_ref.shape[1]
    used = wide + owned

    for group in range(steps // SUB):
        for item in range(used):
            value = None
            for source in range(sources):
                start = (group * SUB * sources + source) * height + item
                part = got_ref[pl.ds(start, SUB, stride=sources * height), :]
                value = part if value is None else value + part
            sum_ref[item, group * SUB : (group + 1) * SUB, :] = value

    coef_ref[...] = start_ref[...]
    weight_ref[...] = jnp.zeros_like(weight_ref)
    moment_ref[...] = jnp.zeros_like(moment_ref)
    system_ref[...] = jnp.zeros_like(system_ref)

    def first_weights():
        for group in range(steps // SUB):
            here = slice(group * SUB, (group + 1) * SUB)
            for fiber in range(owned):
                power = sum_ref[wide + fiber, here, :]
                last = [ready_ref[fiber, 2 * PIX + index, here, :] for index in range(6)]
                sums = last[0:3] + [-(power * last[3]), -(power * last[4])]
                for pixel in range(PIX):
                    image = sum_ref[fiber * PIX + pixel, here, :]
                    sums[3] = sums[3] + image * ready_ref[fiber, pixel, here, :]
                    sums[4] = sums[4] + image * ready_ref[fiber, PIX + pixel, here, :]
                store_weights(weight_ref, sums, power, last[5], fiber, owned, group, steps)

    def later_weights():
        spread_coefficients(coef_ref, splat_ref)
        for group in range(steps // SUB):
            here = slice(group * SUB, (group + 1) * SUB)
            for fiber in range(owned):
                centre, inverse = curves_of(poly_ref, splat_ref, fiber, group, steps)
                power = sum_ref[wide + fiber, here, :]
                sums = [jnp.zeros((SUB, rows), jnp.float32) for _ in range(5)]
                for pixel in range(PIX):
                    shape, bend, widen = profile_at(pixel, centre, inverse * ROOT)
                    resid = sum_ref[fiber * PIX + pixel, here, :] - power * shape
                    terms = [bend * bend, bend * widen, widen * widen, resid * bend, resid * widen]
                    sums = [total + term for total, term in zip(sums, terms)]
                slant = inverse * (1.0 / ROOT)
                store_weights(weight_ref, sums, power, slant, fiber, owned, group, steps)

    def solve_step():
        count = weight_ref.shape[0] // steps
        weights = jnp.concatenate(
            [weight_ref[pl.ds(step, count, stride=steps), :] for step in range(steps)], axis=1
        )
        upper = weights.astype(jnp.bfloat16).astype(jnp.float32)
        both = jnp.concatenate([upper, weights - upper], axis=0).astype(jnp.bfloat16)
        moments = jnp.dot(both, split_ref[...], preferred_element_type=jnp.float32)
        moments = moments[:, 0:LANE] + moments[:, LANE:]
        moment_ref[0:count, :] = moments[0:count] + moments[count:]
        kinds = [moment_ref[kind * owned : kind * owned + SUB, :] for kind in range(5)]
        lane = lax.broadcasted_iota(jnp.int32, (SUB, LANE), 1)

        def three_kinds(one, two, three):
            return jnp.where(lane < KROWS, one, jnp.where(lane < 2 * KROWS, two, three))

        values = jnp.concatenate(
            [three_kinds(kinds[0], kinds[1], kinds[3]), three_kinds(kinds[1], kinds[2], kinds[4])],
            axis=0,
        )
        high = values.astype(jnp.bfloat16).astype(jnp.float32)
        values = jnp.concatenate([high, values - high], axis=0)
        system = jnp.dot(
            jnp.concatenate([values, values], axis=1).astype(jnp.bfloat16),
            map_ref[...],
            preferred_element_type=jnp.float32,
        )
        system = system[0 : 2 * SUB] + system[2 * SUB :]
        for second in range(2):
            for part in range(2):
                turned = system[second * SUB : (second + 1) * SUB, part * LANE : (part + 1) * LANE].T
                system_ref[second, part * LANE : (part + 1) * LANE, 0:SUB] = turned
        row = lax.broadcasted_iota(jnp.int32, (SUB, LANE), 0)
        matrix = []
        for i in range(2 * K):
            second, at = divmod(i, K)
            tiles = {}
            for tile in range(i // SUB, KROWS // SUB):
                start = at * WIDTH + tile * SUB
                tiles[tile] = system_ref[second, start : start + SUB, :]
            value = tiles[i // SUB]
            tiles[i // SUB] = jnp.where(row == i % SUB, 1.5 * value + 1.0, value)
            matrix.append(tiles)

        def entry(i, column):
            return matrix[i][column // SUB][column % SUB : column % SUB + 1]

        for pivot in range(2 * K):
            inverse = 1.0 / entry(pivot, pivot)
            chosen = {tile: value * inverse for tile, value in matrix[pivot].items()}
            for i in range(2 * K):
                if i == pivot:
                    continue
                scale = entry(pivot, i) if i > pivot else entry(i, pivot)
                for tile in range(max(i, pivot + 1) // SUB, KROWS // SUB):
                    matrix[i][tile] = matrix[i][tile] - scale * chosen[tile]
            matrix[pivot] = chosen
        for i in range(2 * K):
            coef_ref[i : i + 1, :] = coef_ref[i : i + 1, :] + entry(i, RHS)

    first_weights()
    solve_step()

    def later_step(index, carry):
        later_weights()
        solve_step()
        return carry

    lax.fori_loop(1, ITERS, later_step, 0)

    square_ref[...] = jnp.zeros_like(square_ref)
    lane = lax.broadcasted_iota(jnp.int32, (KROWS, LANE), 1)
    square_ref[0:KROWS, :] = jnp.where(lane < owned, coef_ref[...], 0.0)
    result = square_ref[...].T[0:owned]
    packed = result[0:1]
    for fiber in range(1, owned):
        packed = packed + pltpu.roll(result[fiber : fiber + 1], fiber * (LANE // owned), 1)
    send_ref[...] = jnp.broadcast_to(packed, send_ref.shape)


def fit(got, start, poly, split, ready, owned, devices, height, sources):
    rows = got.shape[1]
    steps = got.shape[0] // (height * sources)
    count = -(-5 * owned // SUB) * SUB
    vmem = pl.BlockSpec(memory_space=pltpu.VMEM)
    return pl.pallas_call(
        functools.partial(fit_kernel, height, sources, owned),
        out_shape=jax.ShapeDtypeStruct((devices, LANE), jnp.float32),
        in_specs=[vmem] * 6,
        out_specs=vmem,
        scratch_shapes=[
            pltpu.VMEM((owned * PIX + owned, steps, rows), jnp.float32),
            pltpu.VMEM((count * steps, rows), jnp.float32),
            pltpu.VMEM((KROWS, LANE), jnp.float32),
            pltpu.VMEM((owned, KROWS, rows), jnp.float32),
            pltpu.VMEM((LANE, LANE), jnp.float32),
            pltpu.VMEM((count + SUB, LANE), jnp.float32),
            pltpu.VMEM((2, 2 * LANE, LANE), jnp.float32),
        ],
        compiler_params=pltpu.CompilerParams(vmem_limit_bytes=VMEM_BYTES),
        name="fit",
    )(got, start, poly, split, ready, jnp.asarray(system_map()))


def residual_kernel(
    owned,
    coef_ref,
    local_ref,
    weight_ref,
    frames_ref,
    trace_hbm,
    width_hbm,
    image_hbm,
    trace_ref,
    width_ref,
    image_ref,
    shape_ref,
    small_sems,
    image_sems,
):
    lamps, rows, cols = frames_ref.shape
    me = lax.axis_index("rows") * lax.axis_size("fib") + lax.axis_index("fib")
    own = coef_ref[pl.ds(me, 1), :]
    each = LANE // owned
    for fiber in range(owned):
        at = fiber * each
        trace_ref[fiber : fiber + 1, :] = own[:, at : at + K]
        width_ref[fiber : fiber + 1, :] = own[:, at + K : at + 2 * K]
    leaving = start_copies([trace_ref, width_ref], [trace_hbm, width_hbm], small_sems)

    flipped = coef_ref[...].T
    coef = jnp.concatenate(
        [flipped[fiber * each : fiber * each + KROWS] for fiber in range(owned)], axis=1
    )
    centre = jnp.zeros((rows, coef.shape[1]), jnp.float32)
    spread = jnp.zeros((rows, coef.shape[1]), jnp.float32)
    for order in range(K):
        poly = jnp.concatenate([local_ref[order]] * (coef.shape[1] // LANE), axis=1)
        centre = centre + poly * coef[order : order + 1]
        spread = spread + poly * coef[K + order : K + order + 1]
    inverse = jnp.exp(-spread) * coef[RHS : RHS + 1]
    pixel = (lax.broadcasted_iota(jnp.int32, (rows, LANE), 1) % PIX).astype(jnp.float32)
    offset = pixel - (PIX - 1) / 2.0
    def leave(lamp):
        return pltpu.make_async_copy(
            image_ref.at[lamp], image_hbm.at[lamp], image_sems.at[lamp]
        )

    def finish(lamp, here, shape):
        frame = frames_ref[lamp, :, here].astype(jnp.float32)
        model = weight_ref[lamp, :, here] * shape
        image_ref[lamp, :, here] = (frame - model).astype(jnp.bfloat16)

    early = min(EARLY, lamps)
    for tile in range(cols // LANE):
        here = slice(tile * LANE, (tile + 1) * LANE)
        scaled = (offset - per_column(centre, tile, owned, True)) * per_column(
            inverse, tile, owned, True
        )
        shape = jnp.exp(-0.5 * scaled * scaled)
        shape_ref[:, here] = shape
        for lamp in range(early):
            finish(lamp, here, shape)
    for lamp in range(early):
        leave(lamp).start()

    def one_lamp(lamp, carry):
        for tile in range(cols // LANE):
            here = slice(tile * LANE, (tile + 1) * LANE)
            finish(lamp, here, shape_ref[:, here])
        leave(lamp).start()
        return carry

    lax.fori_loop(early, lamps, one_lamp, 0)
    for lamp in range(lamps):
        leave(lamp).wait()
    for copy in leaving:
        copy.wait()


def residual(owned, coef, local, weight, frames):
    lamps, rows, cols = frames.shape
    vmem = pl.BlockSpec(memory_space=pltpu.VMEM)
    hbm = pl.BlockSpec(memory_space=pltpu.HBM)
    fitted = jax.ShapeDtypeStruct((owned, K), jnp.float32)
    return pl.pallas_call(
        functools.partial(residual_kernel, owned),
        out_shape=(fitted, fitted, jax.ShapeDtypeStruct(frames.shape, jnp.bfloat16)),
        in_specs=[vmem] * 4,
        out_specs=[hbm] * 3,
        scratch_shapes=[
            pltpu.VMEM((owned, K), jnp.float32),
            pltpu.VMEM((owned, K), jnp.float32),
            pltpu.VMEM(frames.shape, jnp.bfloat16),
            pltpu.VMEM((rows, cols), jnp.float32),
            pltpu.SemaphoreType.DMA((2,)),
            pltpu.SemaphoreType.DMA((lamps,)),
        ],
        compiler_params=pltpu.CompilerParams(vmem_limit_bytes=VMEM_BYTES),
        name="residual",
    )(coef, local, weight, frames)


def body(frames, amplitude, line_start, bundle_width, fiber_bundle, trace_coef, width_coef):
    sources = lax.axis_size("fib")
    devices = lax.axis_size("rows") * sources
    rows = frames.shape[1]
    owned = trace_coef.shape[0]
    height = owned * PIX + owned
    keep, send, weight, start = collapse(
        frames, amplitude, line_start, bundle_width, fiber_bundle, trace_coef, width_coef, height
    )
    came = lax.ppermute(send, "fib", [(index, index ^ 1) for index in range(sources)])
    poly, split, local, ready = tables(start, owned, rows)
    came, poly, split, local, ready = lax.optimization_barrier((came, poly, split, local, ready))
    alike = [[index for index in range(devices) if index % 2 == odd] for odd in range(2)]
    unit = 4 if height % 4 == 0 else 1
    got = lax.all_to_all(
        (keep + came).reshape(devices // 2, height // unit, unit, rows),
        BOTH,
        0,
        0,
        axis_index_groups=alike,
        tiled=True,
    ).reshape(devices // 2 * height, rows)
    reply = fit(got, start, poly, split, ready, owned, devices, height, sources // 2)
    coef = lax.all_to_all(reply, BOTH, 0, 0, tiled=True)
    return residual(owned, coef, local, weight, frames)


def solution(mesh):
    return jax.shard_map(
        body,
        mesh=mesh,
        in_specs=(
            P("fib", "rows", None),
            P("fib", None),
            P("fib", None),
            P(),
            P(),
            P(BOTH, None),
            P(BOTH, None),
        ),
        out_specs=(P(BOTH, None), P(BOTH, None), P("fib", "rows", None)),
        check_vma=False,
    )
```

```python
import functools
import math

import jax
import jax.numpy as jnp
import numpy as np
from jax import lax
from jax.experimental import pallas as pl
from jax.experimental.pallas import tpu as pltpu
from jax.sharding import PartitionSpec as P

K = 11
PIX = 8
WIN = 8
ITERS = 3
SUB = 8
LANE = 128
KROWS = 24
RHS = 2 * K
WIDTH = RHS + 1
EARLY = 2
READY = 2 * PIX + 6
ROOT = math.sqrt(0.5 / math.log(2.0))
VMEM_BYTES = 20 << 20

HIGH = lax.Precision.HIGHEST
BOTH = ("rows", "fib")


def adams_factor(order):
    value = 1.0
    for index in range(1, order + 1):
        value = value * (2.0 * index - 1.0) / index
    return value


def system_map():
    table = np.zeros((LANE, 2 * LANE))
    for i in range(K):
        table[2 * KROWS + i, i * WIDTH + RHS] = 1.0
        for j in range(K):
            for inner in range(min(i, j) + 1):
                target = i + j - 2 * inner
                value = adams_factor(inner) * adams_factor(i - inner) * adams_factor(j - inner)
                value = value / adams_factor(i + j - inner)
                value = value * (2.0 * target + 1.0) / (2.0 * (i + j - inner) + 1.0)
                table[target, i * WIDTH + j] += value
                table[KROWS + target, i * WIDTH + K + j] += value
    high = table.astype(jnp.bfloat16)
    low = (table - high.astype(np.float64)).astype(jnp.bfloat16)
    return np.concatenate([high, low], axis=0)


def legendre_list(rowpos, total, count):
    tvals = (2.0 * rowpos + 1.0) / total - 1.0
    polys = [jnp.ones_like(tvals), tvals]
    for order in range(1, count - 1):
        polys.append(
            ((2 * order + 1) * tvals * polys[order] - order * polys[order - 1]) / (order + 1)
        )
    return polys


def lit_by_lamp(start, first, rows):
    lamps, lines = start.shape
    rowid = first + lax.broadcasted_iota(jnp.int32, (lamps, rows), 1)
    lit = jnp.zeros((lamps, rows), jnp.float32)
    for line in range(lines):
        away = rowid - start[:, line : line + 1]
        lit = jnp.where((away >= 0) & (away < WIN), 1.0, lit)
    return lit


def lit_columns(lit):
    lamps, rows = lit.shape
    which = lax.broadcasted_iota(jnp.int32, (lamps, lamps * LANE), 1) // LANE
    own = lax.broadcasted_iota(jnp.int32, (lamps, lamps * LANE), 0)
    spread = jnp.where(which == own, 1.0, 0.0)
    return lax.dot_general(
        lit, spread, (((0,), (0,)), ((), ())), preferred_element_type=jnp.float32
    )


def take_lanes(values, index):
    parts = values.shape[1] // LANE
    result = None
    for part in range(parts):
        block = values[:, part * LANE : (part + 1) * LANE]
        taken = jnp.take_along_axis(block, index % LANE, axis=1, mode="promise_in_bounds")
        result = taken if result is None else jnp.where(index // LANE == part, taken, result)
    return result


def per_column(values, tile, owned, grouped):
    fiber = tile * (LANE // PIX) + (
        lax.broadcasted_iota(jnp.int32, (values.shape[0], LANE), 1) // PIX
    )
    if grouped:
        fiber = (fiber % owned) * (values.shape[1] // owned) + fiber // owned
    else:
        part = tile * (LANE // PIX) // LANE
        values = values[:, part * LANE : (part + 1) * LANE]
        fiber = fiber % LANE
    return take_lanes(values, fiber)


def start_copies(sources, targets, sems):
    copies = [
        pltpu.make_async_copy(source, target, sems.at[index])
        for index, (source, target) in enumerate(zip(sources, targets))
    ]
    for copy in copies:
        copy.start()
    return copies


def spread_coefficients(coef_ref, splat_ref):
    owned, _, rows = splat_ref.shape
    for fiber in range(owned):
        splat_ref[fiber] = jnp.broadcast_to(coef_ref[:, fiber : fiber + 1], (KROWS, rows))


def curves_of(poly_ref, splat_ref, fiber, group, steps):
    rows = poly_ref.shape[1]
    centre = jnp.zeros((SUB, rows), jnp.float32)
    spread = jnp.zeros((SUB, rows), jnp.float32)
    for order in range(K):
        poly = poly_ref[order * steps + group * SUB : order * steps + (group + 1) * SUB, :]
        centre = centre + splat_ref[fiber, order : order + 1, :] * poly
        spread = spread + splat_ref[fiber, K + order : K + order + 1, :] * poly
    return centre, jnp.exp(-spread) * splat_ref[fiber, RHS : RHS + 1, :]


def profile_at(pixel, centre, reach):
    scaled = ((pixel - (PIX - 1) / 2.0) - centre) * reach
    shape = jnp.exp2(-(scaled * scaled))
    bend = shape * scaled
    return shape, bend, bend * scaled


def store_weights(weight_ref, sums, power, slant, fiber, owned, group, steps):
    grow = 1.0 / (ROOT * ROOT)
    values = [
        sums[0] * power * slant * slant,
        sums[1] * power * slant * grow,
        sums[2] * power * (grow * grow),
        sums[3] * slant,
        sums[4] * grow,
    ]
    for kind in range(5):
        at = (kind * owned + fiber) * steps + group * SUB
        weight_ref[at : at + SUB, :] = values[kind]


def tables_kernel(coef_ref, poly_ref, split_ref, local_ref, ready_ref, splat_ref):
    rows = poly_ref.shape[1]
    steps = poly_ref.shape[0] // KROWS

    rowpos = (
        (steps - 1 - lax.broadcasted_iota(jnp.int32, (steps, rows), 0)) * rows
        + lax.broadcasted_iota(jnp.int32, (steps, rows), 1)
    ).astype(jnp.float32)
    polys = legendre_list(rowpos, steps * rows, 2 * K - 1)
    for order in range(KROWS):
        poly_ref[order * steps : (order + 1) * steps, :] = (
            polys[order] if order < 2 * K - 1 else jnp.zeros((steps, rows), jnp.float32)
        )

    spare = jnp.zeros((LANE - 3 * KROWS, rows), jnp.float32)
    for step in range(steps):
        stack = poly_ref[pl.ds(step, KROWS, stride=steps), :]
        high = stack.astype(jnp.bfloat16).astype(jnp.float32)
        for half, part in enumerate([high, stack - high]):
            split_ref[step * rows : (step + 1) * rows, half * LANE : (half + 1) * LANE] = (
                jnp.concatenate([part, part, part, spare], axis=0).T.astype(jnp.bfloat16)
            )

    first = lax.axis_index("rows") * rows
    here = (first + lax.broadcasted_iota(jnp.int32, (rows, LANE), 0)).astype(jnp.float32)
    for order, poly in enumerate(legendre_list(here, steps * rows, K)):
        local_ref[order] = poly

    spread_coefficients(coef_ref, splat_ref)
    for group in range(steps // SUB):
        at = slice(group * SUB, (group + 1) * SUB)
        for fiber in range(splat_ref.shape[0]):
            centre, inverse = curves_of(poly_ref, splat_ref, fiber, group, steps)
            sums = [jnp.zeros((SUB, rows), jnp.float32) for _ in range(5)]
            for pixel in range(PIX):
                shape, bend, widen = profile_at(pixel, centre, inverse * ROOT)
                ready_ref[fiber, pixel, at, :] = bend
                ready_ref[fiber, PIX + pixel, at, :] = widen
                terms = [bend * bend, bend * widen, widen * widen, shape * bend, shape * widen]
                sums = [total + term for total, term in zip(sums, terms)]
            for index, total in enumerate(sums + [inverse * (1.0 / ROOT)]):
                ready_ref[fiber, 2 * PIX + index, at, :] = total


def tables(coef, owned, rows):
    steps = lax.axis_size("rows")
    shape = jax.ShapeDtypeStruct
    vmem = pl.BlockSpec(memory_space=pltpu.VMEM)
    size = 2 * LANE * steps * rows
    return pl.pallas_call(
        tables_kernel,
        out_shape=(
            shape((KROWS * steps, rows), jnp.float32),
            shape((steps * rows, 2 * LANE), jnp.bfloat16),
            shape((K, rows, LANE), jnp.float32),
            shape((owned, READY, steps, rows), jnp.float32),
        ),
        in_specs=[vmem],
        out_specs=[vmem] * 4,
        scratch_shapes=[pltpu.VMEM((owned, KROWS, rows), jnp.float32)],
        compiler_params=pltpu.CompilerParams(vmem_limit_bytes=VMEM_BYTES),
        cost_estimate=pl.CostEstimate(flops=8 * size, bytes_accessed=4 * size, transcendentals=0),
        name="tables",
    )(coef)


def collapse_kernel(
    frames_hbm,
    amp_hbm,
    start_hbm,
    bundle_hbm,
    which_hbm,
    trace_hbm,
    width_hbm,
    keep_ref,
    send_ref,
    weight_ref,
    coef_ref,
    frames_ref,
    amp_ref,
    start_ref,
    bundle_ref,
    which_ref,
    trace_ref,
    width_ref,
    square_ref,
    small_sems,
    frame_sems,
):
    lamps, rows, cols = frames_ref.shape
    owned = trace_ref.shape[0]
    fibers = which_ref.shape[1]
    me = lax.axis_index("rows") * lax.axis_size("fib") + lax.axis_index("fib")
    first = lax.axis_index("rows") * rows
    odd = lax.axis_index("fib") % 2 == 1

    small = start_copies(
        [amp_hbm, start_hbm, bundle_hbm, which_hbm, trace_hbm, width_hbm],
        [amp_ref, start_ref, bundle_ref, which_ref, trace_ref, width_ref],
        small_sems,
    )
    arriving = start_copies([frames_hbm], [frames_ref], frame_sems)

    for copy in small:
        copy.wait()
    amp = amp_ref[...]
    lit = lit_by_lamp(start_ref[...], first, rows)
    columns = lit_columns(lit)
    for tile in range(cols // LANE):
        amp_cols = per_column(amp, tile, owned, False)
        for lamp in range(lamps):
            weight_ref[lamp, :, tile * LANE : (tile + 1) * LANE] = (
                columns[:, lamp * LANE : (lamp + 1) * LANE] * amp_cols[lamp : lamp + 1]
            )
    which = which_ref[...]
    bundles = bundle_ref[...]
    base = jnp.zeros((1, fibers), jnp.float32)
    for bundle in range(bundles.shape[1]):
        base = jnp.where(which == bundle, bundles[:, bundle : bundle + 1], base)
    inverse = 1.0 / base
    lane = lax.broadcasted_iota(jnp.int32, (1, fibers), 1)

    square_ref[...] = jnp.zeros_like(square_ref)
    square_ref[0:owned, 0:K] = trace_ref[...]
    square_ref[0:owned, K : 2 * K] = width_ref[...]
    for fiber in range(owned):
        square_ref[fiber : fiber + 1, RHS : RHS + 1] = jnp.sum(
            jnp.where(lane == me * owned + fiber, inverse, 0.0), axis=1, keepdims=True
        )
    coef_ref[...] = square_ref[...].T[0:KROWS]

    square = lax.dot_general(
        amp * amp, lit, (((0,), (0,)), ((), ())), precision=HIGH, preferred_element_type=jnp.float32
    )
    wide = owned * PIX

    height = wide + owned

    def place(block, offset, even_value, odd_value):
        start = (fibers // (2 * owned) - 1 - block) * height + offset
        at = slice(start, start + even_value.shape[0])
        keep_ref[at, :] = jnp.where(odd, odd_value, even_value)
        send_ref[at, :] = jnp.where(odd, even_value, odd_value)

    for block in range(fibers // (2 * owned)):
        low = 2 * block * owned
        place(
            block,
            wide,
            square[low : low + owned],
            square[low + owned : low + 2 * owned],
        )
    for copy in arriving:
        copy.wait()
    for tile in range(cols // LANE):
        at = slice(tile * LANE, (tile + 1) * LANE)
        total = jnp.zeros((rows, LANE), jnp.float32)
        for lamp in range(lamps):
            total = total + weight_ref[lamp, :, at] * frames_ref[lamp, :, at].astype(jnp.float32)
        flipped = total.T
        for pair in range(LANE // (2 * wide)):
            low = 2 * pair * wide
            place(
                tile * (LANE // (2 * wide)) + pair,
                0,
                flipped[low : low + wide],
                flipped[low + wide : low + 2 * wide],
            )


def collapse(
    frames, amplitude, line_start, bundle_width, fiber_bundle, trace_coef, width_coef, height
):
    lamps, rows, cols = frames.shape
    steps = lax.axis_size("rows")
    blocks = steps * lax.axis_size("fib") // 2
    args = (
        frames,
        amplitude,
        line_start,
        bundle_width.reshape(1, -1),
        fiber_bundle.reshape(1, -1),
        trace_coef,
        width_coef,
    )
    shape = jax.ShapeDtypeStruct
    outs = (
        shape((blocks * height, rows), jnp.float32),
        shape((blocks * height, rows), jnp.float32),
        shape((lamps, rows, cols), jnp.float32),
        shape((KROWS, LANE), jnp.float32),
    )
    return pl.pallas_call(
        collapse_kernel,
        out_shape=outs,
        in_specs=[pl.BlockSpec(memory_space=pltpu.HBM)] * len(args),
        out_specs=[pl.BlockSpec(memory_space=pltpu.VMEM)] * len(outs),
        scratch_shapes=[pltpu.VMEM(arg.shape, arg.dtype) for arg in args]
        + [
            pltpu.VMEM((LANE, LANE), jnp.float32),
            pltpu.SemaphoreType.DMA((len(args) - 1,)),
            pltpu.SemaphoreType.DMA((1,)),
        ],
        compiler_params=pltpu.CompilerParams(vmem_limit_bytes=VMEM_BYTES),
        name="collapse",
    )(*[pltpu.with_memory_space_constraint(arg, pltpu.HBM) for arg in args])


def fit_kernel(
    height,
    sources,
    owned,
    got_ref,
    start_ref,
    poly_ref,
    split_ref,
    ready_ref,
    map_ref,
    send_ref,
    sum_ref,
    weight_ref,
    coef_ref,
    splat_ref,
    square_ref,
    moment_ref,
    system_ref,
):
    wide = owned * PIX
    steps = got_ref.shape[0] // (height * sources)
    rows = got_ref.shape[1]
    used = wide + owned

    for group in range(steps // SUB):
        for item in range(used):
            value = None
            for source in range(sources):
                start = (group * SUB * sources + source) * height + item
                part = got_ref[pl.ds(start, SUB, stride=sources * height), :]
                value = part if value is None else value + part
            sum_ref[item, group * SUB : (group + 1) * SUB, :] = value

    coef_ref[...] = start_ref[...]
    weight_ref[...] = jnp.zeros_like(weight_ref)
    moment_ref[...] = jnp.zeros_like(moment_ref)
    system_ref[...] = jnp.zeros_like(system_ref)

    def first_weights():
        for group in range(steps // SUB):
            here = slice(group * SUB, (group + 1) * SUB)
            for fiber in range(owned):
                power = sum_ref[wide + fiber, here, :]
                last = [ready_ref[fiber, 2 * PIX + index, here, :] for index in range(6)]
                sums = last[0:3] + [-(power * last[3]), -(power * last[4])]
                for pixel in range(PIX):
                    image = sum_ref[fiber * PIX + pixel, here, :]
                    sums[3] = sums[3] + image * ready_ref[fiber, pixel, here, :]
                    sums[4] = sums[4] + image * ready_ref[fiber, PIX + pixel, here, :]
                store_weights(weight_ref, sums, power, last[5], fiber, owned, group, steps)

    def later_weights():
        spread_coefficients(coef_ref, splat_ref)
        for group in range(steps // SUB):
            here = slice(group * SUB, (group + 1) * SUB)
            for fiber in range(owned):
                centre, inverse = curves_of(poly_ref, splat_ref, fiber, group, steps)
                power = sum_ref[wide + fiber, here, :]
                sums = [jnp.zeros((SUB, rows), jnp.float32) for _ in range(5)]
                for pixel in range(PIX):
                    shape, bend, widen = profile_at(pixel, centre, inverse * ROOT)
                    resid = sum_ref[fiber * PIX + pixel, here, :] - power * shape
                    terms = [bend * bend, bend * widen, widen * widen, resid * bend, resid * widen]
                    sums = [total + term for total, term in zip(sums, terms)]
                slant = inverse * (1.0 / ROOT)
                store_weights(weight_ref, sums, power, slant, fiber, owned, group, steps)

    def solve_step():
        count = weight_ref.shape[0] // steps
        weights = jnp.concatenate(
            [weight_ref[pl.ds(step, count, stride=steps), :] for step in range(steps)], axis=1
        )
        upper = weights.astype(jnp.bfloat16).astype(jnp.float32)
        both = jnp.concatenate([upper, weights - upper], axis=0).astype(jnp.bfloat16)
        moments = jnp.dot(both, split_ref[...], preferred_element_type=jnp.float32)
        moments = moments[:, 0:LANE] + moments[:, LANE:]
        moment_ref[0:count, :] = moments[0:count] + moments[count:]
        kinds = [moment_ref[kind * owned : kind * owned + SUB, :] for kind in range(5)]
        lane = lax.broadcasted_iota(jnp.int32, (SUB, LANE), 1)

        def three_kinds(one, two, three):
            return jnp.where(lane < KROWS, one, jnp.where(lane < 2 * KROWS, two, three))

        values = jnp.concatenate(
            [three_kinds(kinds[0], kinds[1], kinds[3]), three_kinds(kinds[1], kinds[2], kinds[4])],
            axis=0,
        )
        high = values.astype(jnp.bfloat16).astype(jnp.float32)
        values = jnp.concatenate([high, values - high], axis=0)
        system = jnp.dot(
            jnp.concatenate([values, values], axis=1).astype(jnp.bfloat16),
            map_ref[...],
            preferred_element_type=jnp.float32,
        )
        system = system[0 : 2 * SUB] + system[2 * SUB :]
        for second in range(2):
            for part in range(2):
                turned = system[second * SUB : (second + 1) * SUB, part * LANE : (part + 1) * LANE].T
                system_ref[second, part * LANE : (part + 1) * LANE, 0:SUB] = turned
        row = lax.broadcasted_iota(jnp.int32, (SUB, LANE), 0)
        matrix = []
        for i in range(2 * K):
            second, at = divmod(i, K)
            tiles = {}
            for tile in range(i // SUB, KROWS // SUB):
                start = at * WIDTH + tile * SUB
                tiles[tile] = system_ref[second, start : start + SUB, :]
            value = tiles[i // SUB]
            tiles[i // SUB] = jnp.where(row == i % SUB, 1.5 * value + 1.0, value)
            matrix.append(tiles)

        def entry(i, column):
            return matrix[i][column // SUB][column % SUB : column % SUB + 1]

        for pivot in range(2 * K):
            inverse = 1.0 / entry(pivot, pivot)
            chosen = {tile: value * inverse for tile, value in matrix[pivot].items()}
            for i in range(2 * K):
                if i == pivot:
                    continue
                scale = entry(pivot, i) if i > pivot else entry(i, pivot)
                for tile in range(max(i, pivot + 1) // SUB, KROWS // SUB):
                    matrix[i][tile] = matrix[i][tile] - scale * chosen[tile]
            matrix[pivot] = chosen
        for i in range(2 * K):
            coef_ref[i : i + 1, :] = coef_ref[i : i + 1, :] + entry(i, RHS)

    first_weights()
    solve_step()

    def later_step(index, carry):
        later_weights()
        solve_step()
        return carry

    lax.fori_loop(1, ITERS, later_step, 0)

    square_ref[...] = jnp.zeros_like(square_ref)
    lane = lax.broadcasted_iota(jnp.int32, (KROWS, LANE), 1)
    square_ref[0:KROWS, :] = jnp.where(lane < owned, coef_ref[...], 0.0)
    result = square_ref[...].T[0:owned]
    packed = result[0:1]
    for fiber in range(1, owned):
        packed = packed + pltpu.roll(result[fiber : fiber + 1], fiber * (LANE // owned), 1)
    send_ref[...] = jnp.broadcast_to(packed, send_ref.shape)


def fit(got, start, poly, split, ready, owned, devices, height, sources):
    rows = got.shape[1]
    steps = got.shape[0] // (height * sources)
    count = -(-5 * owned // SUB) * SUB
    vmem = pl.BlockSpec(memory_space=pltpu.VMEM)
    return pl.pallas_call(
        functools.partial(fit_kernel, height, sources, owned),
        out_shape=jax.ShapeDtypeStruct((devices, LANE), jnp.float32),
        in_specs=[vmem] * 6,
        out_specs=vmem,
        scratch_shapes=[
            pltpu.VMEM((owned * PIX + owned, steps, rows), jnp.float32),
            pltpu.VMEM((count * steps, rows), jnp.float32),
            pltpu.VMEM((KROWS, LANE), jnp.float32),
            pltpu.VMEM((owned, KROWS, rows), jnp.float32),
            pltpu.VMEM((LANE, LANE), jnp.float32),
            pltpu.VMEM((count + SUB, LANE), jnp.float32),
            pltpu.VMEM((2, 2 * LANE, LANE), jnp.float32),
        ],
        compiler_params=pltpu.CompilerParams(vmem_limit_bytes=VMEM_BYTES),
        name="fit",
    )(got, start, poly, split, ready, jnp.asarray(system_map()))


def residual_kernel(
    owned,
    coef_ref,
    local_ref,
    weight_ref,
    frames_ref,
    trace_hbm,
    width_hbm,
    image_hbm,
    trace_ref,
    width_ref,
    image_ref,
    shape_ref,
    small_sems,
    image_sems,
):
    lamps, rows, cols = frames_ref.shape
    me = lax.axis_index("rows") * lax.axis_size("fib") + lax.axis_index("fib")
    own = coef_ref[pl.ds(me, 1), :]
    each = LANE // owned
    for fiber in range(owned):
        at = fiber * each
        trace_ref[fiber : fiber + 1, :] = own[:, at : at + K]
        width_ref[fiber : fiber + 1, :] = own[:, at + K : at + 2 * K]
    leaving = start_copies([trace_ref, width_ref], [trace_hbm, width_hbm], small_sems)

    flipped = coef_ref[...].T
    coef = jnp.concatenate(
        [flipped[fiber * each : fiber * each + KROWS] for fiber in range(owned)], axis=1
    )
    centre = jnp.zeros((rows, coef.shape[1]), jnp.float32)
    spread = jnp.zeros((rows, coef.shape[1]), jnp.float32)
    for order in range(K):
        poly = jnp.concatenate([local_ref[order]] * (coef.shape[1] // LANE), axis=1)
        centre = centre + poly * coef[order : order + 1]
        spread = spread + poly * coef[K + order : K + order + 1]
    inverse = jnp.exp(-spread) * coef[RHS : RHS + 1]
    pixel = (lax.broadcasted_iota(jnp.int32, (rows, LANE), 1) % PIX).astype(jnp.float32)
    offset = pixel - (PIX - 1) / 2.0
    def leave(lamp):
        return pltpu.make_async_copy(
            image_ref.at[lamp], image_hbm.at[lamp], image_sems.at[lamp]
        )

    def finish(lamp, here, shape):
        frame = frames_ref[lamp, :, here].astype(jnp.float32)
        model = weight_ref[lamp, :, here] * shape
        image_ref[lamp, :, here] = (frame - model).astype(jnp.bfloat16)

    early = min(EARLY, lamps)
    for tile in range(cols // LANE):
        here = slice(tile * LANE, (tile + 1) * LANE)
        scaled = (offset - per_column(centre, tile, owned, True)) * per_column(
            inverse, tile, owned, True
        )
        shape = jnp.exp(-0.5 * scaled * scaled)
        shape_ref[:, here] = shape
        for lamp in range(early):
            finish(lamp, here, shape)
    for lamp in range(early):
        leave(lamp).start()

    def one_lamp(lamp, carry):
        for tile in range(cols // LANE):
            here = slice(tile * LANE, (tile + 1) * LANE)
            finish(lamp, here, shape_ref[:, here])
        leave(lamp).start()
        return carry

    lax.fori_loop(early, lamps, one_lamp, 0)
    for lamp in range(lamps):
        leave(lamp).wait()
    for copy in leaving:
        copy.wait()


def residual(owned, coef, local, weight, frames):
    lamps, rows, cols = frames.shape
    vmem = pl.BlockSpec(memory_space=pltpu.VMEM)
    hbm = pl.BlockSpec(memory_space=pltpu.HBM)
    fitted = jax.ShapeDtypeStruct((owned, K), jnp.float32)
    return pl.pallas_call(
        functools.partial(residual_kernel, owned),
        out_shape=(fitted, fitted, jax.ShapeDtypeStruct(frames.shape, jnp.bfloat16)),
        in_specs=[vmem] * 4,
        out_specs=[hbm] * 3,
        scratch_shapes=[
            pltpu.VMEM((owned, K), jnp.float32),
            pltpu.VMEM((owned, K), jnp.float32),
            pltpu.VMEM(frames.shape, jnp.bfloat16),
            pltpu.VMEM((rows, cols), jnp.float32),
            pltpu.SemaphoreType.DMA((2,)),
            pltpu.SemaphoreType.DMA((lamps,)),
        ],
        compiler_params=pltpu.CompilerParams(vmem_limit_bytes=VMEM_BYTES),
        name="residual",
    )(coef, local, weight, frames)


def body(frames, amplitude, line_start, bundle_width, fiber_bundle, trace_coef, width_coef):
    sources = lax.axis_size("fib")
    devices = lax.axis_size("rows") * sources
    rows = frames.shape[1]
    owned = trace_coef.shape[0]
    height = owned * PIX + owned
    keep, send, weight, start = collapse(
        frames, amplitude, line_start, bundle_width, fiber_bundle, trace_coef, width_coef, height
    )
    came = lax.ppermute(send, "fib", [(index, index ^ 1) for index in range(sources)])
    poly, split, local, ready = tables(start, owned, rows)
    came, poly, split, local, ready = lax.optimization_barrier((came, poly, split, local, ready))
    alike = [
        [index for index in reversed(range(devices)) if index % 2 == odd] for odd in range(2)
    ]
    unit = 4 if height % 4 == 0 else 1
    got = lax.all_to_all(
        (keep + came).reshape(devices // 2, height // unit, unit, rows),
        BOTH,
        0,
        0,
        axis_index_groups=alike,
        tiled=True,
    ).reshape(devices // 2 * height, rows)
    reply = fit(got, start, poly, split, ready, owned, devices, height, sources // 2)
    coef = lax.all_to_all(reply, BOTH, 0, 0, tiled=True)
    return residual(owned, coef, local, weight, frames)


def solution(mesh):
    return jax.shard_map(
        body,
        mesh=mesh,
        in_specs=(
            P("fib", "rows", None),
            P("fib", None),
            P("fib", None),
            P(),
            P(),
            P(BOTH, None),
            P(BOTH, None),
        ),
        out_specs=(P(BOTH, None), P(BOTH, None), P("fib", "rows", None)),
        check_vma=False,
    )
```

```python
import functools
import math

import jax
import jax.numpy as jnp
import numpy as np
from jax import lax
from jax.experimental import pallas as pl
from jax.experimental.pallas import tpu as pltpu
from jax.sharding import PartitionSpec as P

K = 11
PIX = 8
WIN = 8
ITERS = 3
SUB = 8
LANE = 128
KROWS = 24
RHS = 2 * K
WIDTH = RHS + 1
EARLY = 2
READY = 2 * PIX + 6
ROOT = math.sqrt(0.5 / math.log(2.0))
VMEM_BYTES = 20 << 20

HIGH = lax.Precision.HIGHEST
BOTH = ("rows", "fib")


def adams_factor(order):
    value = 1.0
    for index in range(1, order + 1):
        value = value * (2.0 * index - 1.0) / index
    return value


def system_map():
    table = np.zeros((LANE, 2 * LANE))
    for i in range(K):
        table[2 * KROWS + i, i * WIDTH + RHS] = 1.0
        for j in range(K):
            for inner in range(min(i, j) + 1):
                target = i + j - 2 * inner
                value = adams_factor(inner) * adams_factor(i - inner) * adams_factor(j - inner)
                value = value / adams_factor(i + j - inner)
                value = value * (2.0 * target + 1.0) / (2.0 * (i + j - inner) + 1.0)
                table[target, i * WIDTH + j] += value
                table[KROWS + target, i * WIDTH + K + j] += value
    high = table.astype(jnp.bfloat16)
    low = (table - high.astype(np.float64)).astype(jnp.bfloat16)
    return np.concatenate([high, low], axis=0)


def legendre_list(rowpos, total, count):
    tvals = (2.0 * rowpos + 1.0) / total - 1.0
    polys = [jnp.ones_like(tvals), tvals]
    for order in range(1, count - 1):
        polys.append(
            ((2 * order + 1) * tvals * polys[order] - order * polys[order - 1]) / (order + 1)
        )
    return polys


def lit_by_lamp(start, first, rows):
    lamps, lines = start.shape
    rowid = first + lax.broadcasted_iota(jnp.int32, (lamps, rows), 1)
    lit = jnp.zeros((lamps, rows), jnp.float32)
    for line in range(lines):
        away = rowid - start[:, line : line + 1]
        lit = jnp.where((away >= 0) & (away < WIN), 1.0, lit)
    return lit


def lit_columns(lit):
    lamps, rows = lit.shape
    which = lax.broadcasted_iota(jnp.int32, (lamps, lamps * LANE), 1) // LANE
    own = lax.broadcasted_iota(jnp.int32, (lamps, lamps * LANE), 0)
    spread = jnp.where(which == own, 1.0, 0.0)
    return lax.dot_general(
        lit, spread, (((0,), (0,)), ((), ())), preferred_element_type=jnp.float32
    )


def take_lanes(values, index):
    parts = values.shape[1] // LANE
    result = None
    for part in range(parts):
        block = values[:, part * LANE : (part + 1) * LANE]
        taken = jnp.take_along_axis(block, index % LANE, axis=1, mode="promise_in_bounds")
        result = taken if result is None else jnp.where(index // LANE == part, taken, result)
    return result


def per_column(values, tile, owned, grouped):
    fiber = tile * (LANE // PIX) + (
        lax.broadcasted_iota(jnp.int32, (values.shape[0], LANE), 1) // PIX
    )
    if grouped:
        fiber = (fiber % owned) * (values.shape[1] // owned) + fiber // owned
    else:
        part = tile * (LANE // PIX) // LANE
        values = values[:, part * LANE : (part + 1) * LANE]
        fiber = fiber % LANE
    return take_lanes(values, fiber)


def start_copies(sources, targets, sems):
    copies = [
        pltpu.make_async_copy(source, target, sems.at[index])
        for index, (source, target) in enumerate(zip(sources, targets))
    ]
    for copy in copies:
        copy.start()
    return copies


def spread_coefficients(coef_ref, splat_ref):
    owned, _, rows = splat_ref.shape
    for fiber in range(owned):
        splat_ref[fiber] = jnp.broadcast_to(coef_ref[:, fiber : fiber + 1], (KROWS, rows))


def curves_of(poly_ref, splat_ref, fiber, group, steps):
    rows = poly_ref.shape[1]
    centre = jnp.zeros((SUB, rows), jnp.float32)
    spread = jnp.zeros((SUB, rows), jnp.float32)
    for order in range(K):
        poly = poly_ref[order * steps + group * SUB : order * steps + (group + 1) * SUB, :]
        centre = centre + splat_ref[fiber, order : order + 1, :] * poly
        spread = spread + splat_ref[fiber, K + order : K + order + 1, :] * poly
    return centre, jnp.exp(-spread) * splat_ref[fiber, RHS : RHS + 1, :]


def profile_at(pixel, centre, reach):
    scaled = ((pixel - (PIX - 1) / 2.0) - centre) * reach
    shape = jnp.exp2(-(scaled * scaled))
    bend = shape * scaled
    return shape, bend, bend * scaled


def store_weights(weight_ref, sums, power, slant, fiber, owned, group, steps):
    grow = 1.0 / (ROOT * ROOT)
    values = [
        sums[0] * power * slant * slant,
        sums[1] * power * slant * grow,
        sums[2] * power * (grow * grow),
        sums[3] * slant,
        sums[4] * grow,
    ]
    for kind in range(5):
        at = (kind * owned + fiber) * steps + group * SUB
        weight_ref[at : at + SUB, :] = values[kind]


def tables_kernel(coef_ref, poly_ref, split_ref, local_ref, ready_ref, splat_ref):
    rows = poly_ref.shape[1]
    steps = poly_ref.shape[0] // KROWS

    rowpos = (
        (steps - 1 - lax.broadcasted_iota(jnp.int32, (steps, rows), 0)) * rows
        + lax.broadcasted_iota(jnp.int32, (steps, rows), 1)
    ).astype(jnp.float32)
    polys = legendre_list(rowpos, steps * rows, 2 * K - 1)
    for order in range(KROWS):
        poly_ref[order * steps : (order + 1) * steps, :] = (
            polys[order] if order < 2 * K - 1 else jnp.zeros((steps, rows), jnp.float32)
        )

    spare = jnp.zeros((LANE - 3 * KROWS, rows), jnp.float32)
    for step in range(steps):
        stack = poly_ref[pl.ds(step, KROWS, stride=steps), :]
        high = stack.astype(jnp.bfloat16).astype(jnp.float32)
        for half, part in enumerate([high, stack - high]):
            split_ref[step * rows : (step + 1) * rows, half * LANE : (half + 1) * LANE] = (
                jnp.concatenate([part, part, part, spare], axis=0).T.astype(jnp.bfloat16)
            )

    first = lax.axis_index("rows") * rows
    here = (first + lax.broadcasted_iota(jnp.int32, (rows, LANE), 0)).astype(jnp.float32)
    for order, poly in enumerate(legendre_list(here, steps * rows, K)):
        local_ref[order] = poly

    spread_coefficients(coef_ref, splat_ref)
    for group in range(steps // SUB):
        at = slice(group * SUB, (group + 1) * SUB)
        for fiber in range(splat_ref.shape[0]):
            centre, inverse = curves_of(poly_ref, splat_ref, fiber, group, steps)
            sums = [jnp.zeros((SUB, rows), jnp.float32) for _ in range(5)]
            for pixel in range(PIX):
                shape, bend, widen = profile_at(pixel, centre, inverse * ROOT)
                ready_ref[fiber, pixel, at, :] = bend
                ready_ref[fiber, PIX + pixel, at, :] = widen
                terms = [bend * bend, bend * widen, widen * widen, shape * bend, shape * widen]
                sums = [total + term for total, term in zip(sums, terms)]
            for index, total in enumerate(sums + [inverse * (1.0 / ROOT)]):
                ready_ref[fiber, 2 * PIX + index, at, :] = total


def tables(coef, owned, rows):
    steps = lax.axis_size("rows")
    shape = jax.ShapeDtypeStruct
    vmem = pl.BlockSpec(memory_space=pltpu.VMEM)
    size = 2 * LANE * steps * rows
    return pl.pallas_call(
        tables_kernel,
        out_shape=(
            shape((KROWS * steps, rows), jnp.float32),
            shape((steps * rows, 2 * LANE), jnp.bfloat16),
            shape((K, rows, LANE), jnp.float32),
            shape((owned, READY, steps, rows), jnp.float32),
        ),
        in_specs=[vmem],
        out_specs=[vmem] * 4,
        scratch_shapes=[pltpu.VMEM((owned, KROWS, rows), jnp.float32)],
        compiler_params=pltpu.CompilerParams(vmem_limit_bytes=VMEM_BYTES),
        cost_estimate=pl.CostEstimate(flops=8 * size, bytes_accessed=4 * size, transcendentals=0),
        name="tables",
    )(coef)


def collapse_kernel(
    frames_hbm,
    amp_hbm,
    start_hbm,
    bundle_hbm,
    which_hbm,
    trace_hbm,
    width_hbm,
    keep_ref,
    send_ref,
    weight_ref,
    coef_ref,
    frames_ref,
    amp_ref,
    start_ref,
    bundle_ref,
    which_ref,
    trace_ref,
    width_ref,
    square_ref,
    small_sems,
    frame_sems,
):
    lamps, rows, cols = frames_ref.shape
    owned = trace_ref.shape[0]
    fibers = which_ref.shape[1]
    me = lax.axis_index("rows") * lax.axis_size("fib") + lax.axis_index("fib")
    first = lax.axis_index("rows") * rows
    odd = lax.axis_index("fib") % 2 == 1

    small = start_copies(
        [amp_hbm, start_hbm, bundle_hbm, which_hbm, trace_hbm, width_hbm],
        [amp_ref, start_ref, bundle_ref, which_ref, trace_ref, width_ref],
        small_sems,
    )
    arriving = start_copies([frames_hbm], [frames_ref], frame_sems)

    for copy in small:
        copy.wait()
    amp = amp_ref[...]
    lit = lit_by_lamp(start_ref[...], first, rows)
    columns = lit_columns(lit)
    for tile in range(cols // LANE):
        amp_cols = per_column(amp, tile, owned, False)
        for lamp in range(lamps):
            weight_ref[lamp, :, tile * LANE : (tile + 1) * LANE] = (
                columns[:, lamp * LANE : (lamp + 1) * LANE] * amp_cols[lamp : lamp + 1]
            )
    which = which_ref[...]
    bundles = bundle_ref[...]
    base = jnp.zeros((1, fibers), jnp.float32)
    for bundle in range(bundles.shape[1]):
        base = jnp.where(which == bundle, bundles[:, bundle : bundle + 1], base)
    inverse = 1.0 / base
    lane = lax.broadcasted_iota(jnp.int32, (1, fibers), 1)

    square_ref[...] = jnp.zeros_like(square_ref)
    square_ref[0:owned, 0:K] = trace_ref[...]
    square_ref[0:owned, K : 2 * K] = width_ref[...]
    for fiber in range(owned):
        square_ref[fiber : fiber + 1, RHS : RHS + 1] = jnp.sum(
            jnp.where(lane == me * owned + fiber, inverse, 0.0), axis=1, keepdims=True
        )
    coef_ref[...] = square_ref[...].T[0:KROWS]

    square = lax.dot_general(
        amp * amp, lit, (((0,), (0,)), ((), ())), precision=HIGH, preferred_element_type=jnp.float32
    )
    wide = owned * PIX

    height = wide + owned

    def place(block, offset, even_value, odd_value):
        start = (fibers // (2 * owned) - 1 - block) * height + offset
        at = slice(start, start + even_value.shape[0])
        keep_ref[at, :] = jnp.where(odd, odd_value, even_value)
        send_ref[at, :] = jnp.where(odd, even_value, odd_value)

    for block in range(fibers // (2 * owned)):
        low = 2 * block * owned
        place(
            block,
            wide,
            square[low : low + owned],
            square[low + owned : low + 2 * owned],
        )
    for copy in arriving:
        copy.wait()
    for tile in range(cols // LANE):
        at = slice(tile * LANE, (tile + 1) * LANE)
        total = jnp.zeros((rows, LANE), jnp.float32)
        for lamp in range(lamps):
            total = total + weight_ref[lamp, :, at] * frames_ref[lamp, :, at].astype(jnp.float32)
        flipped = total.T
        for pair in range(LANE // (2 * wide)):
            low = 2 * pair * wide
            place(
                tile * (LANE // (2 * wide)) + pair,
                0,
                flipped[low : low + wide],
                flipped[low + wide : low + 2 * wide],
            )


def collapse(
    frames, amplitude, line_start, bundle_width, fiber_bundle, trace_coef, width_coef, height
):
    lamps, rows, cols = frames.shape
    steps = lax.axis_size("rows")
    blocks = steps * lax.axis_size("fib") // 2
    args = (
        frames,
        amplitude,
        line_start,
        bundle_width.reshape(1, -1),
        fiber_bundle.reshape(1, -1),
        trace_coef,
        width_coef,
    )
    shape = jax.ShapeDtypeStruct
    outs = (
        shape((blocks * height, rows), jnp.float32),
        shape((blocks * height, rows), jnp.float32),
        shape((lamps, rows, cols), jnp.float32),
        shape((KROWS, LANE), jnp.float32),
    )
    return pl.pallas_call(
        collapse_kernel,
        out_shape=outs,
        in_specs=[pl.BlockSpec(memory_space=pltpu.HBM)] * len(args),
        out_specs=[pl.BlockSpec(memory_space=pltpu.VMEM)] * len(outs),
        scratch_shapes=[pltpu.VMEM(arg.shape, arg.dtype) for arg in args]
        + [
            pltpu.VMEM((LANE, LANE), jnp.float32),
            pltpu.SemaphoreType.DMA((len(args) - 1,)),
            pltpu.SemaphoreType.DMA((1,)),
        ],
        compiler_params=pltpu.CompilerParams(vmem_limit_bytes=VMEM_BYTES),
        name="collapse",
    )(*[pltpu.with_memory_space_constraint(arg, pltpu.HBM) for arg in args])


def fit_kernel(
    height,
    sources,
    owned,
    got_ref,
    start_ref,
    poly_ref,
    split_ref,
    ready_ref,
    map_ref,
    send_ref,
    sum_ref,
    weight_ref,
    coef_ref,
    splat_ref,
    square_ref,
    moment_ref,
    system_ref,
):
    wide = owned * PIX
    steps = got_ref.shape[0] // (height * sources)
    rows = got_ref.shape[1]
    used = wide + owned

    for group in range(steps // SUB):
        for item in range(used):
            value = None
            for source in range(sources):
                start = (group * SUB * sources + source) * height + item
                part = got_ref[pl.ds(start, SUB, stride=sources * height), :]
                value = part if value is None else value + part
            sum_ref[item, group * SUB : (group + 1) * SUB, :] = value

    coef_ref[...] = start_ref[...]
    weight_ref[...] = jnp.zeros_like(weight_ref)
    moment_ref[...] = jnp.zeros_like(moment_ref)
    system_ref[...] = jnp.zeros_like(system_ref)

    def first_weights():
        for group in range(steps // SUB):
            here = slice(group * SUB, (group + 1) * SUB)
            for fiber in range(owned):
                power = sum_ref[wide + fiber, here, :]
                last = [ready_ref[fiber, 2 * PIX + index, here, :] for index in range(6)]
                sums = last[0:3] + [-(power * last[3]), -(power * last[4])]
                for pixel in range(PIX):
                    image = sum_ref[fiber * PIX + pixel, here, :]
                    sums[3] = sums[3] + image * ready_ref[fiber, pixel, here, :]
                    sums[4] = sums[4] + image * ready_ref[fiber, PIX + pixel, here, :]
                store_weights(weight_ref, sums, power, last[5], fiber, owned, group, steps)

    def later_weights():
        spread_coefficients(coef_ref, splat_ref)
        for group in range(steps // SUB):
            here = slice(group * SUB, (group + 1) * SUB)
            for fiber in range(owned):
                centre, inverse = curves_of(poly_ref, splat_ref, fiber, group, steps)
                power = sum_ref[wide + fiber, here, :]
                sums = [jnp.zeros((SUB, rows), jnp.float32) for _ in range(5)]
                for pixel in range(PIX):
                    shape, bend, widen = profile_at(pixel, centre, inverse * ROOT)
                    resid = sum_ref[fiber * PIX + pixel, here, :] - power * shape
                    terms = [bend * bend, bend * widen, widen * widen, resid * bend, resid * widen]
                    sums = [total + term for total, term in zip(sums, terms)]
                slant = inverse * (1.0 / ROOT)
                store_weights(weight_ref, sums, power, slant, fiber, owned, group, steps)

    def solve_step():
        count = weight_ref.shape[0] // steps
        weights = jnp.concatenate(
            [weight_ref[pl.ds(step, count, stride=steps), :] for step in range(steps)], axis=1
        )
        upper = weights.astype(jnp.bfloat16).astype(jnp.float32)
        both = jnp.concatenate([upper, weights - upper], axis=0).astype(jnp.bfloat16)
        moments = jnp.dot(both, split_ref[...], preferred_element_type=jnp.float32)
        moments = moments[:, 0:LANE] + moments[:, LANE:]
        moment_ref[0:count, :] = moments[0:count] + moments[count:]
        kinds = [moment_ref[kind * owned : kind * owned + SUB, :] for kind in range(5)]
        lane = lax.broadcasted_iota(jnp.int32, (SUB, LANE), 1)

        def three_kinds(one, two, three):
            return jnp.where(lane < KROWS, one, jnp.where(lane < 2 * KROWS, two, three))

        values = jnp.concatenate(
            [three_kinds(kinds[0], kinds[1], kinds[3]), three_kinds(kinds[1], kinds[2], kinds[4])],
            axis=0,
        )
        high = values.astype(jnp.bfloat16).astype(jnp.float32)
        values = jnp.concatenate([high, values - high], axis=0)
        system = jnp.dot(
            jnp.concatenate([values, values], axis=1).astype(jnp.bfloat16),
            map_ref[...],
            preferred_element_type=jnp.float32,
        )
        system = system[0 : 2 * SUB] + system[2 * SUB :]
        for second in range(2):
            for part in range(2):
                turned = system[second * SUB : (second + 1) * SUB, part * LANE : (part + 1) * LANE].T
                system_ref[second, part * LANE : (part + 1) * LANE, 0:SUB] = turned
        row = lax.broadcasted_iota(jnp.int32, (SUB, LANE), 0)
        matrix = []
        for i in range(2 * K):
            second, at = divmod(i, K)
            tiles = {}
            for tile in range(i // SUB, KROWS // SUB):
                start = at * WIDTH + tile * SUB
                tiles[tile] = system_ref[second, start : start + SUB, :]
            value = tiles[i // SUB]
            tiles[i // SUB] = jnp.where(row == i % SUB, 1.5 * value + 1.0, value)
            matrix.append(tiles)

        def entry(i, column):
            return matrix[i][column // SUB][column % SUB : column % SUB + 1]

        for pivot in range(2 * K):
            inverse = 1.0 / entry(pivot, pivot)
            chosen = {tile: value * inverse for tile, value in matrix[pivot].items()}
            for i in range(2 * K):
                if i == pivot:
                    continue
                scale = entry(pivot, i) if i > pivot else entry(i, pivot)
                for tile in range(max(i, pivot + 1) // SUB, KROWS // SUB):
                    matrix[i][tile] = matrix[i][tile] - scale * chosen[tile]
            matrix[pivot] = chosen
        for tile in range(KROWS // SUB):
            update = jnp.zeros((SUB, LANE), jnp.float32)
            for i in range(tile * SUB, min((tile + 1) * SUB, 2 * K)):
                update = jnp.where(row == i % SUB, entry(i, RHS), update)
            at = slice(tile * SUB, (tile + 1) * SUB)
            coef_ref[at, :] = coef_ref[at, :] + update

    first_weights()
    solve_step()

    def later_step(index, carry):
        later_weights()
        solve_step()
        return carry

    lax.fori_loop(1, ITERS, later_step, 0)

    square_ref[...] = jnp.zeros_like(square_ref)
    lane = lax.broadcasted_iota(jnp.int32, (KROWS, LANE), 1)
    square_ref[0:KROWS, :] = jnp.where(lane < owned, coef_ref[...], 0.0)
    result = square_ref[...].T[0:owned]
    packed = result[0:1]
    for fiber in range(1, owned):
        packed = packed + pltpu.roll(result[fiber : fiber + 1], fiber * (LANE // owned), 1)
    send_ref[...] = jnp.broadcast_to(packed, send_ref.shape)


def fit(got, start, poly, split, ready, owned, devices, height, sources):
    rows = got.shape[1]
    steps = got.shape[0] // (height * sources)
    count = -(-5 * owned // SUB) * SUB
    vmem = pl.BlockSpec(memory_space=pltpu.VMEM)
    return pl.pallas_call(
        functools.partial(fit_kernel, height, sources, owned),
        out_shape=jax.ShapeDtypeStruct((devices, LANE), jnp.float32),
        in_specs=[vmem] * 6,
        out_specs=vmem,
        scratch_shapes=[
            pltpu.VMEM((owned * PIX + owned, steps, rows), jnp.float32),
            pltpu.VMEM((count * steps, rows), jnp.float32),
            pltpu.VMEM((KROWS, LANE), jnp.float32),
            pltpu.VMEM((owned, KROWS, rows), jnp.float32),
            pltpu.VMEM((LANE, LANE), jnp.float32),
            pltpu.VMEM((count + SUB, LANE), jnp.float32),
            pltpu.VMEM((2, 2 * LANE, LANE), jnp.float32),
        ],
        compiler_params=pltpu.CompilerParams(vmem_limit_bytes=VMEM_BYTES),
        name="fit",
    )(got, start, poly, split, ready, jnp.asarray(system_map()))


def residual_kernel(
    owned,
    coef_ref,
    local_ref,
    weight_ref,
    frames_ref,
    trace_hbm,
    width_hbm,
    image_hbm,
    trace_ref,
    width_ref,
    image_ref,
    shape_ref,
    small_sems,
    image_sems,
):
    lamps, rows, cols = frames_ref.shape
    me = lax.axis_index("rows") * lax.axis_size("fib") + lax.axis_index("fib")
    own = coef_ref[pl.ds(me, 1), :]
    each = LANE // owned
    for fiber in range(owned):
        at = fiber * each
        trace_ref[fiber : fiber + 1, :] = own[:, at : at + K]
        width_ref[fiber : fiber + 1, :] = own[:, at + K : at + 2 * K]
    leaving = start_copies([trace_ref, width_ref], [trace_hbm, width_hbm], small_sems)

    flipped = coef_ref[...].T
    coef = jnp.concatenate(
        [flipped[fiber * each : fiber * each + KROWS] for fiber in range(owned)], axis=1
    )
    centre = jnp.zeros((rows, coef.shape[1]), jnp.float32)
    spread = jnp.zeros((rows, coef.shape[1]), jnp.float32)
    for order in range(K):
        poly = jnp.concatenate([local_ref[order]] * (coef.shape[1] // LANE), axis=1)
        centre = centre + poly * coef[order : order + 1]
        spread = spread + poly * coef[K + order : K + order + 1]
    inverse = jnp.exp(-spread) * coef[RHS : RHS + 1]
    pixel = (lax.broadcasted_iota(jnp.int32, (rows, LANE), 1) % PIX).astype(jnp.float32)
    offset = pixel - (PIX - 1) / 2.0
    def leave(lamp):
        return pltpu.make_async_copy(
            image_ref.at[lamp], image_hbm.at[lamp], image_sems.at[lamp]
        )

    def finish(lamp, here, shape):
        frame = frames_ref[lamp, :, here].astype(jnp.float32)
        model = weight_ref[lamp, :, here] * shape
        image_ref[lamp, :, here] = (frame - model).astype(jnp.bfloat16)

    early = min(EARLY, lamps)
    for tile in range(cols // LANE):
        here = slice(tile * LANE, (tile + 1) * LANE)
        scaled = (offset - per_column(centre, tile, owned, True)) * per_column(
            inverse, tile, owned, True
        )
        shape = jnp.exp(-0.5 * scaled * scaled)
        shape_ref[:, here] = shape
        for lamp in range(early):
            finish(lamp, here, shape)
    for lamp in range(early):
        leave(lamp).start()

    def one_lamp(lamp, carry):
        for tile in range(cols // LANE):
            here = slice(tile * LANE, (tile + 1) * LANE)
            finish(lamp, here, shape_ref[:, here])
        leave(lamp).start()
        return carry

    lax.fori_loop(early, lamps, one_lamp, 0)
    for lamp in range(lamps):
        leave(lamp).wait()
    for copy in leaving:
        copy.wait()


def residual(owned, coef, local, weight, frames):
    lamps, rows, cols = frames.shape
    vmem = pl.BlockSpec(memory_space=pltpu.VMEM)
    hbm = pl.BlockSpec(memory_space=pltpu.HBM)
    fitted = jax.ShapeDtypeStruct((owned, K), jnp.float32)
    return pl.pallas_call(
        functools.partial(residual_kernel, owned),
        out_shape=(fitted, fitted, jax.ShapeDtypeStruct(frames.shape, jnp.bfloat16)),
        in_specs=[vmem] * 4,
        out_specs=[hbm] * 3,
        scratch_shapes=[
            pltpu.VMEM((owned, K), jnp.float32),
            pltpu.VMEM((owned, K), jnp.float32),
            pltpu.VMEM(frames.shape, jnp.bfloat16),
            pltpu.VMEM((rows, cols), jnp.float32),
            pltpu.SemaphoreType.DMA((2,)),
            pltpu.SemaphoreType.DMA((lamps,)),
        ],
        compiler_params=pltpu.CompilerParams(vmem_limit_bytes=VMEM_BYTES),
        name="residual",
    )(coef, local, weight, frames)


def body(frames, amplitude, line_start, bundle_width, fiber_bundle, trace_coef, width_coef):
    sources = lax.axis_size("fib")
    devices = lax.axis_size("rows") * sources
    rows = frames.shape[1]
    owned = trace_coef.shape[0]
    height = owned * PIX + owned
    keep, send, weight, start = collapse(
        frames, amplitude, line_start, bundle_width, fiber_bundle, trace_coef, width_coef, height
    )
    came = lax.ppermute(send, "fib", [(index, index ^ 1) for index in range(sources)])
    poly, split, local, ready = tables(start, owned, rows)
    came, poly, split, local, ready = lax.optimization_barrier((came, poly, split, local, ready))
    alike = [
        [index for index in reversed(range(devices)) if index % 2 == odd] for odd in range(2)
    ]
    unit = 4 if height % 4 == 0 else 1
    got = lax.all_to_all(
        (keep + came).reshape(devices // 2, height // unit, unit, rows),
        BOTH,
        0,
        0,
        axis_index_groups=alike,
        tiled=True,
    ).reshape(devices // 2 * height, rows)
    reply = fit(got, start, poly, split, ready, owned, devices, height, sources // 2)
    coef = lax.all_to_all(reply, BOTH, 0, 0, tiled=True)
    return residual(owned, coef, local, weight, frames)


def solution(mesh):
    return jax.shard_map(
        body,
        mesh=mesh,
        in_specs=(
            P("fib", "rows", None),
            P("fib", None),
            P("fib", None),
            P(),
            P(),
            P(BOTH, None),
            P(BOTH, None),
        ),
        out_specs=(P(BOTH, None), P(BOTH, None), P("fib", "rows", None)),
        check_vma=False,
    )
```
